32 devices in a mesh: dp: 16 (over z, y, core), seq: 2 (over x).
Axes of the slice: x: 2, y: 2, z: 4, core: 2. Of those that a mesh axis runs over, the one named last changes fastest.
Arguments:
- tokens: bfloat16 [4096, 2304], P(('dp', 'seq')), may hold values from -6 to 6
- doc_lengths: int32 [16, 3], P('dp'), may hold values from 1 to 170, 256 in all within a row
- attn_weight: bfloat16 [2304, 6144], P(('dp', 'seq')), may hold values from -0.125 to 0.125
- ffn_weight: bfloat16 [9216, 6912], P(('dp', 'seq')), may hold values from -0.125 to 0.125
- gains: bfloat16 [2304, 4], P(('dp', 'seq')), may hold values from 0.099609375 to 1.8984375
- out_grad: bfloat16 [4096, 2304], P(('dp', 'seq')), may hold values from -6 to 6
Outputs:
- block_out: bfloat16 [4096, 2304], P(('dp', 'seq'))
- tokens_grad: float32 [4096, 2304], P(('dp', 'seq'))
- attn_weight_grad: float32 [2304, 6144], P(('dp', 'seq'))
- ffn_weight_grad: float32 [9216, 6912], P(('dp', 'seq'))
- gains_grad: float32 [2304, 4], P(('dp', 'seq'))
The draws below stay inside these ranges and needn't reach their ends.
Inputs may be any that keep to these rules, and one draw needn't show every extreme that they name: `doc_lengths`: row b lists in order the lengths of the 3 documents of pack b; they add up to 256, and one of them is 170.
All inputs are finite; a program needn't handle non-finite values.
Results may differ from the reference program's by a relative error of at most 0.014.
Values may be sent and summed in bfloat16 or wider, within the bound.
A program may use at most 448 MiB of HBM per device.

```python
import math
import jax
import jax.numpy as jnp
import numpy as np
from jax import lax

D = 2304
FF = 9216
HEADS = 8
KV_HEADS = 4
HEAD_DIM = 256
DOCS = 3
PACK = 256
WINDOW = 128
MOST_LEN = 170
ATTN_COLS = 6144
TOKENS = 4096
N_DP = 16


def strengthened(values, rng, source, target, parts, factor):
    def block_of(axis_at):
        return (jnp.arange(values.shape[axis_at]) // (values.shape[axis_at] // parts)).reshape((-1,) + (1,) * (values.ndim - 1 - axis_at))

    one_side = jax.random.permutation(rng, parts)[block_of(target)]
    far = (block_of(target) + parts // 2) % parts
    return jnp.where((block_of(source) == one_side) | (block_of(source) == far), factor * values, values)


def shard_levels(stream_key, shape, pieces, low, largest):
    level, own = 1.0, jax.random.fold_in(stream_key, 6)
    for position, shards_of in pieces:
        draws = jnp.exp(jax.random.uniform(jax.random.fold_in(own, position), (shards_of,), jnp.float32, low / len(pieces), largest / len(pieces)))
        level = level * jnp.repeat(draws, shape[position] // shards_of).reshape([-1 if axis == position else 1 for axis in range(len(shape))])
    return level


def profile(number_of, total, most, skew):
    weights = [(1 << 20) // math.isqrt(rank ** skew) + 1 for rank in range(2, number_of + 1)]
    rest, counts = total - most - (number_of - 1), [1] * (number_of - 1)
    while rest > 0:
        movable = [i for i in range(number_of - 1) if counts[i] < most]
        whole, budget = sum([weights[i] for i in movable]), rest
        for i in movable:
            addition = min(most - counts[i], max(1, budget * weights[i] // whole), rest)
            counts[i] = counts[i] + addition
            rest = rest - addition
    return np.array([most] + counts)


def ragged_sizes(stream_key, count, total, most, lean):
    if count == 2:
        one = jax.random.randint(stream_key, (), max(1, total - most), min(most, total - 1) + 1)
        return jnp.stack([one, total - one])
    sizes = jnp.asarray(profile(count, total, most, lean), jnp.int32)
    pairs = (count - 1) // 2
    source_of, receiver = sizes[1:1 + 2 * pairs:2], sizes[2:2 + 2 * pairs:2]
    margin = jnp.minimum(source_of - 1, most - receiver)
    passed = jax.random.randint(jax.random.fold_in(stream_key, 1), (pairs,), 0, 1 << 20) % (margin + 1)
    sizes = sizes.at[1:1 + 2 * pairs:2].set(source_of - passed).at[2:2 + 2 * pairs:2].set(receiver + passed)
    return sizes[jax.random.permutation(jax.random.fold_in(stream_key, 2), count)]


def bell_draw(key, dims, spread, reach, pieces=(), kind=jnp.bfloat16):
    loudness = shard_levels(key, dims, pieces, -0.22, 0.18) if pieces else 1.0
    values = jax.random.normal(key, dims, jnp.float32) * spread * loudness
    return jnp.minimum(jnp.maximum(values, -reach), reach).astype(kind)


def gaussian_with(key, dims, scale, bound, pieces, heavy, held_as=jnp.bfloat16):
    array = scale * jax.random.normal(key, dims, jnp.float32)
    if pieces:
        array = array * shard_levels(key, dims, pieces, -0.22, 0.18)
    return jnp.clip(strengthened(array, jax.random.fold_in(key, 3), *heavy), -bound, bound).astype(held_as)


def setup_inputs(seed: int = 0) -> dict:
    key_list = jax.random.split(jax.random.key(seed), 7)
    return {
        "tokens": gaussian_with(key_list[0], (TOKENS, D), 1.0, 6.0, ((0, 32),), (0, 1, 32, 2.75)),
        "doc_lengths": jax.vmap(lambda own: ragged_sizes(own, DOCS, PACK, MOST_LEN, 2))(jax.random.split(key_list[1], N_DP)).reshape((N_DP, DOCS)).astype(jnp.int32),
        "attn_weight": bell_draw(key_list[2], (D, ATTN_COLS), D ** -0.5, 0.125, ((0, 32),)),
        "ffn_weight": bell_draw(key_list[3], (FF, 3 * D), D ** -0.5, 0.125, ((0, 32),)),
        "gains": jnp.clip(1.0 + 0.18 * jax.random.normal(key_list[4], (D, 4), jnp.float32), 0.099609375, 1.8984375).astype(jnp.bfloat16),
        "out_grad": bell_draw(key_list[5], (TOKENS, D), 1.0, 6.0, ((0, 32),)),
    }


@jax.custom_vjp
def low(v):
    return lax.optimization_barrier(v.astype(jnp.bfloat16)).astype(jnp.float32)

@jax.custom_vjp
def low_back(v):
    return v

def low_keep(v):
    return (low(v), None)

def low_pass(kept, grad):
    return (grad,)

def back_keep(v):
    return (v, None)

def back_low(kept, grad):
    return (low(grad),)
low.defvjp(low_keep, low_pass)
low_back.defvjp(back_keep, back_low)
soft_cap = 50.0
eps_norm = 1e-06
rope_base = 10000.0
gelu_coef = math.sqrt(2.0 / math.pi)

def matmul(left_side, right_side):
    return jnp.dot(left_side, right_side, precision=lax.Precision.HIGHEST, preferred_element_type=jnp.float32)

def gelu_tanh(value):
    return 0.5 * value * (1.0 + jnp.tanh(gelu_coef * (value + 0.044715 * value * value * value)))

def rms_norm(value, gain_vec):
    return value * lax.rsqrt(lax.optimization_barrier(jnp.mean(value * value, axis=-1, keepdims=True)) + eps_norm) * gain_vec

def doc_layout(lengths, places):
    doc_ends = jnp.cumsum(lengths, dtype=jnp.int32)
    starts = doc_ends - lengths
    doc_ids = lax.optimization_barrier(jnp.sum((places[:, None] >= doc_ends[None, :]).astype(jnp.int32), axis=1, dtype=jnp.int32))
    onehot = doc_ids[:, None] == jnp.arange(lengths.shape[0], dtype=jnp.int32)[None, :]
    doc_first = lax.optimization_barrier(jnp.sum(jnp.where(onehot, starts[None, :], 0), axis=1, dtype=jnp.int32))
    return (doc_ids, places - doc_first)

def rotate(value, doc_pos):
    half_dim = value.shape[-1] // 2
    frequency = rope_base ** (-2.0 * jnp.arange(half_dim, dtype=jnp.float32) / value.shape[-1])
    angles = doc_pos.astype(jnp.float32)[:, None] * frequency[None, :]
    cosine = jnp.cos(angles)[:, None, :]
    sine_part = jnp.sin(angles)[:, None, :]
    first_half = value[..., :half_dim]
    second_half = value[..., half_dim:]
    return jnp.concatenate([first_half * cosine - second_half * sine_part, second_half * cosine + first_half * sine_part], axis=-1)

def pack_attention(pack_item):
    queries, key_rows, values, doc_ids = pack_item
    places = jnp.arange(doc_ids.shape[0], dtype=jnp.int32)
    allowed = (doc_ids[:, None] == doc_ids[None, :]) & (places[None, :] <= places[:, None]) & (places[:, None] - places[None, :] < WINDOW)
    scores = low_back(jnp.einsum('qkgd,pkd->kgqp', queries, key_rows, precision=lax.Precision.HIGHEST, preferred_element_type=jnp.float32))
    capped = jnp.where(allowed[None, None], soft_cap * jnp.tanh(scores / soft_cap), -1e+30)
    row_max = lax.optimization_barrier(jnp.max(capped, axis=-1, keepdims=True))
    exp_terms = jnp.exp(capped - row_max)
    attn_probs = low(exp_terms / lax.optimization_barrier(jnp.sum(exp_terms, axis=-1, keepdims=True)))
    return jnp.einsum('kgqp,pkd->qkgd', attn_probs, values, precision=lax.Precision.HIGHEST, preferred_element_type=jnp.float32)

def forward(tokens_f, attn_f, ffn_f, gains_f, lengths):
    tok_count = tokens_f.shape[0]
    pack_count = lengths.shape[0]
    q_cols = HEADS * HEAD_DIM
    k_cols = KV_HEADS * HEAD_DIM
    proj_cols = q_cols + 2 * k_cols
    group_size = HEADS // KV_HEADS
    places = jnp.broadcast_to(jnp.arange(PACK, dtype=jnp.int32)[None, :], (pack_count, PACK))
    doc_ids, doc_pos = jax.vmap(doc_layout)(lengths, places)
    doc_pos = doc_pos.reshape(tok_count)
    attn_in = low(rms_norm(tokens_f, gains_f[:, 0]))
    projected = low_back(matmul(attn_in, attn_f[:, :proj_cols]))
    queries = low(rotate(projected[:, :q_cols].reshape(tok_count, HEADS, HEAD_DIM), doc_pos) * HEAD_DIM ** (-0.5))
    key_rows = low(rotate(projected[:, q_cols:q_cols + k_cols].reshape(tok_count, KV_HEADS, HEAD_DIM), doc_pos))
    values = low(projected[:, q_cols + k_cols:].reshape(tok_count, KV_HEADS, HEAD_DIM))
    mixed_heads = lax.map(jax.checkpoint(pack_attention), (queries.reshape(pack_count, PACK, KV_HEADS, group_size, HEAD_DIM), key_rows.reshape(pack_count, PACK, KV_HEADS, HEAD_DIM), values.reshape(pack_count, PACK, KV_HEADS, HEAD_DIM), doc_ids))
    mixed_heads = low_back(low(mixed_heads.reshape(tok_count, q_cols)))
    attn_out = low_back(matmul(mixed_heads, attn_f[:, proj_cols:].T))
    middle = tokens_f + rms_norm(attn_out, gains_f[:, 1])
    ffn_input = low(rms_norm(middle, gains_f[:, 2]))
    gate_pre = low_back(matmul(ffn_input, ffn_f[:, :D].T))
    up_pre = low_back(matmul(ffn_input, ffn_f[:, D:2 * D].T))
    hidden = low(gelu_tanh(gate_pre) * up_pre)
    ffn_out = low_back(matmul(hidden, ffn_f[:, 2 * D:]))
    return middle + rms_norm(ffn_out, gains_f[:, 3])

def reference(tokens, doc_lengths, attn_weight, ffn_weight, gains, out_grad):
    group_packs = 1
    for candidate in range(1, N_DP + 1):
        if N_DP % candidate == 0 and candidate * PACK <= 4096:
            group_packs = candidate
    step_count = N_DP // group_packs
    attn_f = attn_weight.astype(jnp.float32)
    ffn_f = ffn_weight.astype(jnp.float32)
    gains_f = gains.astype(jnp.float32)
    inputs = (tokens.astype(jnp.float32).reshape(step_count, group_packs * PACK, D), doc_lengths.reshape(step_count, group_packs, DOCS), out_grad.astype(jnp.float32).reshape(step_count, group_packs * PACK, D))

    def one_group(totals, group_item):
        tokens_g, lengths, cotangent = group_item

        def forward_group(tokens_in, attn_in, ffn_in, gains_in):
            return forward(tokens_in, attn_in, ffn_in, gains_in, lengths)
        result, pull_back = jax.vjp(forward_group, tokens_g, attn_f, ffn_f, gains_f)
        d_tokens, d_attn, d_ffn, d_gains = pull_back(cotangent)
        return ((totals[0] + d_attn, totals[1] + d_ffn, totals[2] + d_gains), (result.astype(jnp.bfloat16), d_tokens))
    initial = (jnp.zeros(attn_f.shape, jnp.float32), jnp.zeros(ffn_f.shape, jnp.float32), jnp.zeros(gains_f.shape, jnp.float32))
    totals, outputs = lax.scan(one_group, initial, inputs)
    block_out = outputs[0].reshape(TOKENS, D)
    tokens_grad = outputs[1].reshape(TOKENS, D)
    return (block_out, tokens_grad, totals[0], totals[1], totals[2])
```

```python
import functools
import math

import jax
import jax.numpy as jnp
from jax import lax
from jax.experimental import pallas as pl
from jax.experimental.pallas import tpu as pltpu
from jax.sharding import PartitionSpec as P

D = 2304
HEADS = 8
KV_HEADS = 4
HEAD_DIM = 256
WINDOW = 128


soft_cap = 50.0
eps_norm = 1e-06
rope_base = 10000.0
gelu_coef = math.sqrt(2.0 / math.pi)


MESH = pl.DeviceIdType.MESH


def gelu_tanh(value):
    return 0.5 * value * (1.0 + jnp.tanh(gelu_coef * (value + 0.044715 * value * value * value)))


def gated_gelu(gate_pre, up_pre):
    return gelu_tanh(gate_pre) * up_pre


def gate_grads(gate_rows, d_hidden):
    d_gate, d_up = jax.vjp(gated_gelu, gate_rows[:, 0], gate_rows[:, 1])[1](d_hidden)
    return jnp.stack([d_gate, d_up], axis=1).astype(jnp.bfloat16)


def rms_norm(value, gain_vec):
    return value * lax.rsqrt(jnp.mean(value * value, axis=-1, keepdims=True) + eps_norm) * gain_vec


def norm_back(value, gain_vec, incoming):
    return jax.vjp(rms_norm, value, gain_vec)[1](incoming)


def doc_layout(lengths, places):
    doc_ends = jnp.cumsum(lengths, dtype=jnp.int32)
    starts = doc_ends - lengths
    doc_ids = jnp.sum(
        (places[:, None] >= doc_ends[None, :]).astype(jnp.int32), axis=1, dtype=jnp.int32
    )
    onehot = doc_ids[:, None] == jnp.arange(lengths.shape[0], dtype=jnp.int32)[None, :]
    doc_first = jnp.sum(jnp.where(onehot, starts[None, :], 0), axis=1, dtype=jnp.int32)
    return (doc_ids, places - doc_first)


def rotate(value, doc_pos):
    half_dim = value.shape[-1] // 2
    frequency = rope_base ** (-2.0 * jnp.arange(half_dim, dtype=jnp.float32) / value.shape[-1])
    angles = doc_pos.astype(jnp.float32)[:, None] * frequency[None, :]
    cosine = jnp.cos(angles)[:, None, :]
    sine_part = jnp.sin(angles)[:, None, :]
    first_half = value[..., :half_dim]
    second_half = value[..., half_dim:]
    return jnp.concatenate(
        [
            first_half * cosine - second_half * sine_part,
            second_half * cosine + first_half * sine_part,
        ],
        axis=-1,
    )


def contract_rows(left_side, right_side):
    return lax.dot_general(
        left_side, right_side, (((0,), (0,)), ((), ())), preferred_element_type=jnp.float32
    )


def contract_cols(left_side, right_side):
    return lax.dot_general(
        left_side, right_side, (((1,), (1,)), ((), ())), preferred_element_type=jnp.float32
    )


def key_mask(query_places, query_docs, key_places, key_docs):
    return (
        (key_places[None, :] >= 0)
        & (query_docs[:, None] == key_docs[None, :])
        & (key_places[None, :] <= query_places[:, None])
        & (query_places[:, None] - key_places[None, :] < WINDOW)
    )


def attn_scores(queries, all_keys, allowed):
    scores = jnp.einsum("qkgd,pkd->kgqp", queries, all_keys, preferred_element_type=jnp.float32)
    capped = jnp.where(allowed[None, None], soft_cap * jnp.tanh(scores / soft_cap), -1e30)
    return (scores, capped)


def swapped(x):
    return lax.ppermute(x, "seq", [(0, 1), (1, 0)])


def place_of(n_dp):
    dp = lax.axis_index("dp")
    seq = lax.axis_index("seq")
    a, b, c = dp // 4, lax.rem(dp // 2, 2), lax.rem(dp, 2)
    return a, b, c, seq


def number(a, b, c):
    return (a * 2 + b) * 2 + c


def enter(line, a, b, c, seq):
    barrier = pltpu.get_barrier_semaphore()

    def tell(a2, b2, c2):
        pl.semaphore_signal(
            barrier, inc=1, device_id=(number(a2, b2, c2), seq), device_id_type=MESH
        )

    tell(a, b, 1 - c)
    tell(a, 1 - b, c)

    @pl.when(a > 0)
    def _():
        tell(a - 1, b, c)

    @pl.when(a < line - 1)
    def _():
        tell(a + 1, b, c)

    peers = 2 + jnp.minimum(a, 1) + jnp.minimum(line - 1 - a, 1)
    pl.semaphore_wait(barrier, peers)


def gather_kernel(n_dp, x_ref, out_ref, own_sem, send_sem, recv_sem):
    line = n_dp // 4
    a, b, c, seq = place_of(n_dp)
    me = number(a, b, c)
    own = pltpu.make_async_copy(x_ref, out_ref.at[me], own_sem)
    own.start()
    enter(line, a, b, c, seq)

    def copy(way, src, block, a2, b2, c2):
        return pltpu.make_async_remote_copy(
            src_ref=src,
            dst_ref=out_ref.at[block],
            send_sem=send_sem.at[way, block],
            recv_sem=recv_sem.at[block],
            device_id=(number(a2, b2, c2), seq),
            device_id_type=MESH,
        )

    def up(src, block):
        return copy(0, src, block, a + 1, b, c)

    def down(src, block):
        return copy(1, src, block, a - 1, b, c)

    def across(src, block):
        return copy(2, src, block, a, 1 - b, c)

    def over(src, block):
        return copy(3, src, block, a, b, 1 - c)

    has_up, has_down = a < line - 1, a > 0

    @pl.when(has_up)
    def _():
        up(x_ref, me).start()

    @pl.when(has_down)
    def _():
        down(x_ref, me).start()

    across(x_ref, me).start()
    over(x_ref, me).start()

    def arrived(block):
        over(out_ref.at[block], block).wait_recv()

    for k in range(1, line + 1):
        if k < line:

            @pl.when(a - k >= 0)
            def _(k=k):
                block = number(a - k, b, c)
                arrived(block)
                view = out_ref.at[block]

                @pl.when(has_up)
                def _():
                    up(view, block).start()

                across(view, block).start()
                over(view, block).start()

            @pl.when(a + k < line)
            def _(k=k):
                block = number(a + k, b, c)
                arrived(block)
                view = out_ref.at[block]

                @pl.when(has_down)
                def _():
                    down(view, block).start()

                across(view, block).start()
                over(view, block).start()

        j = k - 1
        for sign in (-1, 1) if j else (1,):

            @pl.when((a + sign * j >= 0) & (a + sign * j < line))
            def _(j=j, sign=sign):
                block = number(a + sign * j, 1 - b, c)
                arrived(block)
                over(out_ref.at[block], block).start()

    for other in range(n_dp // 2):
        block = other * 2 + 1 - c
        arrived(block)

    own.wait()
    for i in range(line):
        block = number(i, b, c)
        across(out_ref.at[block], block).wait_send()
        over(out_ref.at[block], block).wait_send()
        second = number(i, 1 - b, c)
        over(out_ref.at[second], second).wait_send()

        @pl.when(has_up & (i <= a))
        def _(block=block):
            up(out_ref.at[block], block).wait_send()

        @pl.when(has_down & (i >= a))
        def _(block=block):
            down(out_ref.at[block], block).wait_send()


def gathered(x, n_dp, collective_id):
    return pl.pallas_call(
        functools.partial(gather_kernel, n_dp),
        out_shape=jax.ShapeDtypeStruct((n_dp, *x.shape), x.dtype),
        in_specs=[pl.BlockSpec(memory_space=pltpu.VMEM)],
        out_specs=pl.BlockSpec(memory_space=pl.ANY),
        scratch_shapes=[
            pltpu.SemaphoreType.DMA,
            pltpu.SemaphoreType.DMA((4, n_dp)),
            pltpu.SemaphoreType.DMA((n_dp,)),
        ],
        compiler_params=pltpu.CompilerParams(
            collective_id=collective_id, has_side_effects=True
        ),
    )(x)


def scatter_kernel(n_dp, p_ref, out_ref, from_core, from_pair, up_in, down_in, pair_out, up_out,
                   down_out, core_send, core_recv, pair_send, pair_recv, up_send, up_recv,
                   down_send, down_recv):
    line = n_dp // 4
    a, b, c, seq = place_of(n_dp)
    f32 = jnp.float32
    enter(line, a, b, c, seq)

    def core_copy(block):
        half = block // 2
        return pltpu.make_async_remote_copy(
            src_ref=p_ref.at[block],
            dst_ref=from_core.at[half],
            send_sem=core_send.at[half],
            recv_sem=core_recv.at[half],
            device_id=(number(a, b, 1 - c), seq),
            device_id_type=MESH,
        )

    def pair_copy(to):
        return pltpu.make_async_remote_copy(
            src_ref=pair_out.at[to],
            dst_ref=from_pair.at[to],
            send_sem=pair_send.at[to],
            recv_sem=pair_recv.at[to],
            device_id=(number(a, 1 - b, c), seq),
            device_id_type=MESH,
        )

    def up_copy(to):
        return pltpu.make_async_remote_copy(
            src_ref=up_out.at[to],
            dst_ref=up_in.at[to],
            send_sem=up_send.at[to],
            recv_sem=up_recv.at[to],
            device_id=(number(a + 1, b, c), seq),
            device_id_type=MESH,
        )

    def down_copy(to):
        return pltpu.make_async_remote_copy(
            src_ref=down_out.at[to],
            dst_ref=down_in.at[to],
            send_sem=down_send.at[to],
            recv_sem=down_recv.at[to],
            device_id=(number(a - 1, b, c), seq),
            device_id_type=MESH,
        )

    def each_target(act):
        for k in range(line - 1, 0, -1):

            @pl.when(a + k < line)
            def _(k=k):
                act(a + k, 1)

            @pl.when(a - k >= 0)
            def _(k=k):
                act(a - k, -1)

        act(a, 0)

    each_target(lambda to, way: core_copy(number(to, 1 - b, 1 - c)).start())
    each_target(lambda to, way: core_copy(number(to, b, 1 - c)).start())

    def send_pair(to, way):
        core_copy(number(to, 1 - b, c)).wait_recv()
        pair_out[to] = (
            p_ref[number(to, 1 - b, c)].astype(f32) + from_core[to * 2 + 1 - b].astype(f32)
        ).astype(pair_out.dtype)
        pair_copy(to).start()

    each_target(send_pair)

    def own_sum(to):
        core_copy(number(to, b, c)).wait_recv()
        pair_copy(to).wait_recv()
        return (
            p_ref[number(to, b, c)].astype(f32)
            + from_core[to * 2 + b].astype(f32)
            + from_pair[to].astype(f32)
        )

    def send_line(to, way):
        if way == 1:
            total = own_sum(to)

            @pl.when(a > 0)
            def _():
                up_copy(to).wait_recv()
                up_out[to] = (total + up_in[to].astype(f32)).astype(up_out.dtype)

            @pl.when(a == 0)
            def _():
                up_out[to] = total.astype(up_out.dtype)

            up_copy(to).start()
        elif way == -1:
            total = own_sum(to)

            @pl.when(a < line - 1)
            def _():
                down_copy(to).wait_recv()
                down_out[to] = (total + down_in[to].astype(f32)).astype(down_out.dtype)

            @pl.when(a == line - 1)
            def _():
                down_out[to] = total.astype(down_out.dtype)

            down_copy(to).start()
        else:
            out_ref[...] = own_sum(to)

            @pl.when(a > 0)
            def _():
                up_copy(to).wait_recv()
                out_ref[...] += up_in[to].astype(f32)

            @pl.when(a < line - 1)
            def _():
                down_copy(to).wait_recv()
                out_ref[...] += down_in[to].astype(f32)

    each_target(send_line)

    for i in range(n_dp // 2):
        core_copy(i * 2 + 1 - c).wait_send()
    for i in range(line):
        pair_copy(i).wait_send()

        @pl.when(i > a)
        def _(i=i):
            up_copy(i).wait_send()

        @pl.when(i < a)
        def _(i=i):
            down_copy(i).wait_send()


def scattered(parts, collective_id):
    n_dp, rows, cols = parts.shape
    held = 3 * n_dp * (rows + 16) * cols * 2
    pieces = 1
    while held > pieces * 50 * 2**20 or cols % (128 * pieces):
        pieces += 1
    width = cols // pieces
    return jnp.concatenate(
        [
            scattered_piece(parts[:, :, i * width : (i + 1) * width], collective_id)
            for i in range(pieces)
        ],
        axis=1,
    )


def scattered_piece(parts, collective_id):
    n_dp, rows, cols = parts.shape
    line = n_dp // 4
    block = (rows, cols)
    return pl.pallas_call(
        functools.partial(scatter_kernel, n_dp),
        out_shape=jax.ShapeDtypeStruct(block, jnp.float32),
        in_specs=[pl.BlockSpec(memory_space=pltpu.VMEM)],
        out_specs=pl.BlockSpec(memory_space=pltpu.VMEM),
        scratch_shapes=[pltpu.VMEM((n_dp // 2, *block), parts.dtype)]
        + [pltpu.VMEM((line, *block), parts.dtype)] * 6
        + [pltpu.SemaphoreType.DMA((n_dp // 2,))] * 2
        + [pltpu.SemaphoreType.DMA((line,))] * 6,
        compiler_params=pltpu.CompilerParams(
            collective_id=collective_id, has_side_effects=True
        ),
    )(parts)


def mine_and_other(halves, seq_index):
    first = seq_index == 0
    return (
        jnp.where(first, halves[0], halves[1]),
        jnp.where(first, halves[1], halves[0]),
    )


def in_order(own, other, seq_index):
    first = seq_index == 0
    return jnp.where(first, own, other), jnp.where(first, other, own)


def column_halves(weight):
    q_cols, k_cols = HEADS * HEAD_DIM, KV_HEADS * HEAD_DIM
    starts = (0, q_cols, q_cols + k_cols, q_cols + 2 * k_cols)
    sizes = (q_cols // 2, k_cols // 2, k_cols // 2, q_cols // 2)
    return [
        jnp.concatenate(
            [weight[:, s + h * n : s + (h + 1) * n] for s, n in zip(starts, sizes)], axis=1
        )
        for h in range(2)
    ]


def on_device(tokens, doc_lengths, attn_weight, ffn_weight, gains, out_grad):
    tok_rows = tokens.shape[0]
    n_dp = lax.axis_size("dp")
    heads, kv_heads = HEADS // 2, KV_HEADS // 2
    q_cols = heads * HEAD_DIM
    k_cols = kv_heads * HEAD_DIM
    proj_cols = q_cols + 2 * k_cols
    half_cols = proj_cols + q_cols
    group_size = HEADS // KV_HEADS
    query_scale = HEAD_DIM ** (-0.5)
    bf16 = jnp.bfloat16
    seq_index = lax.axis_index("seq")
    weight_rows = attn_weight.shape[0]

    run = jnp.arange(tok_rows, dtype=jnp.int32)
    places = jnp.concatenate([seq_index * tok_rows + run, (1 - seq_index) * tok_rows + run])
    docs, pos = doc_layout(doc_lengths[0], places)
    allowed = key_mask(places, docs, places, docs)

    gain_cols = jnp.pad(gains, ((0, 0), (0, 124)))
    my_cols, other_cols = mine_and_other(column_halves(attn_weight), seq_index)
    my_cols = jnp.concatenate([my_cols, gain_cols], axis=1)
    other_cols = jnp.concatenate([other_cols, gain_cols], axis=1)
    partner_cols = swapped(other_cols)
    other_tokens = swapped(tokens)
    ffn_own, partner_cols = lax.optimization_barrier((ffn_weight, partner_cols))
    ffn_other = swapped(ffn_own)
    block = jnp.concatenate(in_order(my_cols, partner_cols, seq_index), axis=0)
    attn_full = gathered(block, n_dp, 0).reshape(-1, half_cols + 128)
    gain_vals = attn_full[:, half_cols : half_cols + 4].astype(jnp.float32).T
    attn_weights = attn_full[:, :proj_cols]
    out_weights = attn_full[:, proj_cols:half_cols]

    pack_tokens = jnp.concatenate([tokens, other_tokens]).astype(jnp.float32)
    tokens_f = tokens.astype(jnp.float32)
    attn_in = rms_norm(pack_tokens, gain_vals[0]).astype(bf16)
    projected = jnp.dot(attn_in, attn_weights, preferred_element_type=jnp.float32)
    pack = 2 * tok_rows
    queries = (
        rotate(projected[:, :q_cols].reshape(pack, heads, HEAD_DIM), pos) * query_scale
    ).astype(bf16)
    queries = queries.reshape(pack, kv_heads, group_size, HEAD_DIM)
    keys = rotate(
        projected[:, q_cols : q_cols + k_cols].reshape(pack, kv_heads, HEAD_DIM), pos
    ).astype(bf16)
    values = projected[:, q_cols + k_cols :].reshape(pack, kv_heads, HEAD_DIM).astype(bf16)
    scores, capped = attn_scores(queries, keys, allowed)
    row_max = jnp.max(capped, axis=-1, keepdims=True)
    exp_terms = jnp.exp(capped - row_max)
    row_total = jnp.sum(exp_terms, axis=-1, keepdims=True)
    log_total = row_max + jnp.log(row_total)
    attn_probs = (exp_terms / row_total).astype(bf16)
    mixed_heads = jnp.einsum(
        "kgqp,pkd->qkgd", attn_probs, values, preferred_element_type=jnp.float32
    )
    mixed_heads = mixed_heads.reshape(pack, q_cols).astype(bf16)
    attn_part_out = contract_cols(mixed_heads, out_weights)
    attn_out = attn_part_out[:tok_rows] + swapped(attn_part_out[tok_rows:].astype(bf16)).astype(
        jnp.float32
    )
    middle = tokens_f + rms_norm(attn_out, gain_vals[1])
    ffn_input = rms_norm(middle, gain_vals[2]).astype(bf16)

    unit_weights = jnp.concatenate([ffn_own, ffn_other], axis=0)
    unit_count = unit_weights.shape[0]
    gate_weights = unit_weights[:, :D]
    up_weights = unit_weights[:, D : 2 * D]
    down_weights = unit_weights[:, 2 * D :]
    ffn_all = gathered(ffn_input, n_dp, 1).reshape(-1, D)
    gate = contract_cols(ffn_all, gate_weights)
    up = contract_cols(ffn_all, up_weights)
    hidden = gated_gelu(gate, up).astype(bf16)
    ffn_parts = jnp.dot(hidden, down_weights, preferred_element_type=jnp.float32).astype(bf16)
    ffn_out = scattered(ffn_parts.reshape(n_dp, tok_rows, D), 2)
    out_gain = gain_vals[3]
    block_out = (middle + rms_norm(ffn_out, out_gain)).astype(bf16)
    cotangent = out_grad.astype(jnp.float32)
    d_ffn_f, d_gain_out = norm_back(ffn_out, out_gain, cotangent)
    d_ffn_all = gathered(d_ffn_f.astype(bf16), n_dp, 1).reshape(-1, D)
    d_hidden = contract_cols(d_ffn_all, down_weights)
    d_gate, d_up = jax.vjp(gated_gelu, gate, up)[1](d_hidden)
    d_gate, d_up = d_gate.astype(bf16), d_up.astype(bf16)
    d_parts = (
        jnp.dot(d_gate, gate_weights, preferred_element_type=jnp.float32)
        + jnp.dot(d_up, up_weights, preferred_element_type=jnp.float32)
    ).astype(bf16)
    d_ffn_input = scattered(d_parts.reshape(n_dp, tok_rows, D), 2)

    own_units = unit_count // 2
    weight_sum = [
        contract_rows(d_gate, ffn_all),
        contract_rows(d_up, ffn_all),
        contract_rows(hidden, d_ffn_all),
    ]
    sent = jnp.concatenate([w[own_units:].astype(bf16) for w in weight_sum], axis=1)
    kept = jnp.concatenate([w[:own_units] for w in weight_sum], axis=1)
    ffn_weight_grad = kept + swapped(sent).astype(jnp.float32)

    d_middle_add, d_gain_ffn = norm_back(middle, gain_vals[2], d_ffn_input)
    d_middle = cotangent + d_middle_add
    d_attn_f, d_gain_post = norm_back(attn_out, gain_vals[1], d_middle)
    d_attn_own = d_attn_f.astype(bf16)
    d_attn = jnp.concatenate([d_attn_own, swapped(d_attn_own)])
    out_cols_grad = contract_rows(d_attn, mixed_heads)
    d_mixed = jnp.dot(d_attn, out_weights, preferred_element_type=jnp.float32).astype(bf16)
    d_mixed = d_mixed.reshape(pack, kv_heads, group_size, HEAD_DIM)
    attn_p = jnp.exp(capped - log_total)
    d_probs = jnp.einsum("qkgd,pkd->kgqp", d_mixed, values, preferred_element_type=jnp.float32)
    d_values = jnp.einsum(
        "kgqp,qkgd->pkd", attn_probs, d_mixed, preferred_element_type=jnp.float32
    )
    d_capped = attn_p * (d_probs - jnp.sum(attn_p * d_probs, axis=-1, keepdims=True))
    tanh_part = jnp.tanh(scores / soft_cap)
    d_scores = (d_capped * (1.0 - tanh_part * tanh_part)).astype(bf16)
    d_queries = jnp.einsum("kgqp,pkd->qkgd", d_scores, keys, preferred_element_type=jnp.float32)
    d_keys = jnp.einsum("kgqp,qkgd->pkd", d_scores, queries, preferred_element_type=jnp.float32)
    d_query_raw = rotate(d_queries.reshape(pack, heads, HEAD_DIM) * query_scale, -pos)
    d_key_raw = rotate(d_keys, -pos)
    d_projected = jnp.concatenate(
        [
            d_query_raw.reshape(pack, q_cols),
            d_key_raw.reshape(pack, k_cols),
            d_values.reshape(pack, k_cols),
        ],
        axis=1,
    ).astype(bf16)
    proj_grad = contract_rows(attn_in, d_projected)
    d_attn_in_part = contract_cols(d_projected, attn_weights)
    d_attn_in = d_attn_in_part[:tok_rows] + swapped(
        d_attn_in_part[tok_rows:].astype(bf16)
    ).astype(jnp.float32)
    d_tokens_add, d_gain_in = norm_back(tokens_f, gain_vals[0], d_attn_in)
    tokens_grad = d_middle + d_tokens_add

    gain_part = jnp.stack([d_gain_in, d_gain_post, d_gain_ffn, d_gain_out], axis=1)
    attn_parts = jnp.concatenate(
        [proj_grad.astype(bf16), out_cols_grad.astype(bf16),
         jnp.pad(gain_part.astype(bf16), ((0, 0), (0, 124)))],
        axis=1,
    )
    attn_sum = scattered(attn_parts.reshape(n_dp, 2 * weight_rows, half_cols + 128), 3)
    mine, others = mine_and_other(
        (attn_sum[:weight_rows], attn_sum[weight_rows:]), seq_index
    )
    partner = swapped(others.astype(bf16)).astype(jnp.float32)
    gains_grad = mine[:, half_cols : half_cols + 4] + partner[:, half_cols : half_cols + 4]
    first, second = in_order(mine, partner, seq_index)
    cuts = ((0, q_cols), (q_cols, q_cols + k_cols), (q_cols + k_cols, proj_cols),
            (proj_cols, half_cols))
    attn_weight_grad = jnp.concatenate(
        [half[:, lo:hi] for lo, hi in cuts for half in (first, second)], axis=1
    )
    return (block_out, tokens_grad, attn_weight_grad, ffn_weight_grad, gains_grad)


def solution(mesh):
    return jax.shard_map(
        on_device,
        mesh=mesh,
        in_specs=(
            P(("dp", "seq"), None),
            P("dp", None),
            P(("dp", "seq"), None),
            P(("dp", "seq"), None),
            P(("dp", "seq"), None),
            P(("dp", "seq"), None),
        ),
        out_specs=(
            P(("dp", "seq"), None),
            P(("dp", "seq"), None),
            P(("dp", "seq"), None),
            P(("dp", "seq"), None),
            P(("dp", "seq"), None),
        ),
        check_vma=False,
    )
```

```python
import functools
import math

import jax
import jax.numpy as jnp
from jax import lax
from jax.experimental import pallas as pl
from jax.experimental.pallas import tpu as pltpu
from jax.sharding import PartitionSpec as P

D = 2304
HEADS = 8
KV_HEADS = 4
HEAD_DIM = 256
WINDOW = 128


soft_cap = 50.0
eps_norm = 1e-06
rope_base = 10000.0
gelu_coef = math.sqrt(2.0 / math.pi)


MESH = pl.DeviceIdType.MESH


def gelu_tanh(value):
    return 0.5 * value * (1.0 + jnp.tanh(gelu_coef * (value + 0.044715 * value * value * value)))


def gated_gelu(gate_pre, up_pre):
    return gelu_tanh(gate_pre) * up_pre


def gate_grads(gate_rows, d_hidden):
    d_gate, d_up = jax.vjp(gated_gelu, gate_rows[:, 0], gate_rows[:, 1])[1](d_hidden)
    return jnp.stack([d_gate, d_up], axis=1).astype(jnp.bfloat16)


def rms_norm(value, gain_vec):
    return value * lax.rsqrt(jnp.mean(value * value, axis=-1, keepdims=True) + eps_norm) * gain_vec


def norm_back(value, gain_vec, incoming):
    return jax.vjp(rms_norm, value, gain_vec)[1](incoming)


def doc_layout(lengths, places):
    doc_ends = jnp.cumsum(lengths, dtype=jnp.int32)
    starts = doc_ends - lengths
    doc_ids = jnp.sum(
        (places[:, None] >= doc_ends[None, :]).astype(jnp.int32), axis=1, dtype=jnp.int32
    )
    onehot = doc_ids[:, None] == jnp.arange(lengths.shape[0], dtype=jnp.int32)[None, :]
    doc_first = jnp.sum(jnp.where(onehot, starts[None, :], 0), axis=1, dtype=jnp.int32)
    return (doc_ids, places - doc_first)


def rotate(value, doc_pos):
    half_dim = value.shape[-1] // 2
    frequency = rope_base ** (-2.0 * jnp.arange(half_dim, dtype=jnp.float32) / value.shape[-1])
    angles = doc_pos.astype(jnp.float32)[:, None] * frequency[None, :]
    cosine = jnp.cos(angles)[:, None, :]
    sine_part = jnp.sin(angles)[:, None, :]
    first_half = value[..., :half_dim]
    second_half = value[..., half_dim:]
    return jnp.concatenate(
        [
            first_half * cosine - second_half * sine_part,
            second_half * cosine + first_half * sine_part,
        ],
        axis=-1,
    )


def contract_rows(left_side, right_side):
    return lax.dot_general(
        left_side, right_side, (((0,), (0,)), ((), ())), preferred_element_type=jnp.float32
    )


def contract_cols(left_side, right_side):
    return lax.dot_general(
        left_side, right_side, (((1,), (1,)), ((), ())), preferred_element_type=jnp.float32
    )


def key_mask(query_places, query_docs, key_places, key_docs):
    return (
        (key_places[None, :] >= 0)
        & (query_docs[:, None] == key_docs[None, :])
        & (key_places[None, :] <= query_places[:, None])
        & (query_places[:, None] - key_places[None, :] < WINDOW)
    )


def attn_scores(queries, all_keys, allowed):
    scores = jnp.einsum("qkgd,pkd->kgqp", queries, all_keys, preferred_element_type=jnp.float32)
    capped = jnp.where(allowed[None, None], soft_cap * jnp.tanh(scores / soft_cap), -1e30)
    return (scores, capped)


def swapped(x):
    return lax.ppermute(x, "seq", [(0, 1), (1, 0)])


def place_of(n_dp):
    dp = lax.axis_index("dp")
    seq = lax.axis_index("seq")
    a, b, c = dp // 4, lax.rem(dp // 2, 2), lax.rem(dp, 2)
    return a, b, c, seq


def number(a, b, c):
    return (a * 2 + b) * 2 + c


def enter(line, a, b, c, seq):
    barrier = pltpu.get_barrier_semaphore()

    def tell(a2, b2, c2):
        pl.semaphore_signal(
            barrier, inc=1, device_id=(number(a2, b2, c2), seq), device_id_type=MESH
        )

    tell(a, b, 1 - c)
    tell(a, 1 - b, c)

    @pl.when(a > 0)
    def _():
        tell(a - 1, b, c)

    @pl.when(a < line - 1)
    def _():
        tell(a + 1, b, c)

    peers = 2 + jnp.minimum(a, 1) + jnp.minimum(line - 1 - a, 1)
    pl.semaphore_wait(barrier, peers)


def gather_kernel(n_dp, x_ref, out_ref, own_sem, send_sem, recv_sem):
    line = n_dp // 4
    a, b, c, seq = place_of(n_dp)
    me = number(a, b, c)
    own = pltpu.make_async_copy(x_ref, out_ref.at[me], own_sem)
    own.start()
    enter(line, a, b, c, seq)

    def copy(way, src, block, a2, b2, c2):
        return pltpu.make_async_remote_copy(
            src_ref=src,
            dst_ref=out_ref.at[block],
            send_sem=send_sem.at[way, block],
            recv_sem=recv_sem.at[block],
            device_id=(number(a2, b2, c2), seq),
            device_id_type=MESH,
        )

    def up(src, block):
        return copy(0, src, block, a + 1, b, c)

    def down(src, block):
        return copy(1, src, block, a - 1, b, c)

    def across(src, block):
        return copy(2, src, block, a, 1 - b, c)

    def over(src, block):
        return copy(3, src, block, a, b, 1 - c)

    has_up, has_down = a < line - 1, a > 0

    @pl.when(has_up)
    def _():
        up(x_ref, me).start()

    @pl.when(has_down)
    def _():
        down(x_ref, me).start()

    across(x_ref, me).start()
    over(x_ref, me).start()

    def arrived(block):
        over(out_ref.at[block], block).wait_recv()

    for k in range(1, line + 1):
        if k < line:

            @pl.when(a - k >= 0)
            def _(k=k):
                block = number(a - k, b, c)
                arrived(block)
                view = out_ref.at[block]

                @pl.when(has_up)
                def _():
                    up(view, block).start()

                across(view, block).start()
                over(view, block).start()

            @pl.when(a + k < line)
            def _(k=k):
                block = number(a + k, b, c)
                arrived(block)
                view = out_ref.at[block]

                @pl.when(has_down)
                def _():
                    down(view, block).start()

                across(view, block).start()
                over(view, block).start()

        j = k - 1
        for sign in (-1, 1) if j else (1,):

            @pl.when((a + sign * j >= 0) & (a + sign * j < line))
            def _(j=j, sign=sign):
                block = number(a + sign * j, 1 - b, c)
                arrived(block)
                over(out_ref.at[block], block).start()

    for other in range(n_dp // 2):
        block = other * 2 + 1 - c
        arrived(block)

    own.wait()
    for i in range(line):
        block = number(i, b, c)
        across(out_ref.at[block], block).wait_send()
        over(out_ref.at[block], block).wait_send()
        second = number(i, 1 - b, c)
        over(out_ref.at[second], second).wait_send()

        @pl.when(has_up & (i <= a))
        def _(block=block):
            up(out_ref.at[block], block).wait_send()

        @pl.when(has_down & (i >= a))
        def _(block=block):
            down(out_ref.at[block], block).wait_send()


def gathered(x, n_dp, collective_id):
    return pl.pallas_call(
        functools.partial(gather_kernel, n_dp),
        out_shape=jax.ShapeDtypeStruct((n_dp, *x.shape), x.dtype),
        in_specs=[pl.BlockSpec(memory_space=pltpu.VMEM)],
        out_specs=pl.BlockSpec(memory_space=pl.ANY),
        scratch_shapes=[
            pltpu.SemaphoreType.DMA,
            pltpu.SemaphoreType.DMA((4, n_dp)),
            pltpu.SemaphoreType.DMA((n_dp,)),
        ],
        compiler_params=pltpu.CompilerParams(
            collective_id=collective_id, has_side_effects=True
        ),
        cost_estimate=pl.CostEstimate(
            flops=0, bytes_accessed=150_000_000, transcendentals=0
        ),
    )(x)


def scatter_steps(n_dp, place, produce, core_source, out_ref, from_core, from_pair, up_buf,
                  down_buf, pair_out, core_send, core_recv, pair_send, pair_recv, up_send,
                  up_recv, down_send, down_recv):
    line = n_dp // 4
    a, b, c, seq = place
    enter(line, a, b, c, seq)

    def core_copy(block):
        half = block // 2
        return pltpu.make_async_remote_copy(
            src_ref=core_source(block),
            dst_ref=from_core.at[half],
            send_sem=core_send.at[half],
            recv_sem=core_recv.at[half],
            device_id=(number(a, b, 1 - c), seq),
            device_id_type=MESH,
        )

    def pair_copy(to):
        return pltpu.make_async_remote_copy(
            src_ref=pair_out.at[to],
            dst_ref=from_pair.at[to],
            send_sem=pair_send.at[to],
            recv_sem=pair_recv.at[to],
            device_id=(number(a, 1 - b, c), seq),
            device_id_type=MESH,
        )

    def up_copy(to):
        return pltpu.make_async_remote_copy(
            src_ref=up_buf.at[to],
            dst_ref=up_buf.at[to],
            send_sem=up_send.at[to],
            recv_sem=up_recv.at[to],
            device_id=(number(a + 1, b, c), seq),
            device_id_type=MESH,
        )

    def down_copy(to):
        return pltpu.make_async_remote_copy(
            src_ref=down_buf.at[to],
            dst_ref=down_buf.at[to],
            send_sem=down_send.at[to],
            recv_sem=down_recv.at[to],
            device_id=(number(a - 1, b, c), seq),
            device_id_type=MESH,
        )

    def each_target(act):
        for k in range(line - 1, 0, -1):

            @pl.when(a + k < line)
            def _(k=k):
                act(a + k, 1)

            @pl.when(a - k >= 0)
            def _(k=k):
                act(a - k, -1)

        act(a, 0)

    def send_core(block):
        produce(block, None, core_source(block))
        core_copy(block).start()

    each_target(lambda to, way: send_core(number(to, 1 - b, 1 - c)))
    each_target(lambda to, way: send_core(number(to, b, 1 - c)))

    def send_pair(to, way):
        block = number(to, 1 - b, c)
        core_copy(block).wait_recv()
        produce(block, [from_core.at[block // 2]], pair_out.at[to])
        pair_copy(to).start()

    each_target(send_pair)

    def line_sum(to, more, dst):
        block = number(to, b, c)
        produce(block, [from_core.at[block // 2], from_pair.at[to], *more], dst)

    def send_line(to, way):
        core_copy(number(to, b, c)).wait_recv()
        pair_copy(to).wait_recv()
        if way:
            buf, copy = (up_buf, up_copy) if way == 1 else (down_buf, down_copy)
            at_end = (a == 0) if way == 1 else (a == line - 1)

            @pl.when(at_end)
            def _():
                line_sum(to, [], buf.at[to])

            @pl.when(jnp.logical_not(at_end))
            def _():
                copy(to).wait_recv()
                line_sum(to, [buf.at[to]], buf.at[to])

            copy(to).start()
        else:
            line_sum(to, [], out_ref)
            for copy, buf, there in (
                (up_copy, up_buf, a > 0),
                (down_copy, down_buf, a < line - 1),
            ):

                @pl.when(there)
                def _(copy=copy, buf=buf):
                    copy(to).wait_recv()
                    add_rows(out_ref, buf.at[to])

    each_target(send_line)

    for i in range(n_dp // 2):
        core_copy(i * 2 + 1 - c).wait_send()
    for i in range(line):
        pair_copy(i).wait_send()

        @pl.when(i > a)
        def _(i=i):
            up_copy(i).wait_send()

        @pl.when(i < a)
        def _(i=i):
            down_copy(i).wait_send()


def row_tiles(rows):
    return 16 if rows % 16 == 0 else rows


def add_rows(out_ref, term):
    tile = row_tiles(out_ref.shape[0])

    def step(i, _):
        at = pl.ds(pl.multiple_of(i * tile, tile), tile)
        out_ref[at, :] += term[at, :].astype(jnp.float32)
        return 0

    lax.fori_loop(0, out_ref.shape[0] // tile, step, 0)


def scatter_kernel(n_dp, p_ref, out_ref, *scratch):
    def produce(block, terms, dst):
        if terms is None:
            return
        tile = row_tiles(p_ref.shape[1])

        def step(i, _):
            at = pl.ds(pl.multiple_of(i * tile, tile), tile)
            total = p_ref[block, at, :].astype(jnp.float32)
            for term in terms:
                total += term[at, :].astype(jnp.float32)
            dst[at, :] = total.astype(dst.dtype)
            return 0

        lax.fori_loop(0, p_ref.shape[1] // tile, step, 0)

    scatter_steps(
        n_dp, place_of(n_dp), produce, lambda block: p_ref.at[block], out_ref, *scratch
    )


def product_kernel(n_dp, left_a, right_a, left_b, right_b, extra, out_ref, core_out, *scratch):
    cols_a, cols_b = right_a.shape[1], right_b.shape[1]

    def produce(block, terms, dst):
        def part(left, right, first, wide):
            def step(i, _):
                inner = pl.ds(pl.multiple_of(i * wide, wide), wide)
                outer = pl.ds(pl.multiple_of(first + i * wide, 128), wide)
                total = jnp.dot(
                    left[block], right[:, inner], preferred_element_type=jnp.float32
                )
                for term in terms or []:
                    total += term[:, outer].astype(jnp.float32)
                dst[:, outer] = total.astype(dst.dtype)
                return 0

            lax.fori_loop(0, right.shape[1] // wide, step, 0)

        part(left_a, right_a, 0, 256)
        part(left_b, right_b, cols_a, 256)
        last = pl.ds(cols_a + cols_b, extra.shape[2])
        total = extra[block].astype(jnp.float32)
        for term in terms or []:
            total += term[:, last].astype(jnp.float32)
        dst[:, last] = total.astype(dst.dtype)

    scatter_steps(
        n_dp, place_of(n_dp), produce, lambda block: core_out.at[block // 2], out_ref, *scratch
    )


def scatter_scratch(n_dp, rows, cols, dtype):
    line = n_dp // 4
    return (
        [pltpu.VMEM((n_dp // 2, rows, cols), dtype)]
        + [pltpu.VMEM((line, rows, cols), dtype)] * 4
        + [pltpu.SemaphoreType.DMA((n_dp // 2,))] * 2
        + [pltpu.SemaphoreType.DMA((line,))] * 6
    )


def scattered_products(left_a, right_a, left_b, right_b, extra, collective_id):
    n_dp, rows, _ = left_a.shape
    cols = right_a.shape[1] + right_b.shape[1] + extra.shape[2]
    return pl.pallas_call(
        functools.partial(product_kernel, n_dp),
        out_shape=jax.ShapeDtypeStruct((rows, cols), jnp.float32),
        in_specs=[pl.BlockSpec(memory_space=pltpu.VMEM)] * 5,
        out_specs=pl.BlockSpec(memory_space=pltpu.VMEM),
        scratch_shapes=[pltpu.VMEM((n_dp // 2, rows, cols), jnp.bfloat16)]
        + scatter_scratch(n_dp, rows, cols, jnp.bfloat16),
        compiler_params=pltpu.CompilerParams(
            collective_id=collective_id, has_side_effects=True
        ),
        cost_estimate=pl.CostEstimate(
            flops=0, bytes_accessed=200_000_000, transcendentals=0
        ),
    )(left_a, right_a, left_b, right_b, extra)


def scattered(parts, collective_id):
    n_dp, rows, cols = parts.shape
    held = n_dp * (1 + 1 / 2 + 1) * rows * cols * 2
    pieces = 1
    while held > pieces * 50 * 2**20 or cols % (128 * pieces):
        pieces += 1
    width = cols // pieces
    return jnp.concatenate(
        [
            scattered_piece(parts[:, :, i * width : (i + 1) * width], collective_id)
            for i in range(pieces)
        ],
        axis=1,
    )


def scattered_piece(parts, collective_id):
    n_dp, rows, cols = parts.shape
    return pl.pallas_call(
        functools.partial(scatter_kernel, n_dp),
        out_shape=jax.ShapeDtypeStruct((rows, cols), jnp.float32),
        in_specs=[pl.BlockSpec(memory_space=pltpu.VMEM)],
        out_specs=pl.BlockSpec(memory_space=pltpu.VMEM),
        scratch_shapes=scatter_scratch(n_dp, rows, cols, parts.dtype),
        compiler_params=pltpu.CompilerParams(
            collective_id=collective_id, has_side_effects=True
        ),
        cost_estimate=pl.CostEstimate(
            flops=0, bytes_accessed=150_000_000, transcendentals=0
        ),
    )(parts)


def mine_and_other(halves, seq_index):
    first = seq_index == 0
    return (
        jnp.where(first, halves[0], halves[1]),
        jnp.where(first, halves[1], halves[0]),
    )


def in_order(own, other, seq_index):
    first = seq_index == 0
    return jnp.where(first, own, other), jnp.where(first, other, own)


def column_halves(weight):
    q_cols, k_cols = HEADS * HEAD_DIM, KV_HEADS * HEAD_DIM
    starts = (0, q_cols, q_cols + k_cols, q_cols + 2 * k_cols)
    sizes = (q_cols // 2, k_cols // 2, k_cols // 2, q_cols // 2)
    return [
        jnp.concatenate(
            [weight[:, s + h * n : s + (h + 1) * n] for s, n in zip(starts, sizes)], axis=1
        )
        for h in range(2)
    ]


def on_device(tokens, doc_lengths, attn_weight, ffn_weight, gains, out_grad):
    tok_rows = tokens.shape[0]
    n_dp = lax.axis_size("dp")
    heads, kv_heads = HEADS // 2, KV_HEADS // 2
    q_cols = heads * HEAD_DIM
    k_cols = kv_heads * HEAD_DIM
    proj_cols = q_cols + 2 * k_cols
    half_cols = proj_cols + q_cols
    group_size = HEADS // KV_HEADS
    query_scale = HEAD_DIM ** (-0.5)
    bf16 = jnp.bfloat16
    seq_index = lax.axis_index("seq")
    weight_rows = attn_weight.shape[0]

    run = jnp.arange(tok_rows, dtype=jnp.int32)
    places = jnp.concatenate([seq_index * tok_rows + run, (1 - seq_index) * tok_rows + run])
    docs, pos = doc_layout(doc_lengths[0], places)
    allowed = key_mask(places, docs, places, docs)

    gain_cols = jnp.pad(gains, ((0, 0), (0, 124)))
    my_cols, other_cols = mine_and_other(column_halves(attn_weight), seq_index)
    my_cols = jnp.concatenate([my_cols, gain_cols], axis=1)
    other_cols = jnp.concatenate([other_cols, gain_cols], axis=1)
    partner_cols = swapped(other_cols)
    other_tokens = swapped(tokens)
    ffn_own, partner_cols = lax.optimization_barrier((ffn_weight, partner_cols))
    ffn_other = swapped(ffn_own)
    block = jnp.concatenate(in_order(my_cols, partner_cols, seq_index), axis=0)
    attn_full = gathered(block, n_dp, 0).reshape(-1, half_cols + 128)
    gain_vals = attn_full[:, half_cols : half_cols + 4].astype(jnp.float32).T
    attn_weights = attn_full[:, :proj_cols]
    out_weights = attn_full[:, proj_cols:half_cols]

    pack_tokens = jnp.concatenate([tokens, other_tokens]).astype(jnp.float32)
    tokens_f = tokens.astype(jnp.float32)
    attn_in = rms_norm(pack_tokens, gain_vals[0]).astype(bf16)
    projected = jnp.dot(attn_in, attn_weights, preferred_element_type=jnp.float32)
    pack = 2 * tok_rows
    queries = (
        rotate(projected[:, :q_cols].reshape(pack, heads, HEAD_DIM), pos) * query_scale
    ).astype(bf16)
    queries = queries.reshape(pack, kv_heads, group_size, HEAD_DIM)
    keys = rotate(
        projected[:, q_cols : q_cols + k_cols].reshape(pack, kv_heads, HEAD_DIM), pos
    ).astype(bf16)
    values = projected[:, q_cols + k_cols :].reshape(pack, kv_heads, HEAD_DIM).astype(bf16)
    scores, capped = attn_scores(queries, keys, allowed)
    row_max = jnp.max(capped, axis=-1, keepdims=True)
    exp_terms = jnp.exp(capped - row_max)
    row_total = jnp.sum(exp_terms, axis=-1, keepdims=True)
    log_total = row_max + jnp.log(row_total)
    attn_probs = (exp_terms / row_total).astype(bf16)
    mixed_heads = jnp.einsum(
        "kgqp,pkd->qkgd", attn_probs, values, preferred_element_type=jnp.float32
    )
    mixed_heads = mixed_heads.reshape(pack, q_cols).astype(bf16)
    attn_part_out = contract_cols(mixed_heads, out_weights)
    attn_out = attn_part_out[:tok_rows] + swapped(attn_part_out[tok_rows:].astype(bf16)).astype(
        jnp.float32
    )
    middle = tokens_f + rms_norm(attn_out, gain_vals[1])
    ffn_input = rms_norm(middle, gain_vals[2]).astype(bf16)

    unit_weights = jnp.concatenate([ffn_own, ffn_other], axis=0)
    unit_count = unit_weights.shape[0]
    gate_weights = unit_weights[:, :D]
    up_weights = unit_weights[:, D : 2 * D]
    down_weights = unit_weights[:, 2 * D :]
    ffn_all = gathered(ffn_input, n_dp, 1).reshape(-1, D)
    gate = contract_cols(ffn_all, gate_weights)
    up = contract_cols(ffn_all, up_weights)
    hidden = gated_gelu(gate, up).astype(bf16)
    ffn_parts = jnp.dot(hidden, down_weights, preferred_element_type=jnp.float32).astype(bf16)
    ffn_out = scattered(ffn_parts.reshape(n_dp, tok_rows, D), 2)
    out_gain = gain_vals[3]
    block_out = (middle + rms_norm(ffn_out, out_gain)).astype(bf16)
    cotangent = out_grad.astype(jnp.float32)
    d_ffn_f, d_gain_out = norm_back(ffn_out, out_gain, cotangent)
    d_ffn_all = gathered(d_ffn_f.astype(bf16), n_dp, 1).reshape(-1, D)
    d_hidden = contract_cols(d_ffn_all, down_weights)
    d_gate, d_up = jax.vjp(gated_gelu, gate, up)[1](d_hidden)
    d_gate, d_up = d_gate.astype(bf16), d_up.astype(bf16)
    d_parts = (
        jnp.dot(d_gate, gate_weights, preferred_element_type=jnp.float32)
        + jnp.dot(d_up, up_weights, preferred_element_type=jnp.float32)
    ).astype(bf16)
    d_ffn_input = scattered(d_parts.reshape(n_dp, tok_rows, D), 2)

    own_units = unit_count // 2
    weight_sum = [
        contract_rows(d_gate, ffn_all),
        contract_rows(d_up, ffn_all),
        contract_rows(hidden, d_ffn_all),
    ]
    sent = jnp.concatenate([w[own_units:].astype(bf16) for w in weight_sum], axis=1)
    kept = jnp.concatenate([w[:own_units] for w in weight_sum], axis=1)
    ffn_weight_grad = kept + swapped(sent).astype(jnp.float32)

    d_middle_add, d_gain_ffn = norm_back(middle, gain_vals[2], d_ffn_input)
    d_middle = cotangent + d_middle_add
    d_attn_f, d_gain_post = norm_back(attn_out, gain_vals[1], d_middle)
    d_attn_own = d_attn_f.astype(bf16)
    d_attn = jnp.concatenate([d_attn_own, swapped(d_attn_own)])
    d_mixed = jnp.dot(d_attn, out_weights, preferred_element_type=jnp.float32).astype(bf16)
    d_mixed = d_mixed.reshape(pack, kv_heads, group_size, HEAD_DIM)
    attn_p = jnp.exp(capped - log_total)
    d_probs = jnp.einsum("qkgd,pkd->kgqp", d_mixed, values, preferred_element_type=jnp.float32)
    d_values = jnp.einsum(
        "kgqp,qkgd->pkd", attn_probs, d_mixed, preferred_element_type=jnp.float32
    )
    d_capped = attn_p * (d_probs - jnp.sum(attn_p * d_probs, axis=-1, keepdims=True))
    tanh_part = jnp.tanh(scores / soft_cap)
    d_scores = (d_capped * (1.0 - tanh_part * tanh_part)).astype(bf16)
    d_queries = jnp.einsum("kgqp,pkd->qkgd", d_scores, keys, preferred_element_type=jnp.float32)
    d_keys = jnp.einsum("kgqp,qkgd->pkd", d_scores, queries, preferred_element_type=jnp.float32)
    d_query_raw = rotate(d_queries.reshape(pack, heads, HEAD_DIM) * query_scale, -pos)
    d_key_raw = rotate(d_keys, -pos)
    d_projected = jnp.concatenate(
        [
            d_query_raw.reshape(pack, q_cols),
            d_key_raw.reshape(pack, k_cols),
            d_values.reshape(pack, k_cols),
        ],
        axis=1,
    ).astype(bf16)
    d_attn_in_part = contract_cols(d_projected, attn_weights)
    d_attn_in = d_attn_in_part[:tok_rows] + swapped(
        d_attn_in_part[tok_rows:].astype(bf16)
    ).astype(jnp.float32)
    normed = pack_tokens * lax.rsqrt(
        jnp.mean(pack_tokens * pack_tokens, axis=-1, keepdims=True) + eps_norm
    )
    d_gain_in = jnp.sum(d_attn_in_part * normed, axis=0)

    gain_part = jnp.stack([d_gain_in, d_gain_post, d_gain_ffn, d_gain_out], axis=1)
    block_rows = (n_dp, 2 * weight_rows)
    attn_sum = scattered_products(
        attn_in.T.reshape(*block_rows, pack),
        d_projected,
        d_attn.T.reshape(*block_rows, pack),
        mixed_heads,
        jnp.pad(gain_part.astype(bf16), ((0, 0), (0, 124))).reshape(*block_rows, 128),
        3,
    )
    d_tokens_add = norm_back(tokens_f, gain_vals[0], d_attn_in)[0]
    tokens_grad = d_middle + d_tokens_add
    mine, others = mine_and_other(
        (attn_sum[:weight_rows], attn_sum[weight_rows:]), seq_index
    )
    partner = swapped(others.astype(bf16)).astype(jnp.float32)
    gains_grad = mine[:, half_cols : half_cols + 4] + partner[:, half_cols : half_cols + 4]
    first, second = in_order(mine, partner, seq_index)
    cuts = ((0, q_cols), (q_cols, q_cols + k_cols), (q_cols + k_cols, proj_cols),
            (proj_cols, half_cols))
    attn_weight_grad = jnp.concatenate(
        [half[:, lo:hi] for lo, hi in cuts for half in (first, second)], axis=1
    )
    return (block_out, tokens_grad, attn_weight_grad, ffn_weight_grad, gains_grad)


def solution(mesh):
    return jax.shard_map(
        on_device,
        mesh=mesh,
        in_specs=(
            P(("dp", "seq"), None),
            P("dp", None),
            P(("dp", "seq"), None),
            P(("dp", "seq"), None),
            P(("dp", "seq"), None),
            P(("dp", "seq"), None),
        ),
        out_specs=(
            P(("dp", "seq"), None),
            P(("dp", "seq"), None),
            P(("dp", "seq"), None),
            P(("dp", "seq"), None),
            P(("dp", "seq"), None),
        ),
        check_vma=False,
    )
```

```python
import functools
import math

import jax
import jax.numpy as jnp
from jax import lax
from jax.experimental import pallas as pl
from jax.experimental.pallas import tpu as pltpu
from jax.sharding import PartitionSpec as P

D = 2304
HEADS = 8
KV_HEADS = 4
HEAD_DIM = 256
WINDOW = 128


soft_cap = 50.0
eps_norm = 1e-06
rope_base = 10000.0
gelu_coef = math.sqrt(2.0 / math.pi)


MESH = pl.DeviceIdType.MESH


def gelu_tanh(value):
    return 0.5 * value * (1.0 + jnp.tanh(gelu_coef * (value + 0.044715 * value * value * value)))


def gated_gelu(gate_pre, up_pre):
    return gelu_tanh(gate_pre) * up_pre


def rms_norm(value, gain_vec):
    return value * lax.rsqrt(jnp.mean(value * value, axis=-1, keepdims=True) + eps_norm) * gain_vec


def norm_back(value, gain_vec, incoming):
    return jax.vjp(rms_norm, value, gain_vec)[1](incoming)


def doc_layout(lengths, places):
    doc_ends = jnp.cumsum(lengths, dtype=jnp.int32)
    starts = doc_ends - lengths
    doc_ids = jnp.sum(
        (places[:, None] >= doc_ends[None, :]).astype(jnp.int32), axis=1, dtype=jnp.int32
    )
    onehot = doc_ids[:, None] == jnp.arange(lengths.shape[0], dtype=jnp.int32)[None, :]
    doc_first = jnp.sum(jnp.where(onehot, starts[None, :], 0), axis=1, dtype=jnp.int32)
    return (doc_ids, places - doc_first)


def rotate(value, doc_pos):
    half_dim = value.shape[-1] // 2
    frequency = rope_base ** (-2.0 * jnp.arange(half_dim, dtype=jnp.float32) / value.shape[-1])
    angles = doc_pos.astype(jnp.float32)[:, None] * frequency[None, :]
    cosine = jnp.cos(angles)[:, None, :]
    sine_part = jnp.sin(angles)[:, None, :]
    first_half = value[..., :half_dim]
    second_half = value[..., half_dim:]
    return jnp.concatenate(
        [
            first_half * cosine - second_half * sine_part,
            second_half * cosine + first_half * sine_part,
        ],
        axis=-1,
    )


def contract_rows(left_side, right_side):
    return lax.dot_general(
        left_side, right_side, (((0,), (0,)), ((), ())), preferred_element_type=jnp.float32
    )


def contract_cols(left_side, right_side):
    return lax.dot_general(
        left_side, right_side, (((1,), (1,)), ((), ())), preferred_element_type=jnp.float32
    )


def key_mask(query_places, query_docs, key_places, key_docs):
    return (
        (key_places[None, :] >= 0)
        & (query_docs[:, None] == key_docs[None, :])
        & (key_places[None, :] <= query_places[:, None])
        & (query_places[:, None] - key_places[None, :] < WINDOW)
    )


def attn_scores(queries, all_keys, allowed):
    scores = jnp.einsum("qkgd,pkd->kgqp", queries, all_keys, preferred_element_type=jnp.float32)
    capped = jnp.where(allowed[None, None], soft_cap * jnp.tanh(scores / soft_cap), -1e30)
    return (scores, capped)


def swapped(x):
    return lax.ppermute(x, "seq", [(0, 1), (1, 0)])


def place_of():
    dp = lax.axis_index("dp")
    seq = lax.axis_index("seq")
    a, b, c = dp // 4, lax.rem(dp // 2, 2), lax.rem(dp, 2)
    return a, b, c, seq


def number(a, b, c):
    return (a * 2 + b) * 2 + c


def enter(line, a, b, c, seq):
    barrier = pltpu.get_barrier_semaphore()

    def tell(a2, b2, c2):
        pl.semaphore_signal(
            barrier, inc=1, device_id=(number(a2, b2, c2), seq), device_id_type=MESH
        )

    tell(a, b, 1 - c)
    tell(a, 1 - b, c)

    @pl.when(a > 0)
    def _():
        tell(a - 1, b, c)

    @pl.when(a < line - 1)
    def _():
        tell(a + 1, b, c)

    peers = 2 + jnp.minimum(a, 1) + jnp.minimum(line - 1 - a, 1)
    pl.semaphore_wait(barrier, peers)


def gather_kernel(n_dp, x_ref, out_ref, own_sem, send_sem, recv_sem):
    line = n_dp // 4
    a, b, c, seq = place_of()
    me = number(a, b, c)
    own = pltpu.make_async_copy(x_ref, out_ref.at[me], own_sem)
    own.start()
    enter(line, a, b, c, seq)

    def copy(way, src, block, a2, b2, c2):
        return pltpu.make_async_remote_copy(
            src_ref=src,
            dst_ref=out_ref.at[block],
            send_sem=send_sem.at[way, block],
            recv_sem=recv_sem.at[block],
            device_id=(number(a2, b2, c2), seq),
            device_id_type=MESH,
        )

    def up(src, block):
        return copy(0, src, block, a + 1, b, c)

    def down(src, block):
        return copy(1, src, block, a - 1, b, c)

    def across(src, block):
        return copy(2, src, block, a, 1 - b, c)

    def over(src, block):
        return copy(3, src, block, a, b, 1 - c)

    has_up, has_down = a < line - 1, a > 0

    @pl.when(has_up)
    def _():
        up(x_ref, me).start()

    @pl.when(has_down)
    def _():
        down(x_ref, me).start()

    across(x_ref, me).start()
    over(x_ref, me).start()

    def arrived(block):
        over(out_ref.at[block], block).wait_recv()

    for k in range(1, line + 1):
        if k < line:

            @pl.when(a - k >= 0)
            def _(k=k):
                block = number(a - k, b, c)
                arrived(block)
                view = out_ref.at[block]

                @pl.when(has_up)
                def _():
                    up(view, block).start()

                across(view, block).start()
                over(view, block).start()

            @pl.when(a + k < line)
            def _(k=k):
                block = number(a + k, b, c)
                arrived(block)
                view = out_ref.at[block]

                @pl.when(has_down)
                def _():
                    down(view, block).start()

                across(view, block).start()
                over(view, block).start()

        j = k - 1
        for sign in (-1, 1) if j else (1,):

            @pl.when((a + sign * j >= 0) & (a + sign * j < line))
            def _(j=j, sign=sign):
                block = number(a + sign * j, 1 - b, c)
                arrived(block)
                over(out_ref.at[block], block).start()

    for other in range(n_dp // 2):
        block = other * 2 + 1 - c
        arrived(block)

    own.wait()
    for i in range(line):
        block = number(i, b, c)
        across(out_ref.at[block], block).wait_send()
        over(out_ref.at[block], block).wait_send()
        second = number(i, 1 - b, c)
        over(out_ref.at[second], second).wait_send()

        @pl.when(has_up & (i <= a))
        def _(block=block):
            up(out_ref.at[block], block).wait_send()

        @pl.when(has_down & (i >= a))
        def _(block=block):
            down(out_ref.at[block], block).wait_send()


def gathered(x, n_dp, collective_id):
    return pl.pallas_call(
        functools.partial(gather_kernel, n_dp),
        out_shape=jax.ShapeDtypeStruct((n_dp, *x.shape), x.dtype),
        in_specs=[pl.BlockSpec(memory_space=pltpu.VMEM)],
        out_specs=pl.BlockSpec(memory_space=pl.ANY),
        scratch_shapes=[
            pltpu.SemaphoreType.DMA,
            pltpu.SemaphoreType.DMA((4, n_dp)),
            pltpu.SemaphoreType.DMA((n_dp,)),
        ],
        compiler_params=pltpu.CompilerParams(
            collective_id=collective_id, has_side_effects=True
        ),
        cost_estimate=pl.CostEstimate(
            flops=0, bytes_accessed=150_000_000, transcendentals=0
        ),
    )(x)


def scatter_steps(n_dp, place, produce, core_source, out_ref, from_core, from_pair, up_buf,
                  down_buf, pair_out, core_send, core_recv, pair_send, pair_recv, up_send,
                  up_recv, down_send, down_recv):
    line = n_dp // 4
    a, b, c, seq = place
    enter(line, a, b, c, seq)

    def core_copy(block):
        half = block // 2
        return pltpu.make_async_remote_copy(
            src_ref=core_source(block),
            dst_ref=from_core.at[half],
            send_sem=core_send.at[half],
            recv_sem=core_recv.at[half],
            device_id=(number(a, b, 1 - c), seq),
            device_id_type=MESH,
        )

    def pair_copy(to):
        return pltpu.make_async_remote_copy(
            src_ref=pair_out.at[to],
            dst_ref=from_pair.at[to],
            send_sem=pair_send.at[to],
            recv_sem=pair_recv.at[to],
            device_id=(number(a, 1 - b, c), seq),
            device_id_type=MESH,
        )

    def up_copy(to):
        return pltpu.make_async_remote_copy(
            src_ref=up_buf.at[to],
            dst_ref=up_buf.at[to],
            send_sem=up_send.at[to],
            recv_sem=up_recv.at[to],
            device_id=(number(a + 1, b, c), seq),
            device_id_type=MESH,
        )

    def down_copy(to):
        return pltpu.make_async_remote_copy(
            src_ref=down_buf.at[to],
            dst_ref=down_buf.at[to],
            send_sem=down_send.at[to],
            recv_sem=down_recv.at[to],
            device_id=(number(a - 1, b, c), seq),
            device_id_type=MESH,
        )

    def each_target(act):
        for k in range(line - 1, 0, -1):

            @pl.when(a + k < line)
            def _(k=k):
                act(a + k, 1)

            @pl.when(a - k >= 0)
            def _(k=k):
                act(a - k, -1)

        act(a, 0)

    def send_core(block):
        produce(block, None, core_source(block))
        core_copy(block).start()

    each_target(lambda to, way: send_core(number(to, 1 - b, 1 - c)))
    each_target(lambda to, way: send_core(number(to, b, 1 - c)))

    def send_pair(to, way):
        block = number(to, 1 - b, c)
        core_copy(block).wait_recv()
        produce(block, [from_core.at[block // 2]], pair_out.at[to])
        pair_copy(to).start()

    each_target(send_pair)

    def line_sum(to, more, dst):
        block = number(to, b, c)
        produce(block, [from_core.at[block // 2], from_pair.at[to], *more], dst)

    def send_line(to, way):
        core_copy(number(to, b, c)).wait_recv()
        pair_copy(to).wait_recv()
        if way:
            buf, copy = (up_buf, up_copy) if way == 1 else (down_buf, down_copy)
            at_end = (a == 0) if way == 1 else (a == line - 1)

            @pl.when(at_end)
            def _():
                line_sum(to, [], buf.at[to])

            @pl.when(jnp.logical_not(at_end))
            def _():
                copy(to).wait_recv()
                line_sum(to, [buf.at[to]], buf.at[to])

            copy(to).start()
        else:
            line_sum(to, [], out_ref)
            for copy, buf, there in (
                (up_copy, up_buf, a > 0),
                (down_copy, down_buf, a < line - 1),
            ):

                @pl.when(there)
                def _(copy=copy, buf=buf):
                    copy(to).wait_recv()
                    add_rows(out_ref, buf.at[to])

    each_target(send_line)

    for i in range(n_dp // 2):
        core_copy(i * 2 + 1 - c).wait_send()
    for i in range(line):
        pair_copy(i).wait_send()

        @pl.when(i > a)
        def _(i=i):
            up_copy(i).wait_send()

        @pl.when(i < a)
        def _(i=i):
            down_copy(i).wait_send()


def row_tiles(rows):
    return 16 if rows % 16 == 0 else rows


def add_rows(out_ref, term):
    tile = row_tiles(out_ref.shape[0])

    def step(i, _):
        at = pl.ds(pl.multiple_of(i * tile, tile), tile)
        out_ref[at, :] += term[at, :].astype(jnp.float32)
        return 0

    lax.fori_loop(0, out_ref.shape[0] // tile, step, 0)


def scatter_kernel(n_dp, p_ref, out_ref, *scratch):
    def produce(block, terms, dst):
        if terms is None:
            return
        tile = row_tiles(p_ref.shape[1])

        def step(i, _):
            at = pl.ds(pl.multiple_of(i * tile, tile), tile)
            total = p_ref[block, at, :].astype(jnp.float32)
            for term in terms:
                total += term[at, :].astype(jnp.float32)
            dst[at, :] = total.astype(dst.dtype)
            return 0

        lax.fori_loop(0, p_ref.shape[1] // tile, step, 0)

    scatter_steps(n_dp, place_of(), produce, lambda block: p_ref.at[block], out_ref, *scratch)


def product_kernel(n_dp, left_a, right_a, left_b, right_b, extra, out_ref, core_out, *scratch):
    cols_a, cols_b = right_a.shape[1], right_b.shape[1]

    def produce(block, terms, dst):
        def part(left, right, first, wide):
            def step(i, _):
                inner = pl.ds(pl.multiple_of(i * wide, wide), wide)
                outer = pl.ds(pl.multiple_of(first + i * wide, 128), wide)
                total = jnp.dot(
                    left[block], right[:, inner], preferred_element_type=jnp.float32
                )
                for term in terms or []:
                    total += term[:, outer].astype(jnp.float32)
                dst[:, outer] = total.astype(dst.dtype)
                return 0

            lax.fori_loop(0, right.shape[1] // wide, step, 0)

        part(left_a, right_a, 0, 256)
        part(left_b, right_b, cols_a, 256)
        last = pl.ds(cols_a + cols_b, extra.shape[2])
        total = extra[block].astype(jnp.float32)
        for term in terms or []:
            total += term[:, last].astype(jnp.float32)
        dst[:, last] = total.astype(dst.dtype)

    scatter_steps(
        n_dp, place_of(), produce, lambda block: core_out.at[block // 2], out_ref, *scratch
    )


def scatter_scratch(n_dp, rows, cols, dtype):
    line = n_dp // 4
    return (
        [pltpu.VMEM((n_dp // 2, rows, cols), dtype)]
        + [pltpu.VMEM((line, rows, cols), dtype)] * 4
        + [pltpu.SemaphoreType.DMA((n_dp // 2,))] * 2
        + [pltpu.SemaphoreType.DMA((line,))] * 6
    )


def scattered_products(left_a, right_a, left_b, right_b, extra, collective_id):
    n_dp, rows, _ = left_a.shape
    cols = right_a.shape[1] + right_b.shape[1] + extra.shape[2]
    return pl.pallas_call(
        functools.partial(product_kernel, n_dp),
        out_shape=jax.ShapeDtypeStruct((rows, cols), jnp.float32),
        in_specs=[pl.BlockSpec(memory_space=pltpu.VMEM)] * 5,
        out_specs=pl.BlockSpec(memory_space=pltpu.VMEM),
        scratch_shapes=[pltpu.VMEM((n_dp // 2, rows, cols), jnp.bfloat16)]
        + scatter_scratch(n_dp, rows, cols, jnp.bfloat16),
        compiler_params=pltpu.CompilerParams(
            collective_id=collective_id, has_side_effects=True
        ),
        cost_estimate=pl.CostEstimate(
            flops=0, bytes_accessed=200_000_000, transcendentals=0
        ),
    )(left_a, right_a, left_b, right_b, extra)


def scattered(parts, collective_id):
    n_dp, rows, cols = parts.shape
    held = n_dp * (1 + 1 / 2 + 1) * rows * cols * 2
    pieces = 1
    while held > pieces * 50 * 2**20 or cols % (128 * pieces):
        pieces += 1
    width = cols // pieces
    return jnp.concatenate(
        [
            scattered_piece(parts[:, :, i * width : (i + 1) * width], collective_id)
            for i in range(pieces)
        ],
        axis=1,
    )


def scattered_piece(parts, collective_id):
    n_dp, rows, cols = parts.shape
    return pl.pallas_call(
        functools.partial(scatter_kernel, n_dp),
        out_shape=jax.ShapeDtypeStruct((rows, cols), jnp.float32),
        in_specs=[pl.BlockSpec(memory_space=pltpu.VMEM)],
        out_specs=pl.BlockSpec(memory_space=pltpu.VMEM),
        scratch_shapes=scatter_scratch(n_dp, rows, cols, parts.dtype),
        compiler_params=pltpu.CompilerParams(
            collective_id=collective_id, has_side_effects=True
        ),
        cost_estimate=pl.CostEstimate(
            flops=0, bytes_accessed=150_000_000, transcendentals=0
        ),
    )(parts)


def mine_and_other(halves, seq_index):
    first = seq_index == 0
    return (
        jnp.where(first, halves[0], halves[1]),
        jnp.where(first, halves[1], halves[0]),
    )


def in_order(own, other, seq_index):
    first = seq_index == 0
    return jnp.where(first, own, other), jnp.where(first, other, own)


def column_halves(weight):
    q_cols, k_cols = HEADS * HEAD_DIM, KV_HEADS * HEAD_DIM
    starts = (0, q_cols, q_cols + k_cols, q_cols + 2 * k_cols)
    sizes = (q_cols // 2, k_cols // 2, k_cols // 2, q_cols // 2)
    return [
        jnp.concatenate(
            [weight[:, s + h * n : s + (h + 1) * n] for s, n in zip(starts, sizes)], axis=1
        )
        for h in range(2)
    ]


def layer(tokens, doc_lengths, attn_weight, ffn_weight, gains, out_grad):
    tok_rows = tokens.shape[0]
    n_dp = lax.axis_size("dp")
    heads, kv_heads = HEADS // 2, KV_HEADS // 2
    q_cols = heads * HEAD_DIM
    k_cols = kv_heads * HEAD_DIM
    proj_cols = q_cols + 2 * k_cols
    half_cols = proj_cols + q_cols
    group_size = HEADS // KV_HEADS
    query_scale = HEAD_DIM ** (-0.5)
    bf16 = jnp.bfloat16
    seq_index = lax.axis_index("seq")
    weight_rows = attn_weight.shape[0]

    run = jnp.arange(tok_rows, dtype=jnp.int32)
    places = jnp.concatenate([seq_index * tok_rows + run, (1 - seq_index) * tok_rows + run])
    docs, pos = doc_layout(doc_lengths[0], places)
    allowed = key_mask(places, docs, places, docs)

    gain_cols = jnp.pad(gains, ((0, 0), (0, 124)))
    my_cols, other_cols = mine_and_other(column_halves(attn_weight), seq_index)
    my_cols = jnp.concatenate([my_cols, gain_cols], axis=1)
    other_cols = jnp.concatenate([other_cols, gain_cols], axis=1)
    partner_cols = swapped(other_cols)
    other_tokens = swapped(tokens)
    ffn_own, partner_cols = lax.optimization_barrier((ffn_weight, partner_cols))
    ffn_other = swapped(ffn_own)
    block = jnp.concatenate(in_order(my_cols, partner_cols, seq_index), axis=0)
    attn_full = gathered(block, n_dp, 0).reshape(-1, half_cols + 128)
    gain_vals = attn_full[:, half_cols : half_cols + 4].astype(jnp.float32).T
    attn_weights = attn_full[:, :proj_cols]
    out_weights = attn_full[:, proj_cols:half_cols]

    pack_tokens = jnp.concatenate([tokens, other_tokens]).astype(jnp.float32)
    tokens_f = tokens.astype(jnp.float32)
    attn_in = rms_norm(pack_tokens, gain_vals[0]).astype(bf16)
    projected = jnp.dot(attn_in, attn_weights, preferred_element_type=jnp.float32)
    pack = 2 * tok_rows
    queries = (
        rotate(projected[:, :q_cols].reshape(pack, heads, HEAD_DIM), pos) * query_scale
    ).astype(bf16)
    queries = queries.reshape(pack, kv_heads, group_size, HEAD_DIM)
    keys = rotate(
        projected[:, q_cols : q_cols + k_cols].reshape(pack, kv_heads, HEAD_DIM), pos
    ).astype(bf16)
    values = projected[:, q_cols + k_cols :].reshape(pack, kv_heads, HEAD_DIM).astype(bf16)
    scores, capped = attn_scores(queries, keys, allowed)
    row_max = jnp.max(capped, axis=-1, keepdims=True)
    exp_terms = jnp.exp(capped - row_max)
    row_total = jnp.sum(exp_terms, axis=-1, keepdims=True)
    log_total = row_max + jnp.log(row_total)
    attn_probs = (exp_terms / row_total).astype(bf16)
    mixed_heads = jnp.einsum(
        "kgqp,pkd->qkgd", attn_probs, values, preferred_element_type=jnp.float32
    )
    mixed_heads = mixed_heads.reshape(pack, q_cols).astype(bf16)
    attn_part_out = contract_cols(mixed_heads, out_weights)
    attn_out = attn_part_out[:tok_rows] + swapped(attn_part_out[tok_rows:].astype(bf16)).astype(
        jnp.float32
    )
    middle = tokens_f + rms_norm(attn_out, gain_vals[1])
    ffn_input = rms_norm(middle, gain_vals[2]).astype(bf16)

    unit_weights = jnp.concatenate([ffn_own, ffn_other], axis=0)
    unit_count = unit_weights.shape[0]
    gate_weights = unit_weights[:, :D]
    up_weights = unit_weights[:, D : 2 * D]
    down_weights = unit_weights[:, 2 * D :]
    ffn_all = gathered(ffn_input, n_dp, 1).reshape(-1, D)
    gate = contract_cols(ffn_all, gate_weights)
    up = contract_cols(ffn_all, up_weights)
    hidden = gated_gelu(gate, up).astype(bf16)
    ffn_parts = jnp.dot(hidden, down_weights, preferred_element_type=jnp.float32).astype(bf16)
    ffn_out = scattered(ffn_parts.reshape(n_dp, tok_rows, D), 2)
    out_gain = gain_vals[3]
    block_out = (middle + rms_norm(ffn_out, out_gain)).astype(bf16)
    cotangent = out_grad.astype(jnp.float32)
    d_ffn_f, d_gain_out = norm_back(ffn_out, out_gain, cotangent)
    d_ffn_all = gathered(d_ffn_f.astype(bf16), n_dp, 1).reshape(-1, D)
    d_hidden = contract_cols(d_ffn_all, down_weights)
    d_gate, d_up = jax.vjp(gated_gelu, gate, up)[1](d_hidden)
    d_gate, d_up = d_gate.astype(bf16), d_up.astype(bf16)
    d_parts = (
        jnp.dot(d_gate, gate_weights, preferred_element_type=jnp.float32)
        + jnp.dot(d_up, up_weights, preferred_element_type=jnp.float32)
    ).astype(bf16)
    d_ffn_input = scattered(d_parts.reshape(n_dp, tok_rows, D), 2)

    own_units = unit_count // 2
    weight_sum = [
        contract_rows(d_gate, ffn_all),
        contract_rows(d_up, ffn_all),
        contract_rows(hidden, d_ffn_all),
    ]
    sent = jnp.concatenate([w[own_units:].astype(bf16) for w in weight_sum], axis=1)
    kept = jnp.concatenate([w[:own_units] for w in weight_sum], axis=1)
    grad_other = swapped(sent)
    ffn_weight_grad = kept + grad_other.astype(jnp.float32)

    d_middle_add, d_gain_ffn = norm_back(middle, gain_vals[2], d_ffn_input)
    d_middle = cotangent + d_middle_add
    d_attn_f, d_gain_post = norm_back(attn_out, gain_vals[1], d_middle)
    d_attn_own = d_attn_f.astype(bf16)
    d_attn_other = swapped(d_attn_own)
    d_attn = jnp.concatenate([d_attn_own, d_attn_other])
    d_mixed = jnp.dot(d_attn, out_weights, preferred_element_type=jnp.float32).astype(bf16)
    d_mixed = d_mixed.reshape(pack, kv_heads, group_size, HEAD_DIM)
    attn_p = jnp.exp(capped - log_total)
    d_probs = jnp.einsum("qkgd,pkd->kgqp", d_mixed, values, preferred_element_type=jnp.float32)
    d_values = jnp.einsum(
        "kgqp,qkgd->pkd", attn_probs, d_mixed, preferred_element_type=jnp.float32
    )
    d_capped = attn_p * (d_probs - jnp.sum(attn_p * d_probs, axis=-1, keepdims=True))
    tanh_part = jnp.tanh(scores / soft_cap)
    d_scores = (d_capped * (1.0 - tanh_part * tanh_part)).astype(bf16)
    d_queries = jnp.einsum("kgqp,pkd->qkgd", d_scores, keys, preferred_element_type=jnp.float32)
    d_keys = jnp.einsum("kgqp,qkgd->pkd", d_scores, queries, preferred_element_type=jnp.float32)
    d_query_raw = rotate(d_queries.reshape(pack, heads, HEAD_DIM) * query_scale, -pos)
    d_key_raw = rotate(d_keys, -pos)
    d_projected = jnp.concatenate(
        [
            d_query_raw.reshape(pack, q_cols),
            d_key_raw.reshape(pack, k_cols),
            d_values.reshape(pack, k_cols),
        ],
        axis=1,
    ).astype(bf16)
    d_attn_in_part = contract_cols(d_projected, attn_weights)
    d_attn_in_other = swapped(d_attn_in_part[tok_rows:].astype(bf16))
    d_attn_in = d_attn_in_part[:tok_rows] + d_attn_in_other.astype(jnp.float32)
    normed = pack_tokens * lax.rsqrt(
        jnp.mean(pack_tokens * pack_tokens, axis=-1, keepdims=True) + eps_norm
    )
    d_gain_in = jnp.sum(d_attn_in_part * normed, axis=0)

    gain_part = jnp.stack([d_gain_in, d_gain_post, d_gain_ffn, d_gain_out], axis=1)
    block_rows = (n_dp, 2 * weight_rows)
    attn_sum = scattered_products(
        attn_in.T.reshape(*block_rows, pack),
        d_projected,
        d_attn.T.reshape(*block_rows, pack),
        mixed_heads,
        jnp.pad(gain_part.astype(bf16), ((0, 0), (0, 124))).reshape(*block_rows, 128),
        3,
    )
    d_tokens_add = norm_back(tokens_f, gain_vals[0], d_attn_in)[0]
    tokens_grad = d_middle + d_tokens_add
    mine, others = mine_and_other(
        (attn_sum[:weight_rows], attn_sum[weight_rows:]), seq_index
    )
    partner = swapped(others.astype(bf16)).astype(jnp.float32)
    gains_grad = mine[:, half_cols : half_cols + 4] + partner[:, half_cols : half_cols + 4]
    first, second = in_order(mine, partner, seq_index)
    cuts = ((0, q_cols), (q_cols, q_cols + k_cols), (q_cols + k_cols, proj_cols),
            (proj_cols, half_cols))
    attn_weight_grad = jnp.concatenate(
        [half[:, lo:hi] for lo, hi in cuts for half in (first, second)], axis=1
    )
    return (block_out, tokens_grad, attn_weight_grad, ffn_weight_grad, gains_grad)


def solution(mesh):
    return jax.shard_map(
        layer,
        mesh=mesh,
        in_specs=(
            P(("dp", "seq"), None),
            P("dp", None),
            P(("dp", "seq"), None),
            P(("dp", "seq"), None),
            P(("dp", "seq"), None),
            P(("dp", "seq"), None),
        ),
        out_specs=(
            P(("dp", "seq"), None),
            P(("dp", "seq"), None),
            P(("dp", "seq"), None),
            P(("dp", "seq"), None),
            P(("dp", "seq"), None),
        ),
        check_vma=False,
    )
```

```python
import functools
import math

import jax
import jax.numpy as jnp
from jax import lax
from jax.experimental import pallas as pl
from jax.experimental.pallas import tpu as pltpu
from jax.sharding import PartitionSpec as P

D = 2304
HEADS = 8
KV_HEADS = 4
HEAD_DIM = 256
WINDOW = 128


soft_cap = 50.0
eps_norm = 1e-06
rope_base = 10000.0
gelu_coef = math.sqrt(2.0 / math.pi)


MESH = pl.DeviceIdType.MESH


def gelu_tanh(value):
    return 0.5 * value * (1.0 + jnp.tanh(gelu_coef * (value + 0.044715 * value * value * value)))


def gated_gelu(gate_pre, up_pre):
    return gelu_tanh(gate_pre) * up_pre


def rms_norm(value, gain_vec):
    return value * lax.rsqrt(jnp.mean(value * value, axis=-1, keepdims=True) + eps_norm) * gain_vec


def norm_back(value, gain_vec, incoming):
    return jax.vjp(rms_norm, value, gain_vec)[1](incoming)


def doc_layout(lengths, places):
    doc_ends = jnp.cumsum(lengths, dtype=jnp.int32)
    starts = doc_ends - lengths
    doc_ids = jnp.sum(
        (places[:, None] >= doc_ends[None, :]).astype(jnp.int32), axis=1, dtype=jnp.int32
    )
    onehot = doc_ids[:, None] == jnp.arange(lengths.shape[0], dtype=jnp.int32)[None, :]
    doc_first = jnp.sum(jnp.where(onehot, starts[None, :], 0), axis=1, dtype=jnp.int32)
    return (doc_ids, places - doc_first)


def rotate(value, doc_pos):
    half_dim = value.shape[-1] // 2
    frequency = rope_base ** (-2.0 * jnp.arange(half_dim, dtype=jnp.float32) / value.shape[-1])
    angles = doc_pos.astype(jnp.float32)[:, None] * frequency[None, :]
    cosine = jnp.cos(angles)[:, None, :]
    sine_part = jnp.sin(angles)[:, None, :]
    first_half = value[..., :half_dim]
    second_half = value[..., half_dim:]
    return jnp.concatenate(
        [
            first_half * cosine - second_half * sine_part,
            second_half * cosine + first_half * sine_part,
        ],
        axis=-1,
    )


def contract_rows(left_side, right_side):
    return lax.dot_general(
        left_side, right_side, (((0,), (0,)), ((), ())), preferred_element_type=jnp.float32
    )


def contract_cols(left_side, right_side):
    return lax.dot_general(
        left_side, right_side, (((1,), (1,)), ((), ())), preferred_element_type=jnp.float32
    )


def key_mask(query_places, query_docs, key_places, key_docs):
    return (
        (key_places[None, :] >= 0)
        & (query_docs[:, None] == key_docs[None, :])
        & (key_places[None, :] <= query_places[:, None])
        & (query_places[:, None] - key_places[None, :] < WINDOW)
    )


def attn_scores(queries, all_keys, allowed):
    scores = jnp.einsum("qkgd,pkd->kgqp", queries, all_keys, preferred_element_type=jnp.float32)
    capped = jnp.where(allowed[None, None], soft_cap * jnp.tanh(scores / soft_cap), -1e30)
    return (scores, capped)


def swapped(x):
    return lax.ppermute(x, "seq", [(0, 1), (1, 0)])


def place_of():
    dp = lax.axis_index("dp")
    seq = lax.axis_index("seq")
    a, b, c = dp // 4, lax.rem(dp // 2, 2), lax.rem(dp, 2)
    return a, b, c, seq


def number(a, b, c):
    return (a * 2 + b) * 2 + c


def enter(line, a, b, c, seq):
    barrier = pltpu.get_barrier_semaphore()

    def tell(a2, b2, c2):
        pl.semaphore_signal(
            barrier, inc=1, device_id=(number(a2, b2, c2), seq), device_id_type=MESH
        )

    tell(a, b, 1 - c)
    tell(a, 1 - b, c)

    @pl.when(a > 0)
    def _():
        tell(a - 1, b, c)

    @pl.when(a < line - 1)
    def _():
        tell(a + 1, b, c)

    peers = 2 + jnp.minimum(a, 1) + jnp.minimum(line - 1 - a, 1)
    pl.semaphore_wait(barrier, peers)


def gather_kernel(n_dp, x_ref, out_ref, own_sem, send_sem, recv_sem):
    line = n_dp // 4
    a, b, c, seq = place_of()
    me = number(a, b, c)
    own = pltpu.make_async_copy(x_ref, out_ref.at[me], own_sem)
    own.start()
    enter(line, a, b, c, seq)

    def copy(way, src, block, a2, b2, c2):
        return pltpu.make_async_remote_copy(
            src_ref=src,
            dst_ref=out_ref.at[block],
            send_sem=send_sem.at[way, block],
            recv_sem=recv_sem.at[block],
            device_id=(number(a2, b2, c2), seq),
            device_id_type=MESH,
        )

    def up(src, block):
        return copy(0, src, block, a + 1, b, c)

    def down(src, block):
        return copy(1, src, block, a - 1, b, c)

    def across(src, block):
        return copy(2, src, block, a, 1 - b, c)

    def over(src, block):
        return copy(3, src, block, a, b, 1 - c)

    has_up, has_down = a < line - 1, a > 0

    @pl.when(has_up)
    def _():
        up(x_ref, me).start()

    @pl.when(has_down)
    def _():
        down(x_ref, me).start()

    across(x_ref, me).start()
    over(x_ref, me).start()

    def arrived(block):
        over(out_ref.at[block], block).wait_recv()

    for k in range(1, line + 1):
        if k < line:

            @pl.when(a - k >= 0)
            def _(k=k):
                block = number(a - k, b, c)
                arrived(block)
                view = out_ref.at[block]

                @pl.when(has_up)
                def _():
                    up(view, block).start()

                across(view, block).start()
                over(view, block).start()

            @pl.when(a + k < line)
            def _(k=k):
                block = number(a + k, b, c)
                arrived(block)
                view = out_ref.at[block]

                @pl.when(has_down)
                def _():
                    down(view, block).start()

                across(view, block).start()
                over(view, block).start()

        j = k - 1
        for sign in (-1, 1) if j else (1,):

            @pl.when((a + sign * j >= 0) & (a + sign * j < line))
            def _(j=j, sign=sign):
                block = number(a + sign * j, 1 - b, c)
                arrived(block)
                over(out_ref.at[block], block).start()

    for other in range(n_dp // 2):
        block = other * 2 + 1 - c
        arrived(block)

    own.wait()
    for i in range(line):
        block = number(i, b, c)
        across(out_ref.at[block], block).wait_send()
        over(out_ref.at[block], block).wait_send()
        second = number(i, 1 - b, c)
        over(out_ref.at[second], second).wait_send()

        @pl.when(has_up & (i <= a))
        def _(block=block):
            up(out_ref.at[block], block).wait_send()

        @pl.when(has_down & (i >= a))
        def _(block=block):
            down(out_ref.at[block], block).wait_send()


def gathered(x, n_dp, collective_id):
    return pl.pallas_call(
        functools.partial(gather_kernel, n_dp),
        out_shape=jax.ShapeDtypeStruct((n_dp, *x.shape), x.dtype),
        in_specs=[pl.BlockSpec(memory_space=pltpu.VMEM)],
        out_specs=pl.BlockSpec(memory_space=pl.ANY),
        scratch_shapes=[
            pltpu.SemaphoreType.DMA,
            pltpu.SemaphoreType.DMA((4, n_dp)),
            pltpu.SemaphoreType.DMA((n_dp,)),
        ],
        compiler_params=pltpu.CompilerParams(
            collective_id=collective_id, has_side_effects=True
        ),
        cost_estimate=pl.CostEstimate(
            flops=0, bytes_accessed=150_000_000, transcendentals=0
        ),
    )(x)


def scatter_steps(n_dp, place, prepare, produce, core_source, out_ref, from_core, from_pair, up_buf,
                  down_buf, pair_out, core_send, core_recv, pair_send, pair_recv, up_send,
                  up_recv, down_send, down_recv):
    line = n_dp // 4
    a, b, c, seq = place
    enter(line, a, b, c, seq)

    def core_copy(block):
        half = block // 2
        return pltpu.make_async_remote_copy(
            src_ref=core_source(block),
            dst_ref=from_core.at[half],
            send_sem=core_send.at[half],
            recv_sem=core_recv.at[half],
            device_id=(number(a, b, 1 - c), seq),
            device_id_type=MESH,
        )

    def pair_copy(to):
        return pltpu.make_async_remote_copy(
            src_ref=pair_out.at[to],
            dst_ref=from_pair.at[to],
            send_sem=pair_send.at[to],
            recv_sem=pair_recv.at[to],
            device_id=(number(a, 1 - b, c), seq),
            device_id_type=MESH,
        )

    def up_copy(to):
        return pltpu.make_async_remote_copy(
            src_ref=up_buf.at[to],
            dst_ref=up_buf.at[to],
            send_sem=up_send.at[to],
            recv_sem=up_recv.at[to],
            device_id=(number(a + 1, b, c), seq),
            device_id_type=MESH,
        )

    def down_copy(to):
        return pltpu.make_async_remote_copy(
            src_ref=down_buf.at[to],
            dst_ref=down_buf.at[to],
            send_sem=down_send.at[to],
            recv_sem=down_recv.at[to],
            device_id=(number(a - 1, b, c), seq),
            device_id_type=MESH,
        )

    def each_target(act):
        for k in range(line - 1, 0, -1):

            @pl.when(a + k < line)
            def _(k=k):
                act(a + k, 1)

            @pl.when(a - k >= 0)
            def _(k=k):
                act(a - k, -1)

        act(a, 0)

    def send_core(block):
        produce(block, None, core_source(block))
        core_copy(block).start()

    prepare(1 - b, 1 - c)
    each_target(lambda to, way: send_core(number(to, 1 - b, 1 - c)))
    prepare(1 - b, c)

    def send_pair(to, way):
        block = number(to, 1 - b, c)
        core_copy(block).wait_recv()
        produce(block, [from_core.at[block // 2]], pair_out.at[to])
        pair_copy(to).start()

    each_target(send_pair)
    prepare(b, 1 - c)
    each_target(lambda to, way: send_core(number(to, b, 1 - c)))
    prepare(b, c)

    def line_sum(to, more, dst):
        block = number(to, b, c)
        produce(block, [from_core.at[block // 2], from_pair.at[to], *more], dst)

    def send_line(to, way):
        core_copy(number(to, b, c)).wait_recv()
        pair_copy(to).wait_recv()
        if way:
            buf, copy = (up_buf, up_copy) if way == 1 else (down_buf, down_copy)
            at_end = (a == 0) if way == 1 else (a == line - 1)

            @pl.when(at_end)
            def _():
                line_sum(to, [], buf.at[to])

            @pl.when(jnp.logical_not(at_end))
            def _():
                copy(to).wait_recv()
                line_sum(to, [buf.at[to]], buf.at[to])

            copy(to).start()
        else:
            line_sum(to, [], out_ref)
            for copy, buf, there in (
                (up_copy, up_buf, a > 0),
                (down_copy, down_buf, a < line - 1),
            ):

                @pl.when(there)
                def _(copy=copy, buf=buf):
                    copy(to).wait_recv()
                    add_rows(out_ref, buf.at[to])

    each_target(send_line)

    for i in range(n_dp // 2):
        core_copy(i * 2 + 1 - c).wait_send()
    for i in range(line):
        pair_copy(i).wait_send()

        @pl.when(i > a)
        def _(i=i):
            up_copy(i).wait_send()

        @pl.when(i < a)
        def _(i=i):
            down_copy(i).wait_send()


def row_tiles(rows):
    return 16 if rows % 16 == 0 else rows


def add_rows(out_ref, term):
    tile = row_tiles(out_ref.shape[0])

    def step(i, _):
        at = pl.ds(pl.multiple_of(i * tile, tile), tile)
        out_ref[at, :] += term[at, :].astype(jnp.float32)
        return 0

    lax.fori_loop(0, out_ref.shape[0] // tile, step, 0)


def dots_kernel(n_dp, n_terms, *refs):
    lefts, rights = refs[:n_terms], refs[n_terms : 2 * n_terms]
    out_ref, parts, *scratch = refs[2 * n_terms :]
    _, rows, cols = parts.shape
    f32 = jnp.float32

    def prepare(b, c):
        for first in range(0, n_dp // 4, 4):
            blocks = [number(first + i, b, c) for i in range(4)]

            def step(j, _):
                at = pl.ds(pl.multiple_of(j * 256, 256), 256)
                total = jnp.zeros((4 * rows, 256), f32)
                for left, right in zip(lefts, rights):
                    stacked = jnp.concatenate([left[k] for k in blocks], axis=0)
                    total += jnp.dot(stacked, right[:, at], preferred_element_type=f32)
                for i, k in enumerate(blocks):
                    parts[k, :, at] = total[i * rows : (i + 1) * rows].astype(parts.dtype)
                return 0

            lax.fori_loop(0, cols // 256, step, 0)

    def produce(block, terms, dst):
        if terms is None:
            return
        tile = row_tiles(rows)

        def step(i, _):
            at = pl.ds(pl.multiple_of(i * tile, tile), tile)
            total = parts[block, at, :].astype(f32)
            for term in terms:
                total += term[at, :].astype(f32)
            dst[at, :] = total.astype(dst.dtype)
            return 0

        lax.fori_loop(0, rows // tile, step, 0)

    scatter_steps(
        n_dp, place_of(), prepare, produce, lambda block: parts.at[block], out_ref, *scratch
    )


def product_kernel(n_dp, left_a, right_a, left_b, right_b, extra, out_ref, core_out, *scratch):
    cols_a, cols_b = right_a.shape[1], right_b.shape[1]

    def produce(block, terms, dst):
        def part(left, right, first, wide):
            def step(i, _):
                inner = pl.ds(pl.multiple_of(i * wide, wide), wide)
                outer = pl.ds(pl.multiple_of(first + i * wide, 128), wide)
                total = jnp.dot(
                    left[block], right[:, inner], preferred_element_type=jnp.float32
                )
                for term in terms or []:
                    total += term[:, outer].astype(jnp.float32)
                dst[:, outer] = total.astype(dst.dtype)
                return 0

            lax.fori_loop(0, right.shape[1] // wide, step, 0)

        part(left_a, right_a, 0, 256)
        part(left_b, right_b, cols_a, 256)
        last = pl.ds(cols_a + cols_b, extra.shape[2])
        total = extra[block].astype(jnp.float32)
        for term in terms or []:
            total += term[:, last].astype(jnp.float32)
        dst[:, last] = total.astype(dst.dtype)

    scatter_steps(
        n_dp,
        place_of(),
        lambda b, c: None,
        produce,
        lambda block: core_out.at[block // 2],
        out_ref,
        *scratch,
    )


def scatter_scratch(n_dp, rows, cols, dtype):
    line = n_dp // 4
    return (
        [pltpu.VMEM((n_dp // 2, rows, cols), dtype)]
        + [pltpu.VMEM((line, rows, cols), dtype)] * 4
        + [pltpu.SemaphoreType.DMA((n_dp // 2,))] * 2
        + [pltpu.SemaphoreType.DMA((line,))] * 6
    )


def scattered_products(left_a, right_a, left_b, right_b, extra, collective_id):
    n_dp, rows, _ = left_a.shape
    cols = right_a.shape[1] + right_b.shape[1] + extra.shape[2]
    return pl.pallas_call(
        functools.partial(product_kernel, n_dp),
        out_shape=jax.ShapeDtypeStruct((rows, cols), jnp.float32),
        in_specs=[pl.BlockSpec(memory_space=pltpu.VMEM)] * 5,
        out_specs=pl.BlockSpec(memory_space=pltpu.VMEM),
        scratch_shapes=[pltpu.VMEM((n_dp // 2, rows, cols), jnp.bfloat16)]
        + scatter_scratch(n_dp, rows, cols, jnp.bfloat16),
        compiler_params=pltpu.CompilerParams(
            collective_id=collective_id, has_side_effects=True
        ),
        cost_estimate=pl.CostEstimate(
            flops=0, bytes_accessed=200_000_000, transcendentals=0
        ),
    )(left_a, right_a, left_b, right_b, extra)


def scattered_dots(lefts, rights, collective_id):
    n_dp, rows, _ = lefts[0].shape
    cols = rights[0].shape[1]
    held = n_dp * (1 + 1 / 2 + 1) * rows * cols * 2
    pieces = 1
    while held > pieces * 36 * 2**20 or cols % (256 * pieces):
        pieces += 1
    width = cols // pieces
    return jnp.concatenate(
        [
            scattered_piece(
                lefts, [r[:, i * width : (i + 1) * width] for r in rights], collective_id
            )
            for i in range(pieces)
        ],
        axis=1,
    )


def scattered_piece(lefts, rights, collective_id):
    n_dp, rows, _ = lefts[0].shape
    cols = rights[0].shape[1]
    return pl.pallas_call(
        functools.partial(dots_kernel, n_dp, len(lefts)),
        out_shape=jax.ShapeDtypeStruct((rows, cols), jnp.float32),
        in_specs=[pl.BlockSpec(memory_space=pltpu.VMEM)] * (2 * len(lefts)),
        out_specs=pl.BlockSpec(memory_space=pltpu.VMEM),
        scratch_shapes=[pltpu.VMEM((n_dp, rows, cols), jnp.bfloat16)]
        + scatter_scratch(n_dp, rows, cols, jnp.bfloat16),
        compiler_params=pltpu.CompilerParams(
            collective_id=collective_id, has_side_effects=True
        ),
        cost_estimate=pl.CostEstimate(
            flops=0, bytes_accessed=150_000_000, transcendentals=0
        ),
    )(*lefts, *rights)


def mine_and_other(halves, seq_index):
    first = seq_index == 0
    return (
        jnp.where(first, halves[0], halves[1]),
        jnp.where(first, halves[1], halves[0]),
    )


def in_order(own, other, seq_index):
    first = seq_index == 0
    return jnp.where(first, own, other), jnp.where(first, other, own)


def column_halves(weight):
    q_cols, k_cols = HEADS * HEAD_DIM, KV_HEADS * HEAD_DIM
    starts = (0, q_cols, q_cols + k_cols, q_cols + 2 * k_cols)
    sizes = (q_cols // 2, k_cols // 2, k_cols // 2, q_cols // 2)
    return [
        jnp.concatenate(
            [weight[:, s + h * n : s + (h + 1) * n] for s, n in zip(starts, sizes)], axis=1
        )
        for h in range(2)
    ]


def layer(tokens, doc_lengths, attn_weight, ffn_weight, gains, out_grad):
    tok_rows = tokens.shape[0]
    n_dp = lax.axis_size("dp")
    heads, kv_heads = HEADS // 2, KV_HEADS // 2
    q_cols = heads * HEAD_DIM
    k_cols = kv_heads * HEAD_DIM
    proj_cols = q_cols + 2 * k_cols
    half_cols = proj_cols + q_cols
    group_size = HEADS // KV_HEADS
    query_scale = HEAD_DIM ** (-0.5)
    bf16 = jnp.bfloat16
    seq_index = lax.axis_index("seq")
    weight_rows = attn_weight.shape[0]

    run = jnp.arange(tok_rows, dtype=jnp.int32)
    places = jnp.concatenate([seq_index * tok_rows + run, (1 - seq_index) * tok_rows + run])
    docs, pos = doc_layout(doc_lengths[0], places)
    allowed = key_mask(places, docs, places, docs)

    gain_cols = jnp.pad(gains, ((0, 0), (0, 124)))
    my_cols, other_cols = mine_and_other(column_halves(attn_weight), seq_index)
    my_cols = jnp.concatenate([my_cols, gain_cols], axis=1)
    other_cols = jnp.concatenate([other_cols, gain_cols], axis=1)
    partner_cols = swapped(other_cols)
    other_tokens = swapped(tokens)
    ffn_own, partner_cols = lax.optimization_barrier((ffn_weight, partner_cols))
    ffn_other = swapped(ffn_own)
    block = jnp.concatenate(in_order(my_cols, partner_cols, seq_index), axis=0)
    attn_full = gathered(block, n_dp, 0).reshape(-1, half_cols + 128)
    gain_vals = attn_full[:, half_cols : half_cols + 4].astype(jnp.float32).T
    attn_weights = attn_full[:, :proj_cols]
    out_weights = attn_full[:, proj_cols:half_cols]

    pack_tokens = jnp.concatenate([tokens, other_tokens]).astype(jnp.float32)
    tokens_f = tokens.astype(jnp.float32)
    attn_in = rms_norm(pack_tokens, gain_vals[0]).astype(bf16)
    projected = jnp.dot(attn_in, attn_weights, preferred_element_type=jnp.float32)
    pack = 2 * tok_rows
    queries = (
        rotate(projected[:, :q_cols].reshape(pack, heads, HEAD_DIM), pos) * query_scale
    ).astype(bf16)
    queries = queries.reshape(pack, kv_heads, group_size, HEAD_DIM)
    keys = rotate(
        projected[:, q_cols : q_cols + k_cols].reshape(pack, kv_heads, HEAD_DIM), pos
    ).astype(bf16)
    values = projected[:, q_cols + k_cols :].reshape(pack, kv_heads, HEAD_DIM).astype(bf16)
    scores, capped = attn_scores(queries, keys, allowed)
    row_max = jnp.max(capped, axis=-1, keepdims=True)
    exp_terms = jnp.exp(capped - row_max)
    row_total = jnp.sum(exp_terms, axis=-1, keepdims=True)
    log_total = row_max + jnp.log(row_total)
    attn_probs = (exp_terms / row_total).astype(bf16)
    mixed_heads = jnp.einsum(
        "kgqp,pkd->qkgd", attn_probs, values, preferred_element_type=jnp.float32
    )
    mixed_heads = mixed_heads.reshape(pack, q_cols).astype(bf16)
    attn_part_out = contract_cols(mixed_heads, out_weights)
    attn_part_other = swapped(attn_part_out[tok_rows:].astype(bf16))
    attn_out = attn_part_out[:tok_rows] + attn_part_other.astype(jnp.float32)
    middle = tokens_f + rms_norm(attn_out, gain_vals[1])
    ffn_input = rms_norm(middle, gain_vals[2]).astype(bf16)

    gate_weights, up_weights, down_weights = [
        jnp.concatenate([ffn_own[:, k * D : (k + 1) * D], ffn_other[:, k * D : (k + 1) * D]])
        for k in range(3)
    ]
    unit_count = gate_weights.shape[0]
    ffn_all = gathered(ffn_input, n_dp, 1).reshape(-1, D)
    gate = contract_cols(ffn_all, gate_weights)
    up = contract_cols(ffn_all, up_weights)
    hidden = gated_gelu(gate, up).astype(bf16)
    ffn_out = scattered_dots([hidden.reshape(n_dp, tok_rows, -1)], [down_weights], 2)
    out_gain = gain_vals[3]
    block_out = (middle + rms_norm(ffn_out, out_gain)).astype(bf16)
    cotangent = out_grad.astype(jnp.float32)
    d_ffn_f, d_gain_out = norm_back(ffn_out, out_gain, cotangent)
    d_ffn_all = gathered(d_ffn_f.astype(bf16), n_dp, 1).reshape(-1, D)
    d_hidden = contract_cols(d_ffn_all, down_weights)
    d_gate, d_up = jax.vjp(gated_gelu, gate, up)[1](d_hidden)
    d_gate, d_up = d_gate.astype(bf16), d_up.astype(bf16)
    d_ffn_input = scattered_dots(
        [d_gate.reshape(n_dp, tok_rows, -1), d_up.reshape(n_dp, tok_rows, -1)],
        [gate_weights, up_weights],
        4,
    )

    own_units = unit_count // 2
    weight_sum = [
        contract_rows(d_gate, ffn_all),
        contract_rows(d_up, ffn_all),
        contract_rows(hidden, d_ffn_all),
    ]
    sent = jnp.concatenate([w[own_units:].astype(bf16) for w in weight_sum], axis=1)
    kept = jnp.concatenate([w[:own_units] for w in weight_sum], axis=1)
    grad_other = swapped(sent)
    ffn_weight_grad = kept + grad_other.astype(jnp.float32)

    d_middle_add, d_gain_ffn = norm_back(middle, gain_vals[2], d_ffn_input)
    d_middle = cotangent + d_middle_add
    d_attn_f, d_gain_post = norm_back(attn_out, gain_vals[1], d_middle)
    d_attn_own = d_attn_f.astype(bf16)
    d_attn_other = swapped(d_attn_own)
    d_attn = jnp.concatenate([d_attn_own, d_attn_other])
    d_mixed = jnp.dot(d_attn, out_weights, preferred_element_type=jnp.float32).astype(bf16)
    d_mixed = d_mixed.reshape(pack, kv_heads, group_size, HEAD_DIM)
    attn_p = jnp.exp(capped - log_total)
    d_probs = jnp.einsum("qkgd,pkd->kgqp", d_mixed, values, preferred_element_type=jnp.float32)
    d_values = jnp.einsum(
        "kgqp,qkgd->pkd", attn_probs, d_mixed, preferred_element_type=jnp.float32
    )
    d_capped = attn_p * (d_probs - jnp.sum(attn_p * d_probs, axis=-1, keepdims=True))
    tanh_part = jnp.tanh(scores / soft_cap)
    d_scores = (d_capped * (1.0 - tanh_part * tanh_part)).astype(bf16)
    d_queries = jnp.einsum("kgqp,pkd->qkgd", d_scores, keys, preferred_element_type=jnp.float32)
    d_keys = jnp.einsum("kgqp,qkgd->pkd", d_scores, queries, preferred_element_type=jnp.float32)
    d_query_raw = rotate(d_queries.reshape(pack, heads, HEAD_DIM) * query_scale, -pos)
    d_key_raw = rotate(d_keys, -pos)
    d_projected = jnp.concatenate(
        [
            d_query_raw.reshape(pack, q_cols),
            d_key_raw.reshape(pack, k_cols),
            d_values.reshape(pack, k_cols),
        ],
        axis=1,
    ).astype(bf16)
    d_attn_in_part = contract_cols(d_projected, attn_weights)
    d_attn_in_other = swapped(d_attn_in_part[tok_rows:].astype(bf16))
    d_attn_in = d_attn_in_part[:tok_rows] + d_attn_in_other.astype(jnp.float32)
    normed = pack_tokens * lax.rsqrt(
        jnp.mean(pack_tokens * pack_tokens, axis=-1, keepdims=True) + eps_norm
    )
    d_gain_in = jnp.sum(d_attn_in_part * normed, axis=0)

    gain_part = jnp.stack([d_gain_in, d_gain_post, d_gain_ffn, d_gain_out], axis=1)
    block_rows = (n_dp, 2 * weight_rows)
    attn_sum = scattered_products(
        attn_in.T.reshape(*block_rows, pack),
        d_projected,
        d_attn.T.reshape(*block_rows, pack),
        mixed_heads,
        jnp.pad(gain_part.astype(bf16), ((0, 0), (0, 124))).reshape(*block_rows, 128),
        3,
    )
    d_tokens_add = norm_back(tokens_f, gain_vals[0], d_attn_in)[0]
    tokens_grad = d_middle + d_tokens_add
    mine, others = mine_and_other(
        (attn_sum[:weight_rows], attn_sum[weight_rows:]), seq_index
    )
    partner = swapped(others.astype(bf16)).astype(jnp.float32)
    gains_grad = mine[:, half_cols : half_cols + 4] + partner[:, half_cols : half_cols + 4]
    first, second = in_order(mine, partner, seq_index)
    cuts = ((0, q_cols), (q_cols, q_cols + k_cols), (q_cols + k_cols, proj_cols),
            (proj_cols, half_cols))
    attn_weight_grad = jnp.concatenate(
        [half[:, lo:hi] for lo, hi in cuts for half in (first, second)], axis=1
    )
    return (block_out, tokens_grad, attn_weight_grad, ffn_weight_grad, gains_grad)


def solution(mesh):
    return jax.shard_map(
        layer,
        mesh=mesh,
        in_specs=(
            P(("dp", "seq"), None),
            P("dp", None),
            P(("dp", "seq"), None),
            P(("dp", "seq"), None),
            P(("dp", "seq"), None),
            P(("dp", "seq"), None),
        ),
        out_specs=(
            P(("dp", "seq"), None),
            P(("dp", "seq"), None),
            P(("dp", "seq"), None),
            P(("dp", "seq"), None),
            P(("dp", "seq"), None),
        ),
        check_vma=False,
    )
```

```python
import functools
import math

import jax
import jax.numpy as jnp
from jax import lax
from jax.experimental.layout import Layout, with_layout_constraint
from jax.experimental import pallas as pl
from jax.experimental.pallas import tpu as pltpu
from jax.sharding import PartitionSpec as P

D = 2304
HEADS = 8
KV_HEADS = 4
HEAD_DIM = 256
WINDOW = 128


soft_cap = 50.0
eps_norm = 1e-06
rope_base = 10000.0
gelu_coef = math.sqrt(2.0 / math.pi)


MESH = pl.DeviceIdType.MESH


def gelu_tanh(value):
    return 0.5 * value * (1.0 + jnp.tanh(gelu_coef * (value + 0.044715 * value * value * value)))


def gated_gelu(gate_pre, up_pre):
    return gelu_tanh(gate_pre) * up_pre


def rms_norm(value, gain_vec):
    return value * lax.rsqrt(jnp.mean(value * value, axis=-1, keepdims=True) + eps_norm) * gain_vec


def norm_back(value, gain_vec, incoming):
    return jax.vjp(rms_norm, value, gain_vec)[1](incoming)


def doc_layout(lengths, places):
    doc_ends = jnp.cumsum(lengths, dtype=jnp.int32)
    starts = doc_ends - lengths
    doc_ids = jnp.sum(
        (places[:, None] >= doc_ends[None, :]).astype(jnp.int32), axis=1, dtype=jnp.int32
    )
    onehot = doc_ids[:, None] == jnp.arange(lengths.shape[0], dtype=jnp.int32)[None, :]
    doc_first = jnp.sum(jnp.where(onehot, starts[None, :], 0), axis=1, dtype=jnp.int32)
    return (doc_ids, places - doc_first)


def rotate(value, doc_pos):
    half_dim = value.shape[-1] // 2
    frequency = rope_base ** (-2.0 * jnp.arange(half_dim, dtype=jnp.float32) / value.shape[-1])
    angles = doc_pos.astype(jnp.float32)[:, None] * frequency[None, :]
    cosine = jnp.cos(angles)[:, None, :]
    sine_part = jnp.sin(angles)[:, None, :]
    first_half = value[..., :half_dim]
    second_half = value[..., half_dim:]
    return jnp.concatenate(
        [
            first_half * cosine - second_half * sine_part,
            second_half * cosine + first_half * sine_part,
        ],
        axis=-1,
    )


def contract_rows(left_side, right_side):
    return lax.dot_general(
        left_side, right_side, (((0,), (0,)), ((), ())), preferred_element_type=jnp.float32
    )


def contract_cols(left_side, right_side):
    return lax.dot_general(
        left_side, right_side, (((1,), (1,)), ((), ())), preferred_element_type=jnp.float32
    )


def key_mask(query_places, query_docs, key_places, key_docs):
    return (
        (key_places[None, :] >= 0)
        & (query_docs[:, None] == key_docs[None, :])
        & (key_places[None, :] <= query_places[:, None])
        & (query_places[:, None] - key_places[None, :] < WINDOW)
    )


def attn_scores(queries, all_keys, allowed):
    scores = jnp.einsum("qkgd,pkd->kgqp", queries, all_keys, preferred_element_type=jnp.float32)
    capped = jnp.where(allowed[None, None], soft_cap * jnp.tanh(scores / soft_cap), -1e30)
    return (scores, capped)


def swapped(x):
    return lax.ppermute(x, "seq", [(0, 1), (1, 0)])


def place_of():
    dp = lax.axis_index("dp")
    seq = lax.axis_index("seq")
    a, b, c = dp // 4, lax.rem(dp // 2, 2), lax.rem(dp, 2)
    return a, b, c, seq


def number(a, b, c):
    return (a * 2 + b) * 2 + c


def enter(line, a, b, c, seq):
    barrier = pltpu.get_barrier_semaphore()

    def tell(a2, b2, c2):
        pl.semaphore_signal(
            barrier, inc=1, device_id=(number(a2, b2, c2), seq), device_id_type=MESH
        )

    tell(a, b, 1 - c)
    tell(a, 1 - b, c)

    @pl.when(a > 0)
    def _():
        tell(a - 1, b, c)

    @pl.when(a < line - 1)
    def _():
        tell(a + 1, b, c)

    peers = 2 + jnp.minimum(a, 1) + jnp.minimum(line - 1 - a, 1)
    pl.semaphore_wait(barrier, peers)


def gather_kernel(n_dp, x_ref, out_ref, own_sem, send_sem, recv_sem):
    line = n_dp // 4
    a, b, c, seq = place_of()
    me = number(a, b, c)
    own = pltpu.make_async_copy(x_ref, out_ref.at[me], own_sem)
    own.start()
    enter(line, a, b, c, seq)

    def copy(way, src, block, a2, b2, c2):
        return pltpu.make_async_remote_copy(
            src_ref=src,
            dst_ref=out_ref.at[block],
            send_sem=send_sem.at[way, block],
            recv_sem=recv_sem.at[block],
            device_id=(number(a2, b2, c2), seq),
            device_id_type=MESH,
        )

    def up(src, block):
        return copy(0, src, block, a + 1, b, c)

    def down(src, block):
        return copy(1, src, block, a - 1, b, c)

    def across(src, block):
        return copy(2, src, block, a, 1 - b, c)

    def over(src, block):
        return copy(3, src, block, a, b, 1 - c)

    has_up, has_down = a < line - 1, a > 0

    @pl.when(has_up)
    def _():
        up(x_ref, me).start()

    @pl.when(has_down)
    def _():
        down(x_ref, me).start()

    across(x_ref, me).start()
    over(x_ref, me).start()

    def arrived(block):
        over(out_ref.at[block], block).wait_recv()

    for k in range(1, line + 1):
        if k < line:

            @pl.when(a - k >= 0)
            def _(k=k):
                block = number(a - k, b, c)
                arrived(block)
                view = out_ref.at[block]

                @pl.when(has_up)
                def _():
                    up(view, block).start()

                across(view, block).start()
                over(view, block).start()

            @pl.when(a + k < line)
            def _(k=k):
                block = number(a + k, b, c)
                arrived(block)
                view = out_ref.at[block]

                @pl.when(has_down)
                def _():
                    down(view, block).start()

                across(view, block).start()
                over(view, block).start()

        j = k - 1
        for sign in (-1, 1) if j else (1,):

            @pl.when((a + sign * j >= 0) & (a + sign * j < line))
            def _(j=j, sign=sign):
                block = number(a + sign * j, 1 - b, c)
                arrived(block)
                over(out_ref.at[block], block).start()

    for other in range(n_dp // 2):
        block = other * 2 + 1 - c
        arrived(block)

    own.wait()
    for i in range(line):
        block = number(i, b, c)
        across(out_ref.at[block], block).wait_send()
        over(out_ref.at[block], block).wait_send()
        second = number(i, 1 - b, c)
        over(out_ref.at[second], second).wait_send()

        @pl.when(has_up & (i <= a))
        def _(block=block):
            up(out_ref.at[block], block).wait_send()

        @pl.when(has_down & (i >= a))
        def _(block=block):
            down(out_ref.at[block], block).wait_send()


def gathered(x, n_dp, collective_id):
    return pl.pallas_call(
        functools.partial(gather_kernel, n_dp),
        out_shape=jax.ShapeDtypeStruct((n_dp, *x.shape), x.dtype),
        in_specs=[pl.BlockSpec(memory_space=pltpu.VMEM)],
        out_specs=pl.BlockSpec(memory_space=pl.ANY),
        scratch_shapes=[
            pltpu.SemaphoreType.DMA,
            pltpu.SemaphoreType.DMA((4, n_dp)),
            pltpu.SemaphoreType.DMA((n_dp,)),
        ],
        compiler_params=pltpu.CompilerParams(
            collective_id=collective_id, has_side_effects=True
        ),
        cost_estimate=pl.CostEstimate(
            flops=0, bytes_accessed=150_000_000, transcendentals=0
        ),
    )(x)


def scatter_steps(n_dp, place, prepare, produce, core_source, out_ref, from_core, from_pair, up_buf,
                  down_buf, pair_out, core_send, core_recv, pair_send, pair_recv, up_send,
                  up_recv, down_send, down_recv):
    line = n_dp // 4
    a, b, c, seq = place
    enter(line, a, b, c, seq)

    def core_copy(block):
        half = block // 2
        return pltpu.make_async_remote_copy(
            src_ref=core_source(block),
            dst_ref=from_core.at[half],
            send_sem=core_send.at[half],
            recv_sem=core_recv.at[half],
            device_id=(number(a, b, 1 - c), seq),
            device_id_type=MESH,
        )

    def pair_copy(to):
        return pltpu.make_async_remote_copy(
            src_ref=pair_out.at[to],
            dst_ref=from_pair.at[to],
            send_sem=pair_send.at[to],
            recv_sem=pair_recv.at[to],
            device_id=(number(a, 1 - b, c), seq),
            device_id_type=MESH,
        )

    def up_copy(to):
        return pltpu.make_async_remote_copy(
            src_ref=up_buf.at[to],
            dst_ref=up_buf.at[to],
            send_sem=up_send.at[to],
            recv_sem=up_recv.at[to],
            device_id=(number(a + 1, b, c), seq),
            device_id_type=MESH,
        )

    def down_copy(to):
        return pltpu.make_async_remote_copy(
            src_ref=down_buf.at[to],
            dst_ref=down_buf.at[to],
            send_sem=down_send.at[to],
            recv_sem=down_recv.at[to],
            device_id=(number(a - 1, b, c), seq),
            device_id_type=MESH,
        )

    def each_target(act):
        for k in range(line - 1, 0, -1):

            @pl.when(a + k < line)
            def _(k=k):
                act(a + k, 1)

            @pl.when(a - k >= 0)
            def _(k=k):
                act(a - k, -1)

        act(a, 0)

    def send_core(block):
        produce(block, None, core_source(block))
        core_copy(block).start()

    prepare(1 - b, 1 - c)
    each_target(lambda to, way: send_core(number(to, 1 - b, 1 - c)))
    prepare(1 - b, c)

    def send_pair(to, way):
        block = number(to, 1 - b, c)
        core_copy(block).wait_recv()
        produce(block, [from_core.at[block // 2]], pair_out.at[to])
        pair_copy(to).start()

    each_target(send_pair)
    prepare(b, 1 - c)
    each_target(lambda to, way: send_core(number(to, b, 1 - c)))
    prepare(b, c)

    def line_sum(to, more, dst):
        block = number(to, b, c)
        produce(block, [from_core.at[block // 2], from_pair.at[to], *more], dst)

    def send_line(to, way):
        core_copy(number(to, b, c)).wait_recv()
        pair_copy(to).wait_recv()
        if way:
            buf, copy = (up_buf, up_copy) if way == 1 else (down_buf, down_copy)
            at_end = (a == 0) if way == 1 else (a == line - 1)

            @pl.when(at_end)
            def _():
                line_sum(to, [], buf.at[to])

            @pl.when(jnp.logical_not(at_end))
            def _():
                copy(to).wait_recv()
                line_sum(to, [buf.at[to]], buf.at[to])

            copy(to).start()
        else:
            line_sum(to, [], out_ref)
            for copy, buf, there in (
                (up_copy, up_buf, a > 0),
                (down_copy, down_buf, a < line - 1),
            ):

                @pl.when(there)
                def _(copy=copy, buf=buf):
                    copy(to).wait_recv()
                    add_rows(out_ref, buf.at[to])

    each_target(send_line)

    for i in range(n_dp // 2):
        core_copy(i * 2 + 1 - c).wait_send()
    for i in range(line):
        pair_copy(i).wait_send()

        @pl.when(i > a)
        def _(i=i):
            up_copy(i).wait_send()

        @pl.when(i < a)
        def _(i=i):
            down_copy(i).wait_send()


def row_tiles(rows):
    return 16 if rows % 16 == 0 else rows


def add_rows(out_ref, term):
    tile = row_tiles(out_ref.shape[0])

    def step(i, _):
        at = pl.ds(pl.multiple_of(i * tile, tile), tile)
        out_ref[at, :] += term[at, :].astype(jnp.float32)
        return 0

    lax.fori_loop(0, out_ref.shape[0] // tile, step, 0)


def dots_kernel(n_dp, n_terms, *refs):
    lefts, rights = refs[:n_terms], refs[n_terms : 2 * n_terms]
    out_ref, parts, *scratch = refs[2 * n_terms :]
    _, rows, cols = parts.shape
    f32 = jnp.float32

    def prepare(b, c):
        for first in range(0, n_dp // 4, 4):
            blocks = [number(first + i, b, c) for i in range(4)]

            def step(j, _):
                at = pl.ds(pl.multiple_of(j * 256, 256), 256)
                total = jnp.zeros((4 * rows, 256), f32)
                for left, right in zip(lefts, rights):
                    stacked = jnp.concatenate([left[k] for k in blocks], axis=0)
                    total += jnp.dot(stacked, right[:, at], preferred_element_type=f32)
                for i, k in enumerate(blocks):
                    parts[k, :, at] = total[i * rows : (i + 1) * rows].astype(parts.dtype)
                return 0

            lax.fori_loop(0, cols // 256, step, 0)

    def produce(block, terms, dst):
        if terms is None:
            return
        tile = row_tiles(rows)

        def step(i, _):
            at = pl.ds(pl.multiple_of(i * tile, tile), tile)
            total = parts[block, at, :].astype(f32)
            for term in terms:
                total += term[at, :].astype(f32)
            dst[at, :] = total.astype(dst.dtype)
            return 0

        lax.fori_loop(0, rows // tile, step, 0)

    scatter_steps(
        n_dp, place_of(), prepare, produce, lambda block: parts.at[block], out_ref, *scratch
    )


def product_kernel(n_dp, left_a, right_a, left_b, right_b, extra, out_ref, core_out, *scratch):
    cols_a, cols_b = right_a.shape[1], right_b.shape[1]

    def produce(block, terms, dst):
        def part(left, right, first, wide):
            def step(i, _):
                inner = pl.ds(pl.multiple_of(i * wide, wide), wide)
                outer = pl.ds(pl.multiple_of(first + i * wide, 128), wide)
                total = jnp.dot(
                    left[block], right[:, inner], preferred_element_type=jnp.float32
                )
                for term in terms or []:
                    total += term[:, outer].astype(jnp.float32)
                dst[:, outer] = total.astype(dst.dtype)
                return 0

            lax.fori_loop(0, right.shape[1] // wide, step, 0)

        part(left_a, right_a, 0, 256)
        part(left_b, right_b, cols_a, 256)
        last = pl.ds(cols_a + cols_b, extra.shape[2])
        total = extra[block].astype(jnp.float32)
        for term in terms or []:
            total += term[:, last].astype(jnp.float32)
        dst[:, last] = total.astype(dst.dtype)

    scatter_steps(
        n_dp,
        place_of(),
        lambda b, c: None,
        produce,
        lambda block: core_out.at[block // 2],
        out_ref,
        *scratch,
    )


def scatter_scratch(n_dp, rows, cols, dtype):
    line = n_dp // 4
    return (
        [pltpu.VMEM((n_dp // 2, rows, cols), dtype)]
        + [pltpu.VMEM((line, rows, cols), dtype)] * 4
        + [pltpu.SemaphoreType.DMA((n_dp // 2,))] * 2
        + [pltpu.SemaphoreType.DMA((line,))] * 6
    )


def scattered_products(left_a, right_a, left_b, right_b, extra, collective_id):
    n_dp, rows, _ = left_a.shape
    cols = right_a.shape[1] + right_b.shape[1] + extra.shape[2]
    return pl.pallas_call(
        functools.partial(product_kernel, n_dp),
        out_shape=jax.ShapeDtypeStruct((rows, cols), jnp.float32),
        in_specs=[pl.BlockSpec(memory_space=pltpu.VMEM)] * 5,
        out_specs=pl.BlockSpec(memory_space=pltpu.VMEM),
        scratch_shapes=[pltpu.VMEM((n_dp // 2, rows, cols), jnp.bfloat16)]
        + scatter_scratch(n_dp, rows, cols, jnp.bfloat16),
        compiler_params=pltpu.CompilerParams(
            collective_id=collective_id, has_side_effects=True
        ),
        cost_estimate=pl.CostEstimate(
            flops=0, bytes_accessed=200_000_000, transcendentals=0
        ),
    )(left_a, right_a, left_b, right_b, extra)


def scattered_dots(lefts, rights, collective_id):
    n_dp, rows, _ = lefts[0].shape
    cols = rights[0].shape[1]
    held = n_dp * (1 + 1 / 2 + 1) * rows * cols * 2
    pieces = 1
    while held > pieces * 36 * 2**20 or cols % (256 * pieces):
        pieces += 1
    width = cols // pieces
    return jnp.concatenate(
        [
            scattered_piece(
                lefts, [r[:, i * width : (i + 1) * width] for r in rights], collective_id
            )
            for i in range(pieces)
        ],
        axis=1,
    )


def scattered_piece(lefts, rights, collective_id):
    n_dp, rows, _ = lefts[0].shape
    cols = rights[0].shape[1]
    return pl.pallas_call(
        functools.partial(dots_kernel, n_dp, len(lefts)),
        out_shape=jax.ShapeDtypeStruct((rows, cols), jnp.float32),
        in_specs=[pl.BlockSpec(memory_space=pltpu.VMEM)] * (2 * len(lefts)),
        out_specs=pl.BlockSpec(memory_space=pltpu.VMEM),
        scratch_shapes=[pltpu.VMEM((n_dp, rows, cols), jnp.bfloat16)]
        + scatter_scratch(n_dp, rows, cols, jnp.bfloat16),
        compiler_params=pltpu.CompilerParams(
            collective_id=collective_id, has_side_effects=True
        ),
        cost_estimate=pl.CostEstimate(
            flops=0, bytes_accessed=150_000_000, transcendentals=0
        ),
    )(*lefts, *rights)


def row_major(x):
    return with_layout_constraint(x, Layout(major_to_minor=(0, 1)))


def mine_and_other(halves, seq_index):
    first = seq_index == 0
    return (
        jnp.where(first, halves[0], halves[1]),
        jnp.where(first, halves[1], halves[0]),
    )


def in_order(own, other, seq_index):
    first = seq_index == 0
    return jnp.where(first, own, other), jnp.where(first, other, own)


def column_halves(weight):
    q_cols, k_cols = HEADS * HEAD_DIM, KV_HEADS * HEAD_DIM
    starts = (0, q_cols, q_cols + k_cols, q_cols + 2 * k_cols)
    sizes = (q_cols // 2, k_cols // 2, k_cols // 2, q_cols // 2)
    return [
        jnp.concatenate(
            [weight[:, s + h * n : s + (h + 1) * n] for s, n in zip(starts, sizes)], axis=1
        )
        for h in range(2)
    ]


def layer(tokens, doc_lengths, attn_weight, ffn_weight, gains, out_grad):
    tok_rows = tokens.shape[0]
    n_dp = lax.axis_size("dp")
    heads, kv_heads = HEADS // 2, KV_HEADS // 2
    q_cols = heads * HEAD_DIM
    k_cols = kv_heads * HEAD_DIM
    proj_cols = q_cols + 2 * k_cols
    half_cols = proj_cols + q_cols
    group_size = HEADS // KV_HEADS
    query_scale = HEAD_DIM ** (-0.5)
    bf16 = jnp.bfloat16
    seq_index = lax.axis_index("seq")
    weight_rows = attn_weight.shape[0]

    run = jnp.arange(tok_rows, dtype=jnp.int32)
    places = jnp.concatenate([seq_index * tok_rows + run, (1 - seq_index) * tok_rows + run])
    docs, pos = doc_layout(doc_lengths[0], places)
    allowed = key_mask(places, docs, places, docs)

    gain_cols = jnp.pad(gains, ((0, 0), (0, 124)))
    my_cols, other_cols = mine_and_other(column_halves(attn_weight), seq_index)
    my_cols = jnp.concatenate([my_cols, gain_cols], axis=1)
    other_cols = jnp.concatenate([other_cols, gain_cols], axis=1)
    partner_cols = swapped(other_cols)
    other_tokens = swapped(tokens)
    ffn_own, partner_cols = lax.optimization_barrier((ffn_weight, partner_cols))
    ffn_other = swapped(ffn_own)
    block = jnp.concatenate(in_order(my_cols, partner_cols, seq_index), axis=0)
    attn_full = gathered(block, n_dp, 0).reshape(-1, half_cols + 128)
    gain_vals = attn_full[:, half_cols : half_cols + 4].astype(jnp.float32).T
    attn_weights = attn_full[:, :proj_cols]
    out_weights = attn_full[:, proj_cols:half_cols]

    pack_tokens = jnp.concatenate([tokens, other_tokens]).astype(jnp.float32)
    tokens_f = tokens.astype(jnp.float32)
    attn_in = rms_norm(pack_tokens, gain_vals[0]).astype(bf16)
    projected = jnp.dot(attn_in, attn_weights, preferred_element_type=jnp.float32)
    pack = 2 * tok_rows
    queries = (
        rotate(projected[:, :q_cols].reshape(pack, heads, HEAD_DIM), pos) * query_scale
    ).astype(bf16)
    queries = queries.reshape(pack, kv_heads, group_size, HEAD_DIM)
    keys = rotate(
        projected[:, q_cols : q_cols + k_cols].reshape(pack, kv_heads, HEAD_DIM), pos
    ).astype(bf16)
    values = projected[:, q_cols + k_cols :].reshape(pack, kv_heads, HEAD_DIM).astype(bf16)
    scores, capped = attn_scores(queries, keys, allowed)
    row_max = jnp.max(capped, axis=-1, keepdims=True)
    exp_terms = jnp.exp(capped - row_max)
    row_total = jnp.sum(exp_terms, axis=-1, keepdims=True)
    log_total = row_max + jnp.log(row_total)
    attn_probs = (exp_terms / row_total).astype(bf16)
    mixed_heads = jnp.einsum(
        "kgqp,pkd->qkgd", attn_probs, values, preferred_element_type=jnp.float32
    )
    mixed_heads = mixed_heads.reshape(pack, q_cols).astype(bf16)
    attn_part_out = contract_cols(mixed_heads, out_weights)
    attn_part_other = swapped(attn_part_out[tok_rows:].astype(bf16))
    attn_out = attn_part_out[:tok_rows] + attn_part_other.astype(jnp.float32)
    middle = tokens_f + rms_norm(attn_out, gain_vals[1])
    ffn_input = rms_norm(middle, gain_vals[2]).astype(bf16)

    gate_weights, up_weights, down_weights = [
        jnp.concatenate([ffn_own[:, k * D : (k + 1) * D], ffn_other[:, k * D : (k + 1) * D]])
        for k in range(3)
    ]
    unit_count = gate_weights.shape[0]
    ffn_all = gathered(ffn_input, n_dp, 1).reshape(-1, D)
    gate = contract_cols(ffn_all, gate_weights)
    up = contract_cols(ffn_all, up_weights)
    hidden = row_major(gated_gelu(gate, up).astype(bf16))
    ffn_out = scattered_dots([hidden.reshape(n_dp, tok_rows, -1)], [down_weights], 2)
    out_gain = gain_vals[3]
    block_out = (middle + rms_norm(ffn_out, out_gain)).astype(bf16)
    cotangent = out_grad.astype(jnp.float32)
    d_ffn_f, d_gain_out = norm_back(ffn_out, out_gain, cotangent)
    d_ffn_all = gathered(d_ffn_f.astype(bf16), n_dp, 1).reshape(-1, D)
    d_hidden = contract_cols(d_ffn_all, down_weights)
    d_gate, d_up = jax.vjp(gated_gelu, gate, up)[1](d_hidden)
    d_gate, d_up = row_major(d_gate.astype(bf16)), row_major(d_up.astype(bf16))
    d_ffn_input = scattered_dots(
        [d_gate.reshape(n_dp, tok_rows, -1), d_up.reshape(n_dp, tok_rows, -1)],
        [gate_weights, up_weights],
        4,
    )

    own_units = unit_count // 2
    weight_sum = [
        contract_rows(d_gate, ffn_all),
        contract_rows(d_up, ffn_all),
        contract_rows(hidden, d_ffn_all),
    ]
    sent = jnp.concatenate([w[own_units:].astype(bf16) for w in weight_sum], axis=1)
    kept = jnp.concatenate([w[:own_units] for w in weight_sum], axis=1)
    grad_other = swapped(sent)
    ffn_weight_grad = kept + grad_other.astype(jnp.float32)

    d_middle_add, d_gain_ffn = norm_back(middle, gain_vals[2], d_ffn_input)
    d_middle = cotangent + d_middle_add
    d_attn_f, d_gain_post = norm_back(attn_out, gain_vals[1], d_middle)
    d_attn_own = d_attn_f.astype(bf16)
    d_attn_other = swapped(d_attn_own)
    d_attn = jnp.concatenate([d_attn_own, d_attn_other])
    d_mixed = jnp.dot(d_attn, out_weights, preferred_element_type=jnp.float32).astype(bf16)
    d_mixed = d_mixed.reshape(pack, kv_heads, group_size, HEAD_DIM)
    attn_p = jnp.exp(capped - log_total)
    d_probs = jnp.einsum("qkgd,pkd->kgqp", d_mixed, values, preferred_element_type=jnp.float32)
    d_values = jnp.einsum(
        "kgqp,qkgd->pkd", attn_probs, d_mixed, preferred_element_type=jnp.float32
    )
    d_capped = attn_p * (d_probs - jnp.sum(attn_p * d_probs, axis=-1, keepdims=True))
    tanh_part = jnp.tanh(scores / soft_cap)
    d_scores = (d_capped * (1.0 - tanh_part * tanh_part)).astype(bf16)
    d_queries = jnp.einsum("kgqp,pkd->qkgd", d_scores, keys, preferred_element_type=jnp.float32)
    d_keys = jnp.einsum("kgqp,qkgd->pkd", d_scores, queries, preferred_element_type=jnp.float32)
    d_query_raw = rotate(d_queries.reshape(pack, heads, HEAD_DIM) * query_scale, -pos)
    d_key_raw = rotate(d_keys, -pos)
    d_projected = jnp.concatenate(
        [
            d_query_raw.reshape(pack, q_cols),
            d_key_raw.reshape(pack, k_cols),
            d_values.reshape(pack, k_cols),
        ],
        axis=1,
    ).astype(bf16)
    d_attn_in_part = contract_cols(d_projected, attn_weights)
    d_attn_in_other = swapped(d_attn_in_part[tok_rows:].astype(bf16))
    d_attn_in = d_attn_in_part[:tok_rows] + d_attn_in_other.astype(jnp.float32)
    normed = pack_tokens * lax.rsqrt(
        jnp.mean(pack_tokens * pack_tokens, axis=-1, keepdims=True) + eps_norm
    )
    d_gain_in = jnp.sum(d_attn_in_part * normed, axis=0)

    gain_part = jnp.stack([d_gain_in, d_gain_post, d_gain_ffn, d_gain_out], axis=1)
    block_rows = (n_dp, 2 * weight_rows)
    attn_sum = scattered_products(
        attn_in.T.reshape(*block_rows, pack),
        d_projected,
        d_attn.T.reshape(*block_rows, pack),
        mixed_heads,
        jnp.pad(gain_part.astype(bf16), ((0, 0), (0, 124))).reshape(*block_rows, 128),
        3,
    )
    d_tokens_add = norm_back(tokens_f, gain_vals[0], d_attn_in)[0]
    tokens_grad = d_middle + d_tokens_add
    mine, others = mine_and_other(
        (attn_sum[:weight_rows], attn_sum[weight_rows:]), seq_index
    )
    partner = swapped(others.astype(bf16)).astype(jnp.float32)
    gains_grad = mine[:, half_cols : half_cols + 4] + partner[:, half_cols : half_cols + 4]
    first, second = in_order(mine, partner, seq_index)
    cuts = ((0, q_cols), (q_cols, q_cols + k_cols), (q_cols + k_cols, proj_cols),
            (proj_cols, half_cols))
    attn_weight_grad = jnp.concatenate(
        [half[:, lo:hi] for lo, hi in cuts for half in (first, second)], axis=1
    )
    return (block_out, tokens_grad, attn_weight_grad, ffn_weight_grad, gains_grad)


def solution(mesh):
    return jax.shard_map(
        layer,
        mesh=mesh,
        in_specs=(
            P(("dp", "seq"), None),
            P("dp", None),
            P(("dp", "seq"), None),
            P(("dp", "seq"), None),
            P(("dp", "seq"), None),
            P(("dp", "seq"), None),
        ),
        out_specs=(
            P(("dp", "seq"), None),
            P(("dp", "seq"), None),
            P(("dp", "seq"), None),
            P(("dp", "seq"), None),
            P(("dp", "seq"), None),
        ),
        check_vma=False,
    )
```

```python
import functools
import math

import jax
import jax.numpy as jnp
from jax import lax
from jax.experimental.layout import Layout, with_layout_constraint
from jax.experimental import pallas as pl
from jax.experimental.pallas import tpu as pltpu
from jax.sharding import PartitionSpec as P

D = 2304
HEADS = 8
KV_HEADS = 4
HEAD_DIM = 256
WINDOW = 128


soft_cap = 50.0
eps_norm = 1e-06
rope_base = 10000.0
gelu_coef = math.sqrt(2.0 / math.pi)


MESH = pl.DeviceIdType.MESH


def gelu_tanh(value):
    return 0.5 * value * (1.0 + jnp.tanh(gelu_coef * (value + 0.044715 * value * value * value)))


def gated_gelu(gate_pre, up_pre):
    return gelu_tanh(gate_pre) * up_pre


def rms_norm(value, gain_vec):
    return value * lax.rsqrt(jnp.mean(value * value, axis=-1, keepdims=True) + eps_norm) * gain_vec


def norm_back(value, gain_vec, incoming):
    return jax.vjp(rms_norm, value, gain_vec)[1](incoming)


def doc_layout(lengths, places):
    doc_ends = jnp.cumsum(lengths, dtype=jnp.int32)
    starts = doc_ends - lengths
    doc_ids = jnp.sum(
        (places[:, None] >= doc_ends[None, :]).astype(jnp.int32), axis=1, dtype=jnp.int32
    )
    onehot = doc_ids[:, None] == jnp.arange(lengths.shape[0], dtype=jnp.int32)[None, :]
    doc_first = jnp.sum(jnp.where(onehot, starts[None, :], 0), axis=1, dtype=jnp.int32)
    return (doc_ids, places - doc_first)


def rotate(value, doc_pos):
    half_dim = value.shape[-1] // 2
    frequency = rope_base ** (-2.0 * jnp.arange(half_dim, dtype=jnp.float32) / value.shape[-1])
    angles = doc_pos.astype(jnp.float32)[:, None] * frequency[None, :]
    cosine = jnp.cos(angles)[:, None, :]
    sine_part = jnp.sin(angles)[:, None, :]
    first_half = value[..., :half_dim]
    second_half = value[..., half_dim:]
    return jnp.concatenate(
        [
            first_half * cosine - second_half * sine_part,
            second_half * cosine + first_half * sine_part,
        ],
        axis=-1,
    )


def contract_rows(left_side, right_side):
    return lax.dot_general(
        left_side, right_side, (((0,), (0,)), ((), ())), preferred_element_type=jnp.float32
    )


def contract_cols(left_side, right_side):
    return lax.dot_general(
        left_side, right_side, (((1,), (1,)), ((), ())), preferred_element_type=jnp.float32
    )


def key_mask(query_places, query_docs, key_places, key_docs):
    return (
        (key_places[None, :] >= 0)
        & (query_docs[:, None] == key_docs[None, :])
        & (key_places[None, :] <= query_places[:, None])
        & (query_places[:, None] - key_places[None, :] < WINDOW)
    )


def attn_scores(queries, all_keys, allowed):
    scores = jnp.einsum("qkgd,pkd->kgqp", queries, all_keys, preferred_element_type=jnp.float32)
    capped = jnp.where(allowed[None, None], soft_cap * jnp.tanh(scores / soft_cap), -1e30)
    return (scores, capped)


def swapped(x):
    return lax.ppermute(x, "seq", [(0, 1), (1, 0)])


def place_of():
    dp = lax.axis_index("dp")
    seq = lax.axis_index("seq")
    a, b, c = dp // 4, lax.rem(dp // 2, 2), lax.rem(dp, 2)
    return a, b, c, seq


def number(a, b, c):
    return (a * 2 + b) * 2 + c


def enter(line, a, b, c, seq):
    barrier = pltpu.get_barrier_semaphore()

    def tell(a2, b2, c2):
        pl.semaphore_signal(
            barrier, inc=1, device_id=(number(a2, b2, c2), seq), device_id_type=MESH
        )

    tell(a, b, 1 - c)
    tell(a, 1 - b, c)

    @pl.when(a > 0)
    def _():
        tell(a - 1, b, c)

    @pl.when(a < line - 1)
    def _():
        tell(a + 1, b, c)

    peers = 2 + jnp.minimum(a, 1) + jnp.minimum(line - 1 - a, 1)
    pl.semaphore_wait(barrier, peers)


def split_at(cols):
    return cols // 768 * 128


def gather_kernel(n_dp, x_ref, out_ref, own_sem, send_sem, recv_sem):
    line = n_dp // 4
    a, b, c, seq = place_of()
    me, pair = number(a, b, c), number(a, 1 - b, c)
    cols = x_ref.shape[1]
    late = split_at(cols)
    spans = (pl.ds(late, cols - late), pl.ds(0, late))
    own = pltpu.make_async_copy(x_ref, out_ref.at[me], own_sem)
    own.start()
    enter(line, a, b, c, seq)

    def copy(way, block, piece, own=False):
        a2 = a + (1 if way == 0 else -1 if way == 1 else 0)
        b2 = 1 - b if way == 2 else b
        c2 = 1 - c if way == 3 else c
        there = out_ref.at[block, :, spans[piece]]
        return pltpu.make_async_remote_copy(
            src_ref=x_ref.at[:, spans[piece]] if own else there,
            dst_ref=there,
            send_sem=send_sem.at[way, block, piece],
            recv_sem=recv_sem.at[block, piece],
            device_id=(number(a2, b2, c2), seq),
            device_id_type=MESH,
        )

    up, down, across, over = range(4)
    has_up, has_down = a < line - 1, a > 0

    def start(way, block, piece, own=False):
        if way in (up, down):

            @pl.when(has_up if way == up else has_down)
            def _():
                copy(way, block, piece, own).start()

        else:
            copy(way, block, piece, own).start()

    def pass_on(block, piece, ways):
        copy(over, block, piece).wait_recv()
        for way in ways:
            start(way, block, piece)

    for way, piece in (
        (across, 1), (up, 0), (down, 0), (across, 0), (up, 1), (down, 1), (over, 1), (over, 0)
    ):
        start(way, me, piece, own=True)
    pass_on(pair, 1, (up, down, over))

    for k in range(1, line + 1):
        if k < line:
            for near, piece in ((True, 0), (True, 1), (False, 1)):
                for sign, way in ((-1, up), (1, down)):

                    @pl.when((a + sign * k >= 0) & (a + sign * k < line))
                    def _(near=near, piece=piece, sign=sign, way=way, k=k):
                        block = number(a + sign * k, b if near else 1 - b, c)
                        pass_on(block, piece, (way, over) if piece else (way, across, over))

        j = k - 1
        for sign in (-1, 1) if j else (1,):

            @pl.when((a + sign * j >= 0) & (a + sign * j < line))
            def _(j=j, sign=sign):
                pass_on(number(a + sign * j, 1 - b, c), 0, (over,))

    for other in range(n_dp // 2):
        for piece in range(2):
            copy(over, other * 2 + 1 - c, piece).wait_recv()

    own.wait()
    copy(across, me, 1).wait_send()
    for i in range(line):
        near, far = number(i, b, c), number(i, 1 - b, c)
        copy(across, near, 0).wait_send()
        for block, piece in ((near, 0), (near, 1), (far, 0), (far, 1)):
            copy(over, block, piece).wait_send()
        for block, piece in ((near, 0), (near, 1), (far, 1)):

            @pl.when(has_up & (i <= a))
            def _(block=block, piece=piece):
                copy(up, block, piece).wait_send()

            @pl.when(has_down & (i >= a))
            def _(block=block, piece=piece):
                copy(down, block, piece).wait_send()


def gathered(x, n_dp, collective_id):
    return pl.pallas_call(
        functools.partial(gather_kernel, n_dp),
        out_shape=jax.ShapeDtypeStruct((n_dp, *x.shape), x.dtype),
        in_specs=[pl.BlockSpec(memory_space=pltpu.VMEM)],
        out_specs=pl.BlockSpec(memory_space=pl.ANY),
        scratch_shapes=[
            pltpu.SemaphoreType.DMA,
            pltpu.SemaphoreType.DMA((4, n_dp, 2)),
            pltpu.SemaphoreType.DMA((n_dp, 2)),
        ],
        compiler_params=pltpu.CompilerParams(
            collective_id=collective_id, has_side_effects=True
        ),
        cost_estimate=pl.CostEstimate(
            flops=0, bytes_accessed=150_000_000, transcendentals=0
        ),
    )(x)


def scatter_steps(n_dp, place, prepare, produce, core_source, out_ref, from_core, from_pair,
                  up_buf, down_buf, pair_out, up_few, down_few, pair_few, core_send, core_recv,
                  pair_send, pair_recv, up_send, up_recv, down_send, down_recv, few_send,
                  few_recv):
    line = n_dp // 4
    a, b, c, seq = place
    cols = out_ref.shape[1]
    late = split_at(cols)
    most, few = (late, cols), (0, late)
    enter(line, a, b, c, seq)

    def remote(src, dst, send, recv, to_a, to_b, to_c):
        return pltpu.make_async_remote_copy(
            src_ref=src,
            dst_ref=dst,
            send_sem=send,
            recv_sem=recv,
            device_id=(number(to_a, to_b, to_c), seq),
            device_id_type=MESH,
        )

    def core_copy(block):
        half = block // 2
        return remote(
            core_source(block), from_core.at[half], core_send.at[half], core_recv.at[half],
            a, b, 1 - c,
        )

    def pair_copy(to):
        return remote(
            pair_out.at[to], from_pair.at[to], pair_send.at[to], pair_recv.at[to], a, 1 - b, c
        )

    def few_copy():
        return remote(
            pair_few.at[0], pair_few.at[1], few_send.at[0], few_recv.at[0], a, 1 - b, c
        )

    def line_copy(way, to, column):
        wide, thin = (up_buf, up_few) if way == 1 else (down_buf, down_few)
        send, recv = (up_send, up_recv) if way == 1 else (down_send, down_recv)
        buf = wide.at[to] if column is None else thin.at[to * 2 + column]
        at = to * 3 + (2 if column is None else column)
        return buf, remote(buf, buf, send.at[at], recv.at[at], a + way, b, c)

    def each_target(act, own=True):
        for k in range(line - 1, 0, -1):

            @pl.when(a + k < line)
            def _(k=k):
                act(a + k, 1)

            @pl.when(a - k >= 0)
            def _(k=k):
                act(a - k, -1)

        if own:
            act(a, 0)

    def send_core(block):
        produce(block, [], core_source(block), 0, few)
        produce(block, [], core_source(block), 0, most)
        core_copy(block).start()

    def send_pair(to, way):
        block = number(to, 1 - b, c)
        core_copy(block).wait_recv()
        produce(block, [(from_core.at[block // 2], 0)], pair_out.at[to], late, most)
        pair_copy(to).start()

    def chain(to, way, column, block, terms, base, span):
        buf, copy = line_copy(way, to, column)
        at_end = (a == 0) if way == 1 else (a == line - 1)

        @pl.when(at_end)
        def _():
            produce(block, terms, buf, base, span)

        @pl.when(jnp.logical_not(at_end))
        def _():
            copy.wait_recv()
            produce(block, [*terms, (buf, base)], buf, base, span)

        copy.start()

    def collect(column, dst, lo):
        for way, there in ((1, a > 0), (-1, a < line - 1)):

            @pl.when(there)
            def _(way=way):
                buf, copy = line_copy(way, a, column)
                copy.wait_recv()
                add_rows(dst, buf, lo)

    def send_few(b2):
        def act(to, way):
            block = number(to, b2, c)
            chain(to, way, b2, block, [(from_core.at[block // 2], 0)], 0, few)

        each_target(act, own=False)

    prepare(1 - b, 1 - c)
    each_target(lambda to, way: send_core(number(to, 1 - b, 1 - c)))
    prepare(1 - b, c)
    each_target(send_pair)
    prepare(b, 1 - c)
    each_target(lambda to, way: send_core(number(to, b, 1 - c)))
    prepare(b, c)
    send_few(1 - b)
    each_target(lambda to, way: core_copy(number(to, b, c)).wait_recv())
    send_few(b)

    far = number(a, 1 - b, c)
    produce(far, [(from_core.at[far // 2], 0)], pair_few.at[0], 0, few)
    collect(1 - b, pair_few.at[0], 0)
    few_copy().start()

    def send_line(to, way):
        block = number(to, b, c)
        pair_copy(to).wait_recv()
        terms = [(from_core.at[block // 2], 0), (from_pair.at[to], late)]
        if way:
            chain(to, way, None, block, terms, late, most)
        else:
            produce(block, terms, out_ref, 0, most)
            collect(None, out_ref, late)

    each_target(send_line)
    me = number(a, b, c)
    few_copy().wait_recv()
    produce(me, [(from_core.at[me // 2], 0), (pair_few.at[1], 0)], out_ref, 0, few)
    collect(b, out_ref, 0)

    for i in range(n_dp // 2):
        core_copy(i * 2 + 1 - c).wait_send()
    few_copy().wait_send()
    for i in range(line):
        pair_copy(i).wait_send()
        for column in (None, 0, 1):

            @pl.when(i > a)
            def _(i=i, column=column):
                line_copy(1, i, column)[1].wait_send()

            @pl.when(i < a)
            def _(i=i, column=column):
                line_copy(-1, i, column)[1].wait_send()


def row_tiles(rows):
    return 16 if rows % 16 == 0 else rows


def add_rows(dst, term, lo):
    tile = row_tiles(dst.shape[0])
    width = term.shape[1]

    def step(i, _):
        at = pl.ds(pl.multiple_of(i * tile, tile), tile)
        total = dst[at, lo : lo + width].astype(jnp.float32) + term[at, :].astype(jnp.float32)
        dst[at, lo : lo + width] = total.astype(dst.dtype)
        return 0

    lax.fori_loop(0, dst.shape[0] // tile, step, 0)


def dots_kernel(n_dp, n_terms, *refs):
    lefts, rights = refs[:n_terms], refs[n_terms : 2 * n_terms]
    out_ref, parts, *scratch = refs[2 * n_terms :]
    _, rows, cols = parts.shape
    f32 = jnp.float32

    def prepare(b, c):
        for first in range(0, n_dp // 4, 4):
            blocks = [number(first + i, b, c) for i in range(4)]

            def step(j, _):
                at = pl.ds(pl.multiple_of(j * 256, 256), 256)
                total = jnp.zeros((4 * rows, 256), f32)
                for left, right in zip(lefts, rights):
                    stacked = jnp.concatenate([left[k] for k in blocks], axis=0)
                    total += jnp.dot(stacked, right[:, at], preferred_element_type=f32)
                for i, k in enumerate(blocks):
                    parts[k, :, at] = total[i * rows : (i + 1) * rows].astype(parts.dtype)
                return 0

            lax.fori_loop(0, cols // 256, step, 0)

    def produce(block, terms, dst, base, span):
        if not terms:
            return
        lo, hi = span
        tile = row_tiles(rows)

        def step(i, _):
            at = pl.ds(pl.multiple_of(i * tile, tile), tile)
            total = parts[block, at, lo:hi].astype(f32)
            for term, first in terms:
                total += term[at, lo - first : hi - first].astype(f32)
            dst[at, lo - base : hi - base] = total.astype(dst.dtype)
            return 0

        lax.fori_loop(0, rows // tile, step, 0)

    scatter_steps(
        n_dp, place_of(), prepare, produce, lambda block: parts.at[block], out_ref, *scratch
    )


def product_kernel(n_dp, left_a, right_a, left_b, right_b, extra, out_ref, core_out, *scratch):
    cols_a, cols_b = right_a.shape[1], right_b.shape[1]

    def produce(block, terms, dst, base, span):
        lo, hi = span

        def part(left, right, begin, end, offset):
            def step(i, _):
                inner = pl.ds(pl.multiple_of(begin + i * 256, 128), 256)
                col = offset + begin + i * 256
                total = jnp.dot(
                    left[block], right[:, inner], preferred_element_type=jnp.float32
                )
                for term, first in terms:
                    total += term[:, pl.ds(pl.multiple_of(col - first, 128), 256)].astype(
                        jnp.float32
                    )
                dst[:, pl.ds(pl.multiple_of(col - base, 128), 256)] = total.astype(dst.dtype)
                return 0

            lax.fori_loop(0, (end - begin) // 256, step, 0)

        part(left_a, right_a, lo, min(hi, cols_a), 0)
        if hi > cols_a:
            part(left_b, right_b, 0, cols_b, cols_a)
            at = cols_a + cols_b
            total = extra[block].astype(jnp.float32)
            for term, first in terms:
                total += term[:, at - first : hi - first].astype(jnp.float32)
            dst[:, at - base : hi - base] = total.astype(dst.dtype)

    scatter_steps(
        n_dp,
        place_of(),
        lambda b, c: None,
        produce,
        lambda block: core_out.at[block // 2],
        out_ref,
        *scratch,
    )


def scatter_scratch(n_dp, rows, cols, dtype):
    line = n_dp // 4
    late = split_at(cols)
    return (
        [pltpu.VMEM((n_dp // 2, rows, cols), dtype)]
        + [pltpu.VMEM((line, rows, cols - late), dtype)] * 4
        + [pltpu.VMEM((2 * line, rows, late), dtype)] * 2
        + [pltpu.VMEM((2, rows, late), dtype)]
        + [pltpu.SemaphoreType.DMA((n_dp // 2,))] * 2
        + [pltpu.SemaphoreType.DMA((line,))] * 2
        + [pltpu.SemaphoreType.DMA((3 * line,))] * 4
        + [pltpu.SemaphoreType.DMA((1,))] * 2
    )


def scattered_products(left_a, right_a, left_b, right_b, extra, collective_id):
    n_dp, rows, _ = left_a.shape
    cols = right_a.shape[1] + right_b.shape[1] + extra.shape[2]
    return pl.pallas_call(
        functools.partial(product_kernel, n_dp),
        out_shape=jax.ShapeDtypeStruct((rows, cols), jnp.float32),
        in_specs=[pl.BlockSpec(memory_space=pltpu.VMEM)] * 5,
        out_specs=pl.BlockSpec(memory_space=pltpu.VMEM),
        scratch_shapes=[pltpu.VMEM((n_dp // 2, rows, cols), jnp.bfloat16)]
        + scatter_scratch(n_dp, rows, cols, jnp.bfloat16),
        compiler_params=pltpu.CompilerParams(
            collective_id=collective_id, has_side_effects=True
        ),
        cost_estimate=pl.CostEstimate(
            flops=0, bytes_accessed=200_000_000, transcendentals=0
        ),
    )(left_a, right_a, left_b, right_b, extra)


def scattered_dots(lefts, rights, collective_id):
    n_dp, rows, _ = lefts[0].shape
    cols = rights[0].shape[1]
    held = n_dp * (1 + 1 / 2 + 1) * rows * cols * 2
    pieces = 1
    while held > pieces * 36 * 2**20 or cols % (256 * pieces):
        pieces += 1
    width = cols // pieces
    return jnp.concatenate(
        [
            scattered_piece(
                lefts, [r[:, i * width : (i + 1) * width] for r in rights], collective_id
            )
            for i in range(pieces)
        ],
        axis=1,
    )


def scattered_piece(lefts, rights, collective_id):
    n_dp, rows, _ = lefts[0].shape
    cols = rights[0].shape[1]
    return pl.pallas_call(
        functools.partial(dots_kernel, n_dp, len(lefts)),
        out_shape=jax.ShapeDtypeStruct((rows, cols), jnp.float32),
        in_specs=[pl.BlockSpec(memory_space=pltpu.VMEM)] * (2 * len(lefts)),
        out_specs=pl.BlockSpec(memory_space=pltpu.VMEM),
        scratch_shapes=[pltpu.VMEM((n_dp, rows, cols), jnp.bfloat16)]
        + scatter_scratch(n_dp, rows, cols, jnp.bfloat16),
        compiler_params=pltpu.CompilerParams(
            collective_id=collective_id, has_side_effects=True
        ),
        cost_estimate=pl.CostEstimate(
            flops=0, bytes_accessed=150_000_000, transcendentals=0
        ),
    )(*lefts, *rights)


def row_major(x):
    return with_layout_constraint(x, Layout(major_to_minor=(0, 1)))


def mine_and_other(halves, seq_index):
    first = seq_index == 0
    return (
        jnp.where(first, halves[0], halves[1]),
        jnp.where(first, halves[1], halves[0]),
    )


def in_order(own, other, seq_index):
    first = seq_index == 0
    return jnp.where(first, own, other), jnp.where(first, other, own)


def column_halves(weight):
    q_cols, k_cols = HEADS * HEAD_DIM, KV_HEADS * HEAD_DIM
    starts = (0, q_cols, q_cols + k_cols, q_cols + 2 * k_cols)
    sizes = (q_cols // 2, k_cols // 2, k_cols // 2, q_cols // 2)
    return [
        jnp.concatenate(
            [weight[:, s + h * n : s + (h + 1) * n] for s, n in zip(starts, sizes)], axis=1
        )
        for h in range(2)
    ]


def layer(tokens, doc_lengths, attn_weight, ffn_weight, gains, out_grad):
    tok_rows = tokens.shape[0]
    n_dp = lax.axis_size("dp")
    heads, kv_heads = HEADS // 2, KV_HEADS // 2
    q_cols = heads * HEAD_DIM
    k_cols = kv_heads * HEAD_DIM
    proj_cols = q_cols + 2 * k_cols
    half_cols = proj_cols + q_cols
    group_size = HEADS // KV_HEADS
    query_scale = HEAD_DIM ** (-0.5)
    bf16 = jnp.bfloat16
    seq_index = lax.axis_index("seq")
    weight_rows = attn_weight.shape[0]

    run = jnp.arange(tok_rows, dtype=jnp.int32)
    places = jnp.concatenate([seq_index * tok_rows + run, (1 - seq_index) * tok_rows + run])
    docs, pos = doc_layout(doc_lengths[0], places)
    allowed = key_mask(places, docs, places, docs)

    gain_cols = jnp.pad(gains, ((0, 0), (0, 124)))
    my_cols, other_cols = mine_and_other(column_halves(attn_weight), seq_index)
    my_cols = jnp.concatenate([my_cols, gain_cols], axis=1)
    other_cols = jnp.concatenate([other_cols, gain_cols], axis=1)
    partner_cols = swapped(other_cols)
    other_tokens = swapped(tokens)
    ffn_own, partner_cols = lax.optimization_barrier((ffn_weight, partner_cols))
    ffn_other = swapped(ffn_own)
    block = jnp.concatenate(in_order(my_cols, partner_cols, seq_index), axis=0)
    attn_full = gathered(block, n_dp, 0).reshape(-1, half_cols + 128)
    gain_vals = attn_full[:, half_cols : half_cols + 4].astype(jnp.float32).T
    attn_weights = attn_full[:, :proj_cols]
    out_weights = attn_full[:, proj_cols:half_cols]

    pack_tokens = jnp.concatenate([tokens, other_tokens]).astype(jnp.float32)
    tokens_f = tokens.astype(jnp.float32)
    attn_in = rms_norm(pack_tokens, gain_vals[0]).astype(bf16)
    projected = jnp.dot(attn_in, attn_weights, preferred_element_type=jnp.float32)
    pack = 2 * tok_rows
    queries = (
        rotate(projected[:, :q_cols].reshape(pack, heads, HEAD_DIM), pos) * query_scale
    ).astype(bf16)
    queries = queries.reshape(pack, kv_heads, group_size, HEAD_DIM)
    keys = rotate(
        projected[:, q_cols : q_cols + k_cols].reshape(pack, kv_heads, HEAD_DIM), pos
    ).astype(bf16)
    values = projected[:, q_cols + k_cols :].reshape(pack, kv_heads, HEAD_DIM).astype(bf16)
    scores, capped = attn_scores(queries, keys, allowed)
    row_max = jnp.max(capped, axis=-1, keepdims=True)
    exp_terms = jnp.exp(capped - row_max)
    row_total = jnp.sum(exp_terms, axis=-1, keepdims=True)
    log_total = row_max + jnp.log(row_total)
    attn_probs = (exp_terms / row_total).astype(bf16)
    mixed_heads = jnp.einsum(
        "kgqp,pkd->qkgd", attn_probs, values, preferred_element_type=jnp.float32
    )
    mixed_heads = mixed_heads.reshape(pack, q_cols).astype(bf16)
    attn_part_out = contract_cols(mixed_heads, out_weights)
    attn_part_other = swapped(attn_part_out[tok_rows:].astype(bf16))
    attn_out = attn_part_out[:tok_rows] + attn_part_other.astype(jnp.float32)
    middle = tokens_f + rms_norm(attn_out, gain_vals[1])
    ffn_input = rms_norm(middle, gain_vals[2]).astype(bf16)

    gate_weights, up_weights, down_weights = [
        jnp.concatenate([ffn_own[:, k * D : (k + 1) * D], ffn_other[:, k * D : (k + 1) * D]])
        for k in range(3)
    ]
    unit_count = gate_weights.shape[0]
    ffn_all = gathered(ffn_input, n_dp, 1).reshape(-1, D)
    gate = contract_cols(ffn_all, gate_weights)
    up = contract_cols(ffn_all, up_weights)
    hidden = row_major(gated_gelu(gate, up).astype(bf16))
    ffn_out = scattered_dots([hidden.reshape(n_dp, tok_rows, -1)], [down_weights], 2)
    out_gain = gain_vals[3]
    block_out = (middle + rms_norm(ffn_out, out_gain)).astype(bf16)
    cotangent = out_grad.astype(jnp.float32)
    d_ffn_f, d_gain_out = norm_back(ffn_out, out_gain, cotangent)
    d_ffn_all = gathered(d_ffn_f.astype(bf16), n_dp, 1).reshape(-1, D)
    d_hidden = contract_cols(d_ffn_all, down_weights)
    d_gate, d_up = jax.vjp(gated_gelu, gate, up)[1](d_hidden)
    d_gate, d_up = row_major(d_gate.astype(bf16)), row_major(d_up.astype(bf16))
    d_ffn_input = scattered_dots(
        [d_gate.reshape(n_dp, tok_rows, -1), d_up.reshape(n_dp, tok_rows, -1)],
        [gate_weights, up_weights],
        4,
    )

    own_units = unit_count // 2
    weight_sum = [
        contract_rows(d_gate, ffn_all),
        contract_rows(d_up, ffn_all),
        contract_rows(hidden, d_ffn_all),
    ]
    sent = jnp.concatenate([w[own_units:].astype(bf16) for w in weight_sum], axis=1)
    kept = jnp.concatenate([w[:own_units] for w in weight_sum], axis=1)
    grad_other = swapped(sent)
    ffn_weight_grad = kept + grad_other.astype(jnp.float32)

    d_middle_add, d_gain_ffn = norm_back(middle, gain_vals[2], d_ffn_input)
    d_middle = cotangent + d_middle_add
    d_attn_f, d_gain_post = norm_back(attn_out, gain_vals[1], d_middle)
    d_attn_own = d_attn_f.astype(bf16)
    d_attn_other = swapped(d_attn_own)
    d_attn = jnp.concatenate([d_attn_own, d_attn_other])
    d_mixed = jnp.dot(d_attn, out_weights, preferred_element_type=jnp.float32).astype(bf16)
    d_mixed = d_mixed.reshape(pack, kv_heads, group_size, HEAD_DIM)
    attn_p = jnp.exp(capped - log_total)
    d_probs = jnp.einsum("qkgd,pkd->kgqp", d_mixed, values, preferred_element_type=jnp.float32)
    d_values = jnp.einsum(
        "kgqp,qkgd->pkd", attn_probs, d_mixed, preferred_element_type=jnp.float32
    )
    d_capped = attn_p * (d_probs - jnp.sum(attn_p * d_probs, axis=-1, keepdims=True))
    tanh_part = jnp.tanh(scores / soft_cap)
    d_scores = (d_capped * (1.0 - tanh_part * tanh_part)).astype(bf16)
    d_queries = jnp.einsum("kgqp,pkd->qkgd", d_scores, keys, preferred_element_type=jnp.float32)
    d_keys = jnp.einsum("kgqp,qkgd->pkd", d_scores, queries, preferred_element_type=jnp.float32)
    d_query_raw = rotate(d_queries.reshape(pack, heads, HEAD_DIM) * query_scale, -pos)
    d_key_raw = rotate(d_keys, -pos)
    d_projected = jnp.concatenate(
        [
            d_query_raw.reshape(pack, q_cols),
            d_key_raw.reshape(pack, k_cols),
            d_values.reshape(pack, k_cols),
        ],
        axis=1,
    ).astype(bf16)
    d_attn_in_part = contract_cols(d_projected, attn_weights)
    d_attn_in_other = swapped(d_attn_in_part[tok_rows:].astype(bf16))
    d_attn_in = d_attn_in_part[:tok_rows] + d_attn_in_other.astype(jnp.float32)
    normed = pack_tokens * lax.rsqrt(
        jnp.mean(pack_tokens * pack_tokens, axis=-1, keepdims=True) + eps_norm
    )
    d_gain_in = jnp.sum(d_attn_in_part * normed, axis=0)

    gain_part = jnp.stack([d_gain_in, d_gain_post, d_gain_ffn, d_gain_out], axis=1)
    block_rows = (n_dp, 2 * weight_rows)
    attn_sum = scattered_products(
        attn_in.T.reshape(*block_rows, pack),
        d_projected,
        d_attn.T.reshape(*block_rows, pack),
        mixed_heads,
        jnp.pad(gain_part.astype(bf16), ((0, 0), (0, 124))).reshape(*block_rows, 128),
        3,
    )
    d_tokens_add = norm_back(tokens_f, gain_vals[0], d_attn_in)[0]
    tokens_grad = d_middle + d_tokens_add
    mine, others = mine_and_other(
        (attn_sum[:weight_rows], attn_sum[weight_rows:]), seq_index
    )
    partner = swapped(others.astype(bf16)).astype(jnp.float32)
    gains_grad = mine[:, half_cols : half_cols + 4] + partner[:, half_cols : half_cols + 4]
    first, second = in_order(mine, partner, seq_index)
    cuts = ((0, q_cols), (q_cols, q_cols + k_cols), (q_cols + k_cols, proj_cols),
            (proj_cols, half_cols))
    attn_weight_grad = jnp.concatenate(
        [half[:, lo:hi] for lo, hi in cuts for half in (first, second)], axis=1
    )
    return (block_out, tokens_grad, attn_weight_grad, ffn_weight_grad, gains_grad)


def solution(mesh):
    return jax.shard_map(
        layer,
        mesh=mesh,
        in_specs=(
            P(("dp", "seq"), None),
            P("dp", None),
            P(("dp", "seq"), None),
            P(("dp", "seq"), None),
            P(("dp", "seq"), None),
            P(("dp", "seq"), None),
        ),
        out_specs=(
            P(("dp", "seq"), None),
            P(("dp", "seq"), None),
            P(("dp", "seq"), None),
            P(("dp", "seq"), None),
            P(("dp", "seq"), None),
        ),
        check_vma=False,
    )
```

```python
import functools
import math

import jax
import jax.numpy as jnp
from jax import lax
from jax.experimental.layout import Layout, with_layout_constraint
from jax.experimental import pallas as pl
from jax.experimental.pallas import tpu as pltpu
from jax.sharding import PartitionSpec as P

D = 2304
HEADS = 8
KV_HEADS = 4
HEAD_DIM = 256
WINDOW = 128


soft_cap = 50.0
eps_norm = 1e-06
rope_base = 10000.0
gelu_coef = math.sqrt(2.0 / math.pi)


MESH = pl.DeviceIdType.MESH


def gelu_tanh(value):
    return 0.5 * value * (1.0 + jnp.tanh(gelu_coef * (value + 0.044715 * value * value * value)))


def gated_gelu(gate_pre, up_pre):
    return gelu_tanh(gate_pre) * up_pre


def rms_norm(value, gain_vec):
    return value * lax.rsqrt(jnp.mean(value * value, axis=-1, keepdims=True) + eps_norm) * gain_vec


def norm_back(value, gain_vec, incoming):
    return jax.vjp(rms_norm, value, gain_vec)[1](incoming)


def doc_layout(lengths, places):
    doc_ends = jnp.cumsum(lengths, dtype=jnp.int32)
    starts = doc_ends - lengths
    doc_ids = jnp.sum(
        (places[:, None] >= doc_ends[None, :]).astype(jnp.int32), axis=1, dtype=jnp.int32
    )
    onehot = doc_ids[:, None] == jnp.arange(lengths.shape[0], dtype=jnp.int32)[None, :]
    doc_first = jnp.sum(jnp.where(onehot, starts[None, :], 0), axis=1, dtype=jnp.int32)
    return (doc_ids, places - doc_first)


def rotate(value, doc_pos):
    half_dim = value.shape[-1] // 2
    frequency = rope_base ** (-2.0 * jnp.arange(half_dim, dtype=jnp.float32) / value.shape[-1])
    angles = doc_pos.astype(jnp.float32)[:, None] * frequency[None, :]
    cosine = jnp.cos(angles)[:, None, :]
    sine_part = jnp.sin(angles)[:, None, :]
    first_half = value[..., :half_dim]
    second_half = value[..., half_dim:]
    return jnp.concatenate(
        [
            first_half * cosine - second_half * sine_part,
            second_half * cosine + first_half * sine_part,
        ],
        axis=-1,
    )


def contract_rows(left_side, right_side):
    return lax.dot_general(
        left_side, right_side, (((0,), (0,)), ((), ())), preferred_element_type=jnp.float32
    )


def contract_cols(left_side, right_side):
    return lax.dot_general(
        left_side, right_side, (((1,), (1,)), ((), ())), preferred_element_type=jnp.float32
    )


def key_mask(query_places, query_docs, key_places, key_docs):
    return (
        (key_places[None, :] >= 0)
        & (query_docs[:, None] == key_docs[None, :])
        & (key_places[None, :] <= query_places[:, None])
        & (query_places[:, None] - key_places[None, :] < WINDOW)
    )


def attn_scores(queries, all_keys, allowed):
    scores = jnp.einsum("qkgd,pkd->kgqp", queries, all_keys, preferred_element_type=jnp.float32)
    capped = jnp.where(allowed[None, None], soft_cap * jnp.tanh(scores / soft_cap), -1e30)
    return (scores, capped)


def swapped(x):
    return lax.ppermute(x, "seq", [(0, 1), (1, 0)])


def place_of():
    dp = lax.axis_index("dp")
    seq = lax.axis_index("seq")
    a, b, c = dp // 4, lax.rem(dp // 2, 2), lax.rem(dp, 2)
    return a, b, c, seq


def number(a, b, c):
    return (a * 2 + b) * 2 + c


def enter(line, a, b, c, seq):
    barrier = pltpu.get_barrier_semaphore()

    def tell(a2, b2, c2):
        pl.semaphore_signal(
            barrier, inc=1, device_id=(number(a2, b2, c2), seq), device_id_type=MESH
        )

    tell(a, b, 1 - c)
    tell(a, 1 - b, c)

    @pl.when(a > 0)
    def _():
        tell(a - 1, b, c)

    @pl.when(a < line - 1)
    def _():
        tell(a + 1, b, c)

    peers = 2 + jnp.minimum(a, 1) + jnp.minimum(line - 1 - a, 1)
    pl.semaphore_wait(barrier, peers)


def split_at(cols):
    return cols // 768 * 128


def gather_kernel(n_dp, x_ref, out_ref, own_sem, send_sem, recv_sem):
    line = n_dp // 4
    a, b, c, seq = place_of()
    me, pair = number(a, b, c), number(a, 1 - b, c)
    cols = x_ref.shape[1]
    late = split_at(cols)
    spans = (pl.ds(late, cols - late), pl.ds(0, late))
    own = pltpu.make_async_copy(x_ref, out_ref.at[me], own_sem)
    own.start()
    enter(line, a, b, c, seq)

    def copy(way, block, piece, own=False):
        a2 = a + (1 if way == 0 else -1 if way == 1 else 0)
        b2 = 1 - b if way == 2 else b
        c2 = 1 - c if way == 3 else c
        there = out_ref.at[block, :, spans[piece]]
        return pltpu.make_async_remote_copy(
            src_ref=x_ref.at[:, spans[piece]] if own else there,
            dst_ref=there,
            send_sem=send_sem.at[way, block, piece],
            recv_sem=recv_sem.at[block, piece],
            device_id=(number(a2, b2, c2), seq),
            device_id_type=MESH,
        )

    up, down, across, over = range(4)
    has_up, has_down = a < line - 1, a > 0

    def start(way, block, piece, own=False):
        if way in (up, down):

            @pl.when(has_up if way == up else has_down)
            def _():
                copy(way, block, piece, own).start()

        else:
            copy(way, block, piece, own).start()

    def pass_on(block, piece, ways):
        copy(over, block, piece).wait_recv()
        for way in ways:
            start(way, block, piece)

    for way, piece in ((up, 0), (down, 0), (across, 1), (across, 0), (over, 0), (over, 1)):
        start(way, me, piece, own=True)

    def each_at(k, act):
        for sign, way in ((-1, up), (1, down)) if k else ((1, over),):

            @pl.when((a + sign * k >= 0) & (a + sign * k < line))
            def _(sign=sign, way=way):
                act(a + sign * k, way)

    pass_on(pair, 1, (over,))

    def after(k):
        for way, last in ((up, a == k), (down, line - 1 - a == k)):

            @pl.when(last)
            def _(way=way):
                start(way, me, 1, own=True)
                start(way, pair, 1)

    def from_pair(k):
        each_at(k, lambda i, way: pass_on(number(i, 1 - b, c), 0, (over,)))

    after(0)
    for k in range(1, line):
        each_at(k, lambda i, way: pass_on(number(i, b, c), 0, (way, across, over)))
        after(k)
    half = line // 2
    for k in range(half):
        from_pair(k)
    for k in range(1, line):
        for b2 in (b, 1 - b):
            each_at(k, lambda i, way, b2=b2: pass_on(number(i, b2, c), 1, (way, over)))
    for k in range(half, line):
        from_pair(k)

    for other in range(n_dp // 2):
        for piece in range(2):
            copy(over, other * 2 + 1 - c, piece).wait_recv()

    own.wait()
    copy(across, me, 1).wait_send()
    for i in range(line):
        near, far = number(i, b, c), number(i, 1 - b, c)
        copy(across, near, 0).wait_send()
        for block, piece in ((near, 0), (near, 1), (far, 0), (far, 1)):
            copy(over, block, piece).wait_send()
        for block, piece in ((near, 0), (near, 1), (far, 1)):

            @pl.when(has_up & (i <= a))
            def _(block=block, piece=piece):
                copy(up, block, piece).wait_send()

            @pl.when(has_down & (i >= a))
            def _(block=block, piece=piece):
                copy(down, block, piece).wait_send()


def gathered(x, n_dp, collective_id):
    return pl.pallas_call(
        functools.partial(gather_kernel, n_dp),
        out_shape=jax.ShapeDtypeStruct((n_dp, *x.shape), x.dtype),
        in_specs=[pl.BlockSpec(memory_space=pltpu.VMEM)],
        out_specs=pl.BlockSpec(memory_space=pl.ANY),
        scratch_shapes=[
            pltpu.SemaphoreType.DMA,
            pltpu.SemaphoreType.DMA((4, n_dp, 2)),
            pltpu.SemaphoreType.DMA((n_dp, 2)),
        ],
        compiler_params=pltpu.CompilerParams(
            collective_id=collective_id, has_side_effects=True
        ),
        cost_estimate=pl.CostEstimate(
            flops=0, bytes_accessed=150_000_000, transcendentals=0
        ),
    )(x)


def scatter_steps(n_dp, place, prepare, produce, core_source, out_ref, from_core, from_pair, up_buf,
                  down_buf, pair_out, core_send, core_recv, pair_send, pair_recv, up_send,
                  up_recv, down_send, down_recv):
    line = n_dp // 4
    a, b, c, seq = place
    enter(line, a, b, c, seq)

    def core_copy(block):
        half = block // 2
        return pltpu.make_async_remote_copy(
            src_ref=core_source(block),
            dst_ref=from_core.at[half],
            send_sem=core_send.at[half],
            recv_sem=core_recv.at[half],
            device_id=(number(a, b, 1 - c), seq),
            device_id_type=MESH,
        )

    def pair_copy(to):
        return pltpu.make_async_remote_copy(
            src_ref=pair_out.at[to],
            dst_ref=from_pair.at[to],
            send_sem=pair_send.at[to],
            recv_sem=pair_recv.at[to],
            device_id=(number(a, 1 - b, c), seq),
            device_id_type=MESH,
        )

    def up_copy(to):
        return pltpu.make_async_remote_copy(
            src_ref=up_buf.at[to],
            dst_ref=up_buf.at[to],
            send_sem=up_send.at[to],
            recv_sem=up_recv.at[to],
            device_id=(number(a + 1, b, c), seq),
            device_id_type=MESH,
        )

    def down_copy(to):
        return pltpu.make_async_remote_copy(
            src_ref=down_buf.at[to],
            dst_ref=down_buf.at[to],
            send_sem=down_send.at[to],
            recv_sem=down_recv.at[to],
            device_id=(number(a - 1, b, c), seq),
            device_id_type=MESH,
        )

    def each_target(act):
        for k in range(line - 1, 0, -1):

            @pl.when(a + k < line)
            def _(k=k):
                act(a + k, 1)

            @pl.when(a - k >= 0)
            def _(k=k):
                act(a - k, -1)

        act(a, 0)

    def send_core(block):
        produce(block, None, core_source(block))
        core_copy(block).start()

    prepare(1 - b, 1 - c)
    each_target(lambda to, way: send_core(number(to, 1 - b, 1 - c)))
    prepare(1 - b, c)

    def send_pair(to, way):
        block = number(to, 1 - b, c)
        core_copy(block).wait_recv()
        produce(block, [from_core.at[block // 2]], pair_out.at[to])
        pair_copy(to).start()

    each_target(send_pair)
    prepare(b, 1 - c)
    each_target(lambda to, way: send_core(number(to, b, 1 - c)))
    prepare(b, c)

    def line_sum(to, more, dst):
        block = number(to, b, c)
        produce(block, [from_core.at[block // 2], from_pair.at[to], *more], dst)

    def send_line(to, way):
        core_copy(number(to, b, c)).wait_recv()
        pair_copy(to).wait_recv()
        if way:
            buf, copy = (up_buf, up_copy) if way == 1 else (down_buf, down_copy)
            at_end = (a == 0) if way == 1 else (a == line - 1)

            @pl.when(at_end)
            def _():
                line_sum(to, [], buf.at[to])

            @pl.when(jnp.logical_not(at_end))
            def _():
                copy(to).wait_recv()
                line_sum(to, [buf.at[to]], buf.at[to])

            copy(to).start()
        else:
            line_sum(to, [], out_ref)
            for copy, buf, there in (
                (up_copy, up_buf, a > 0),
                (down_copy, down_buf, a < line - 1),
            ):

                @pl.when(there)
                def _(copy=copy, buf=buf):
                    copy(to).wait_recv()
                    add_rows(out_ref, buf.at[to])

    each_target(send_line)

    for i in range(n_dp // 2):
        core_copy(i * 2 + 1 - c).wait_send()
    for i in range(line):
        pair_copy(i).wait_send()

        @pl.when(i > a)
        def _(i=i):
            up_copy(i).wait_send()

        @pl.when(i < a)
        def _(i=i):
            down_copy(i).wait_send()


def row_tiles(rows):
    return 16 if rows % 16 == 0 else rows


def add_rows(out_ref, term):
    tile = row_tiles(out_ref.shape[0])

    def step(i, _):
        at = pl.ds(pl.multiple_of(i * tile, tile), tile)
        out_ref[at, :] += term[at, :].astype(jnp.float32)
        return 0

    lax.fori_loop(0, out_ref.shape[0] // tile, step, 0)


def dots_kernel(n_dp, n_terms, *refs):
    lefts, rights = refs[:n_terms], refs[n_terms : 2 * n_terms]
    out_ref, parts, *scratch = refs[2 * n_terms :]
    _, rows, cols = parts.shape
    f32 = jnp.float32

    def prepare(b, c):
        for first in range(0, n_dp // 4, 4):
            blocks = [number(first + i, b, c) for i in range(4)]

            def step(j, _):
                at = pl.ds(pl.multiple_of(j * 256, 256), 256)
                total = jnp.zeros((4 * rows, 256), f32)
                for left, right in zip(lefts, rights):
                    stacked = jnp.concatenate([left[k] for k in blocks], axis=0)
                    total += jnp.dot(stacked, right[:, at], preferred_element_type=f32)
                for i, k in enumerate(blocks):
                    parts[k, :, at] = total[i * rows : (i + 1) * rows].astype(parts.dtype)
                return 0

            lax.fori_loop(0, cols // 256, step, 0)

    def produce(block, terms, dst):
        if terms is None:
            return
        tile = row_tiles(rows)

        def step(i, _):
            at = pl.ds(pl.multiple_of(i * tile, tile), tile)
            total = parts[block, at, :].astype(f32)
            for term in terms:
                total += term[at, :].astype(f32)
            dst[at, :] = total.astype(dst.dtype)
            return 0

        lax.fori_loop(0, rows // tile, step, 0)

    scatter_steps(
        n_dp, place_of(), prepare, produce, lambda block: parts.at[block], out_ref, *scratch
    )


def product_kernel(n_dp, left_a, right_a, left_b, right_b, extra, out_ref, core_out, *scratch):
    cols_a, cols_b = right_a.shape[1], right_b.shape[1]

    def produce(block, terms, dst):
        def part(left, right, first, wide):
            def step(i, _):
                inner = pl.ds(pl.multiple_of(i * wide, wide), wide)
                outer = pl.ds(pl.multiple_of(first + i * wide, 128), wide)
                total = jnp.dot(
                    left[block], right[:, inner], preferred_element_type=jnp.float32
                )
                for term in terms or []:
                    total += term[:, outer].astype(jnp.float32)
                dst[:, outer] = total.astype(dst.dtype)
                return 0

            lax.fori_loop(0, right.shape[1] // wide, step, 0)

        part(left_a, right_a, 0, 256)
        part(left_b, right_b, cols_a, 256)
        last = pl.ds(cols_a + cols_b, extra.shape[2])
        total = extra[block].astype(jnp.float32)
        for term in terms or []:
            total += term[:, last].astype(jnp.float32)
        dst[:, last] = total.astype(dst.dtype)

    scatter_steps(
        n_dp,
        place_of(),
        lambda b, c: None,
        produce,
        lambda block: core_out.at[block // 2],
        out_ref,
        *scratch,
    )


def scatter_scratch(n_dp, rows, cols, dtype):
    line = n_dp // 4
    return (
        [pltpu.VMEM((n_dp // 2, rows, cols), dtype)]
        + [pltpu.VMEM((line, rows, cols), dtype)] * 4
        + [pltpu.SemaphoreType.DMA((n_dp // 2,))] * 2
        + [pltpu.SemaphoreType.DMA((line,))] * 6
    )


def scattered_products(left_a, right_a, left_b, right_b, extra, collective_id):
    n_dp, rows, _ = left_a.shape
    cols = right_a.shape[1] + right_b.shape[1] + extra.shape[2]
    return pl.pallas_call(
        functools.partial(product_kernel, n_dp),
        out_shape=jax.ShapeDtypeStruct((rows, cols), jnp.float32),
        in_specs=[pl.BlockSpec(memory_space=pltpu.VMEM)] * 5,
        out_specs=pl.BlockSpec(memory_space=pltpu.VMEM),
        scratch_shapes=[pltpu.VMEM((n_dp // 2, rows, cols), jnp.bfloat16)]
        + scatter_scratch(n_dp, rows, cols, jnp.bfloat16),
        compiler_params=pltpu.CompilerParams(
            collective_id=collective_id, has_side_effects=True
        ),
        cost_estimate=pl.CostEstimate(
            flops=0, bytes_accessed=200_000_000, transcendentals=0
        ),
    )(left_a, right_a, left_b, right_b, extra)


def scattered_dots(lefts, rights, collective_id):
    n_dp, rows, _ = lefts[0].shape
    cols = rights[0].shape[1]
    held = n_dp * (1 + 1 / 2 + 1) * rows * cols * 2
    pieces = 1
    while held > pieces * 36 * 2**20 or cols % (256 * pieces):
        pieces += 1
    width = cols // pieces
    return jnp.concatenate(
        [
            scattered_piece(
                lefts, [r[:, i * width : (i + 1) * width] for r in rights], collective_id
            )
            for i in range(pieces)
        ],
        axis=1,
    )


def scattered_piece(lefts, rights, collective_id):
    n_dp, rows, _ = lefts[0].shape
    cols = rights[0].shape[1]
    return pl.pallas_call(
        functools.partial(dots_kernel, n_dp, len(lefts)),
        out_shape=jax.ShapeDtypeStruct((rows, cols), jnp.float32),
        in_specs=[pl.BlockSpec(memory_space=pltpu.VMEM)] * (2 * len(lefts)),
        out_specs=pl.BlockSpec(memory_space=pltpu.VMEM),
        scratch_shapes=[pltpu.VMEM((n_dp, rows, cols), jnp.bfloat16)]
        + scatter_scratch(n_dp, rows, cols, jnp.bfloat16),
        compiler_params=pltpu.CompilerParams(
            collective_id=collective_id, has_side_effects=True
        ),
        cost_estimate=pl.CostEstimate(
            flops=0, bytes_accessed=150_000_000, transcendentals=0
        ),
    )(*lefts, *rights)


def row_major(x):
    return with_layout_constraint(x, Layout(major_to_minor=(0, 1)))


def mine_and_other(halves, seq_index):
    first = seq_index == 0
    return (
        jnp.where(first, halves[0], halves[1]),
        jnp.where(first, halves[1], halves[0]),
    )


def in_order(own, other, seq_index):
    first = seq_index == 0
    return jnp.where(first, own, other), jnp.where(first, other, own)


def column_halves(weight):
    q_cols, k_cols = HEADS * HEAD_DIM, KV_HEADS * HEAD_DIM
    starts = (0, q_cols, q_cols + k_cols, q_cols + 2 * k_cols)
    sizes = (q_cols // 2, k_cols // 2, k_cols // 2, q_cols // 2)
    return [
        jnp.concatenate(
            [weight[:, s + h * n : s + (h + 1) * n] for s, n in zip(starts, sizes)], axis=1
        )
        for h in range(2)
    ]


def layer(tokens, doc_lengths, attn_weight, ffn_weight, gains, out_grad):
    tok_rows = tokens.shape[0]
    n_dp = lax.axis_size("dp")
    heads, kv_heads = HEADS // 2, KV_HEADS // 2
    q_cols = heads * HEAD_DIM
    k_cols = kv_heads * HEAD_DIM
    proj_cols = q_cols + 2 * k_cols
    half_cols = proj_cols + q_cols
    group_size = HEADS // KV_HEADS
    query_scale = HEAD_DIM ** (-0.5)
    bf16 = jnp.bfloat16
    seq_index = lax.axis_index("seq")
    weight_rows = attn_weight.shape[0]

    run = jnp.arange(tok_rows, dtype=jnp.int32)
    places = jnp.concatenate([seq_index * tok_rows + run, (1 - seq_index) * tok_rows + run])
    docs, pos = doc_layout(doc_lengths[0], places)
    allowed = key_mask(places, docs, places, docs)

    gain_cols = jnp.pad(gains, ((0, 0), (0, 124)))
    my_cols, other_cols = mine_and_other(column_halves(attn_weight), seq_index)
    my_cols = jnp.concatenate([my_cols, gain_cols], axis=1)
    other_cols = jnp.concatenate([other_cols, gain_cols], axis=1)
    partner_cols = swapped(other_cols)
    other_tokens = swapped(tokens)
    ffn_own, partner_cols = lax.optimization_barrier((ffn_weight, partner_cols))
    ffn_other = swapped(ffn_own)
    block = jnp.concatenate(in_order(my_cols, partner_cols, seq_index), axis=0)
    attn_full = gathered(block, n_dp, 0).reshape(-1, half_cols + 128)
    gain_vals = attn_full[:, half_cols : half_cols + 4].astype(jnp.float32).T
    attn_weights = attn_full[:, :proj_cols]
    out_weights = attn_full[:, proj_cols:half_cols]

    pack_tokens = jnp.concatenate([tokens, other_tokens]).astype(jnp.float32)
    tokens_f = tokens.astype(jnp.float32)
    attn_in = rms_norm(pack_tokens, gain_vals[0]).astype(bf16)
    projected = jnp.dot(attn_in, attn_weights, preferred_element_type=jnp.float32)
    pack = 2 * tok_rows
    queries = (
        rotate(projected[:, :q_cols].reshape(pack, heads, HEAD_DIM), pos) * query_scale
    ).astype(bf16)
    queries = queries.reshape(pack, kv_heads, group_size, HEAD_DIM)
    keys = rotate(
        projected[:, q_cols : q_cols + k_cols].reshape(pack, kv_heads, HEAD_DIM), pos
    ).astype(bf16)
    values = projected[:, q_cols + k_cols :].reshape(pack, kv_heads, HEAD_DIM).astype(bf16)
    scores, capped = attn_scores(queries, keys, allowed)
    row_max = jnp.max(capped, axis=-1, keepdims=True)
    exp_terms = jnp.exp(capped - row_max)
    row_total = jnp.sum(exp_terms, axis=-1, keepdims=True)
    log_total = row_max + jnp.log(row_total)
    attn_probs = (exp_terms / row_total).astype(bf16)
    mixed_heads = jnp.einsum(
        "kgqp,pkd->qkgd", attn_probs, values, preferred_element_type=jnp.float32
    )
    mixed_heads = mixed_heads.reshape(pack, q_cols).astype(bf16)
    attn_part_out = contract_cols(mixed_heads, out_weights)
    attn_part_other = swapped(attn_part_out[tok_rows:].astype(bf16))
    attn_out = attn_part_out[:tok_rows] + attn_part_other.astype(jnp.float32)
    middle = tokens_f + rms_norm(attn_out, gain_vals[1])
    ffn_input = rms_norm(middle, gain_vals[2]).astype(bf16)

    gate_weights, up_weights, down_weights = [
        jnp.concatenate([ffn_own[:, k * D : (k + 1) * D], ffn_other[:, k * D : (k + 1) * D]])
        for k in range(3)
    ]
    unit_count = gate_weights.shape[0]
    ffn_all = gathered(ffn_input, n_dp, 1).reshape(-1, D)
    gate = contract_cols(ffn_all, gate_weights)
    up = contract_cols(ffn_all, up_weights)
    hidden = row_major(gated_gelu(gate, up).astype(bf16))
    ffn_out = scattered_dots([hidden.reshape(n_dp, tok_rows, -1)], [down_weights], 2)
    out_gain = gain_vals[3]
    block_out = (middle + rms_norm(ffn_out, out_gain)).astype(bf16)
    cotangent = out_grad.astype(jnp.float32)
    d_ffn_f, d_gain_out = norm_back(ffn_out, out_gain, cotangent)
    d_ffn_all = gathered(d_ffn_f.astype(bf16), n_dp, 1).reshape(-1, D)
    d_hidden = contract_cols(d_ffn_all, down_weights)
    d_gate, d_up = jax.vjp(gated_gelu, gate, up)[1](d_hidden)
    d_gate, d_up = row_major(d_gate.astype(bf16)), row_major(d_up.astype(bf16))
    d_ffn_input = scattered_dots(
        [d_gate.reshape(n_dp, tok_rows, -1), d_up.reshape(n_dp, tok_rows, -1)],
        [gate_weights, up_weights],
        4,
    )

    own_units = unit_count // 2
    weight_sum = [
        contract_rows(d_gate, ffn_all),
        contract_rows(d_up, ffn_all),
        contract_rows(hidden, d_ffn_all),
    ]
    sent = jnp.concatenate([w[own_units:].astype(bf16) for w in weight_sum], axis=1)
    kept = jnp.concatenate([w[:own_units] for w in weight_sum], axis=1)
    grad_other = swapped(sent)
    ffn_weight_grad = kept + grad_other.astype(jnp.float32)

    d_middle_add, d_gain_ffn = norm_back(middle, gain_vals[2], d_ffn_input)
    d_middle = cotangent + d_middle_add
    d_attn_f, d_gain_post = norm_back(attn_out, gain_vals[1], d_middle)
    d_attn_own = d_attn_f.astype(bf16)
    d_attn_other = swapped(d_attn_own)
    d_attn = jnp.concatenate([d_attn_own, d_attn_other])
    d_mixed = jnp.dot(d_attn, out_weights, preferred_element_type=jnp.float32).astype(bf16)
    d_mixed = d_mixed.reshape(pack, kv_heads, group_size, HEAD_DIM)
    attn_p = jnp.exp(capped - log_total)
    d_probs = jnp.einsum("qkgd,pkd->kgqp", d_mixed, values, preferred_element_type=jnp.float32)
    d_values = jnp.einsum(
        "kgqp,qkgd->pkd", attn_probs, d_mixed, preferred_element_type=jnp.float32
    )
    d_capped = attn_p * (d_probs - jnp.sum(attn_p * d_probs, axis=-1, keepdims=True))
    tanh_part = jnp.tanh(scores / soft_cap)
    d_scores = (d_capped * (1.0 - tanh_part * tanh_part)).astype(bf16)
    d_queries = jnp.einsum("kgqp,pkd->qkgd", d_scores, keys, preferred_element_type=jnp.float32)
    d_keys = jnp.einsum("kgqp,qkgd->pkd", d_scores, queries, preferred_element_type=jnp.float32)
    d_query_raw = rotate(d_queries.reshape(pack, heads, HEAD_DIM) * query_scale, -pos)
    d_key_raw = rotate(d_keys, -pos)
    d_projected = jnp.concatenate(
        [
            d_query_raw.reshape(pack, q_cols),
            d_key_raw.reshape(pack, k_cols),
            d_values.reshape(pack, k_cols),
        ],
        axis=1,
    ).astype(bf16)
    d_attn_in_part = contract_cols(d_projected, attn_weights)
    d_attn_in_other = swapped(d_attn_in_part[tok_rows:].astype(bf16))
    d_attn_in = d_attn_in_part[:tok_rows] + d_attn_in_other.astype(jnp.float32)
    normed = pack_tokens * lax.rsqrt(
        jnp.mean(pack_tokens * pack_tokens, axis=-1, keepdims=True) + eps_norm
    )
    d_gain_in = jnp.sum(d_attn_in_part * normed, axis=0)

    gain_part = jnp.stack([d_gain_in, d_gain_post, d_gain_ffn, d_gain_out], axis=1)
    block_rows = (n_dp, 2 * weight_rows)
    attn_sum = scattered_products(
        attn_in.T.reshape(*block_rows, pack),
        d_projected,
        d_attn.T.reshape(*block_rows, pack),
        mixed_heads,
        jnp.pad(gain_part.astype(bf16), ((0, 0), (0, 124))).reshape(*block_rows, 128),
        3,
    )
    d_tokens_add = norm_back(tokens_f, gain_vals[0], d_attn_in)[0]
    tokens_grad = d_middle + d_tokens_add
    mine, others = mine_and_other(
        (attn_sum[:weight_rows], attn_sum[weight_rows:]), seq_index
    )
    partner = swapped(others.astype(bf16)).astype(jnp.float32)
    gains_grad = mine[:, half_cols : half_cols + 4] + partner[:, half_cols : half_cols + 4]
    first, second = in_order(mine, partner, seq_index)
    cuts = ((0, q_cols), (q_cols, q_cols + k_cols), (q_cols + k_cols, proj_cols),
            (proj_cols, half_cols))
    attn_weight_grad = jnp.concatenate(
        [half[:, lo:hi] for lo, hi in cuts for half in (first, second)], axis=1
    )
    return (block_out, tokens_grad, attn_weight_grad, ffn_weight_grad, gains_grad)


def solution(mesh):
    return jax.shard_map(
        layer,
        mesh=mesh,
        in_specs=(
            P(("dp", "seq"), None),
            P("dp", None),
            P(("dp", "seq"), None),
            P(("dp", "seq"), None),
            P(("dp", "seq"), None),
            P(("dp", "seq"), None),
        ),
        out_specs=(
            P(("dp", "seq"), None),
            P(("dp", "seq"), None),
            P(("dp", "seq"), None),
            P(("dp", "seq"), None),
            P(("dp", "seq"), None),
        ),
        check_vma=False,
    )
```

```python
import functools
import math

import jax
import jax.numpy as jnp
from jax import lax
from jax.experimental.layout import Layout, with_layout_constraint
from jax.experimental import pallas as pl
from jax.experimental.pallas import tpu as pltpu
from jax.sharding import PartitionSpec as P

D = 2304
HEADS = 8
KV_HEADS = 4
HEAD_DIM = 256
WINDOW = 128


soft_cap = 50.0
eps_norm = 1e-06
rope_base = 10000.0
gelu_coef = math.sqrt(2.0 / math.pi)


MESH = pl.DeviceIdType.MESH


def gelu_tanh(value):
    return 0.5 * value * (1.0 + jnp.tanh(gelu_coef * (value + 0.044715 * value * value * value)))


def gated_gelu(gate_pre, up_pre):
    return gelu_tanh(gate_pre) * up_pre


def rms_norm(value, gain_vec):
    return value * lax.rsqrt(jnp.mean(value * value, axis=-1, keepdims=True) + eps_norm) * gain_vec


def norm_back(value, gain_vec, incoming):
    return jax.vjp(rms_norm, value, gain_vec)[1](incoming)


def doc_layout(lengths, places):
    doc_ends = jnp.cumsum(lengths, dtype=jnp.int32)
    starts = doc_ends - lengths
    doc_ids = jnp.sum(
        (places[:, None] >= doc_ends[None, :]).astype(jnp.int32), axis=1, dtype=jnp.int32
    )
    onehot = doc_ids[:, None] == jnp.arange(lengths.shape[0], dtype=jnp.int32)[None, :]
    doc_first = jnp.sum(jnp.where(onehot, starts[None, :], 0), axis=1, dtype=jnp.int32)
    return (doc_ids, places - doc_first)


def rotate(value, doc_pos):
    half_dim = value.shape[-1] // 2
    frequency = rope_base ** (-2.0 * jnp.arange(half_dim, dtype=jnp.float32) / value.shape[-1])
    angles = doc_pos.astype(jnp.float32)[:, None] * frequency[None, :]
    cosine = jnp.cos(angles)[:, None, :]
    sine_part = jnp.sin(angles)[:, None, :]
    first_half = value[..., :half_dim]
    second_half = value[..., half_dim:]
    return jnp.concatenate(
        [
            first_half * cosine - second_half * sine_part,
            second_half * cosine + first_half * sine_part,
        ],
        axis=-1,
    )


def contract_rows(left_side, right_side):
    return lax.dot_general(
        left_side, right_side, (((0,), (0,)), ((), ())), preferred_element_type=jnp.float32
    )


def contract_cols(left_side, right_side):
    return lax.dot_general(
        left_side, right_side, (((1,), (1,)), ((), ())), preferred_element_type=jnp.float32
    )


def key_mask(query_places, query_docs, key_places, key_docs):
    return (
        (key_places[None, :] >= 0)
        & (query_docs[:, None] == key_docs[None, :])
        & (key_places[None, :] <= query_places[:, None])
        & (query_places[:, None] - key_places[None, :] < WINDOW)
    )


def attn_scores(queries, all_keys, allowed):
    scores = jnp.einsum("qkgd,pkd->kgqp", queries, all_keys, preferred_element_type=jnp.float32)
    capped = jnp.where(allowed[None, None], soft_cap * jnp.tanh(scores / soft_cap), -1e30)
    return (scores, capped)


def swapped(x):
    return lax.ppermute(x, "seq", [(0, 1), (1, 0)])


def place_of():
    dp = lax.axis_index("dp")
    seq = lax.axis_index("seq")
    a, b, c = dp // 4, lax.rem(dp // 2, 2), lax.rem(dp, 2)
    return a, b, c, seq


def number(a, b, c):
    return (a * 2 + b) * 2 + c


def enter(line, a, b, c, seq):
    barrier = pltpu.get_barrier_semaphore()

    def tell(a2, b2, c2):
        pl.semaphore_signal(
            barrier, inc=1, device_id=(number(a2, b2, c2), seq), device_id_type=MESH
        )

    tell(a, b, 1 - c)
    tell(a, 1 - b, c)

    @pl.when(a > 0)
    def _():
        tell(a - 1, b, c)

    @pl.when(a < line - 1)
    def _():
        tell(a + 1, b, c)

    peers = 2 + jnp.minimum(a, 1) + jnp.minimum(line - 1 - a, 1)
    pl.semaphore_wait(barrier, peers)


def split_at(cols):
    return cols // 768 * 128


def gather_kernel(n_dp, x_ref, out_ref, own_sem, send_sem, recv_sem):
    line = n_dp // 4
    a, b, c, seq = place_of()
    me, pair = number(a, b, c), number(a, 1 - b, c)
    halves, _, cols = x_ref.shape
    late = split_at(cols)
    spans = (pl.ds(late, cols - late), pl.ds(0, late))
    large, small = range(halves), range(halves, 2 * halves)
    own = pltpu.make_async_copy(x_ref, out_ref.at[me], own_sem)
    own.start()
    enter(line, a, b, c, seq)

    def copy(way, block, piece, own=False):
        a2 = a + (1 if way == 0 else -1 if way == 1 else 0)
        b2 = 1 - b if way == 2 else b
        c2 = 1 - c if way == 3 else c
        half, span = piece % halves, spans[piece // halves]
        there = out_ref.at[block, half, :, span]
        return pltpu.make_async_remote_copy(
            src_ref=x_ref.at[half, :, span] if own else there,
            dst_ref=there,
            send_sem=send_sem.at[way, block, piece],
            recv_sem=recv_sem.at[block, piece],
            device_id=(number(a2, b2, c2), seq),
            device_id_type=MESH,
        )

    up, down, across, over = range(4)
    has_up, has_down = a < line - 1, a > 0

    def start(way, block, piece, own=False):
        if way in (up, down):

            @pl.when(has_up if way == up else has_down)
            def _():
                copy(way, block, piece, own).start()

        else:
            copy(way, block, piece, own).start()

    def pass_on(block, piece, ways):
        copy(over, block, piece).wait_recv()
        for way in ways:
            start(way, block, piece)

    for way, pieces in ((across, small), (up, large), (down, large), (across, large),
                        (over, large), (over, small)):
        for piece in pieces:
            start(way, me, piece, own=True)

    def each_at(k, act):
        for sign, way in ((-1, up), (1, down)) if k else ((1, over),):

            @pl.when((a + sign * k >= 0) & (a + sign * k < line))
            def _(sign=sign, way=way):
                act(a + sign * k, way)

    for piece in small:
        pass_on(pair, piece, (over,))

    def after(k):
        for way, last in ((up, a == k), (down, line - 1 - a == k)):

            @pl.when(last)
            def _(way=way):
                for piece in small:
                    start(way, me, piece, own=True)
                    start(way, pair, piece)

    def from_pair(k):
        for p in large:
            each_at(k, lambda i, way, p=p: pass_on(number(i, 1 - b, c), p, (over,)))

    after(0)
    for k in range(1, line):
        for p in large:
            each_at(k, lambda i, way, p=p: pass_on(number(i, b, c), p, (way, across, over)))
        after(k)
    half_line = line // 2
    for k in range(half_line):
        from_pair(k)
    for k in range(1, line):
        for b2 in (b, 1 - b):
            for p in small:
                each_at(k, lambda i, way, b2=b2, p=p: pass_on(number(i, b2, c), p, (way, over)))
    for k in range(half_line, line):
        from_pair(k)

    for other in range(n_dp // 2):
        for piece in range(2 * halves):
            copy(over, other * 2 + 1 - c, piece).wait_recv()

    own.wait()
    for p in small:
        copy(across, me, p).wait_send()
    for i in range(line):
        near, far = number(i, b, c), number(i, 1 - b, c)
        for p in large:
            copy(across, near, p).wait_send()
        for block in (near, far):
            for piece in range(2 * halves):
                copy(over, block, piece).wait_send()
        for block, pieces in ((near, large), (near, small), (far, small)):
            for piece in pieces:

                @pl.when(has_up & (i <= a))
                def _(block=block, piece=piece):
                    copy(up, block, piece).wait_send()

                @pl.when(has_down & (i >= a))
                def _(block=block, piece=piece):
                    copy(down, block, piece).wait_send()


def gathered(x, n_dp, collective_id):
    rows, cols = x.shape
    x = x.reshape(2, rows // 2, cols)
    return pl.pallas_call(
        functools.partial(gather_kernel, n_dp),
        out_shape=jax.ShapeDtypeStruct((n_dp, *x.shape), x.dtype),
        in_specs=[pl.BlockSpec(memory_space=pltpu.VMEM)],
        out_specs=pl.BlockSpec(memory_space=pl.ANY),
        scratch_shapes=[
            pltpu.SemaphoreType.DMA,
            pltpu.SemaphoreType.DMA((4, n_dp, 4)),
            pltpu.SemaphoreType.DMA((n_dp, 4)),
        ],
        compiler_params=pltpu.CompilerParams(
            collective_id=collective_id, has_side_effects=True
        ),
        cost_estimate=pl.CostEstimate(
            flops=0, bytes_accessed=150_000_000, transcendentals=0
        ),
    )(x)


def scatter_steps(n_dp, place, prepare, produce, core_source, out_ref, from_core, from_pair, up_buf,
                  down_buf, pair_out, core_send, core_recv, pair_send, pair_recv, up_send,
                  up_recv, down_send, down_recv):
    line = n_dp // 4
    a, b, c, seq = place
    enter(line, a, b, c, seq)

    def core_copy(block):
        half = block // 2
        return pltpu.make_async_remote_copy(
            src_ref=core_source(block),
            dst_ref=from_core.at[half],
            send_sem=core_send.at[half],
            recv_sem=core_recv.at[half],
            device_id=(number(a, b, 1 - c), seq),
            device_id_type=MESH,
        )

    def pair_copy(to):
        return pltpu.make_async_remote_copy(
            src_ref=pair_out.at[to],
            dst_ref=from_pair.at[to],
            send_sem=pair_send.at[to],
            recv_sem=pair_recv.at[to],
            device_id=(number(a, 1 - b, c), seq),
            device_id_type=MESH,
        )

    def up_copy(to):
        return pltpu.make_async_remote_copy(
            src_ref=up_buf.at[to],
            dst_ref=up_buf.at[to],
            send_sem=up_send.at[to],
            recv_sem=up_recv.at[to],
            device_id=(number(a + 1, b, c), seq),
            device_id_type=MESH,
        )

    def down_copy(to):
        return pltpu.make_async_remote_copy(
            src_ref=down_buf.at[to],
            dst_ref=down_buf.at[to],
            send_sem=down_send.at[to],
            recv_sem=down_recv.at[to],
            device_id=(number(a - 1, b, c), seq),
            device_id_type=MESH,
        )

    def target_at(k, act):
        if k == 0:
            act(a, 0)
            return

        @pl.when(a + k < line)
        def _():
            act(a + k, 1)

        @pl.when(a - k >= 0)
        def _():
            act(a - k, -1)

    def each_target(act):
        for k in range(line - 1, -1, -1):
            target_at(k, act)

    def send_core(block):
        produce(block, None, core_source(block))
        core_copy(block).start()

    def send_pair(to, way):
        block = number(to, 1 - b, c)
        core_copy(block).wait_recv()
        produce(block, [from_core.at[block // 2]], pair_out.at[to])
        pair_copy(to).start()

    def first_core(to, way):
        send_core(number(to, 1 - b, 1 - c))

    prepare(1 - b, 1 - c)
    target_at(line - 1, first_core)
    prepare(1 - b, c)
    for k in range(line - 1, -1, -1):
        if k:
            target_at(k - 1, first_core)
        target_at(k, send_pair)
    prepare(b, 1 - c)
    each_target(lambda to, way: send_core(number(to, b, 1 - c)))
    prepare(b, c)

    def line_sum(to, more, dst):
        block = number(to, b, c)
        produce(block, [from_core.at[block // 2], from_pair.at[to], *more], dst)

    def send_line(to, way):
        core_copy(number(to, b, c)).wait_recv()
        pair_copy(to).wait_recv()
        if way:
            buf, copy = (up_buf, up_copy) if way == 1 else (down_buf, down_copy)
            at_end = (a == 0) if way == 1 else (a == line - 1)

            @pl.when(at_end)
            def _():
                line_sum(to, [], buf.at[to])

            @pl.when(jnp.logical_not(at_end))
            def _():
                copy(to).wait_recv()
                line_sum(to, [buf.at[to]], buf.at[to])

            copy(to).start()
        else:
            line_sum(to, [], out_ref)
            for copy, buf, there in (
                (up_copy, up_buf, a > 0),
                (down_copy, down_buf, a < line - 1),
            ):

                @pl.when(there)
                def _(copy=copy, buf=buf):
                    copy(to).wait_recv()
                    add_rows(out_ref, buf.at[to])

    each_target(send_line)

    for i in range(n_dp // 2):
        core_copy(i * 2 + 1 - c).wait_send()
    for i in range(line):
        pair_copy(i).wait_send()

        @pl.when(i > a)
        def _(i=i):
            up_copy(i).wait_send()

        @pl.when(i < a)
        def _(i=i):
            down_copy(i).wait_send()


def row_tiles(rows):
    return 16 if rows % 16 == 0 else rows


def add_rows(out_ref, term):
    tile = row_tiles(out_ref.shape[0])

    def step(i, _):
        at = pl.ds(pl.multiple_of(i * tile, tile), tile)
        out_ref[at, :] += term[at, :].astype(jnp.float32)
        return 0

    lax.fori_loop(0, out_ref.shape[0] // tile, step, 0)


def dots_kernel(n_dp, n_terms, *refs):
    lefts, rights = refs[:n_terms], refs[n_terms : 2 * n_terms]
    out_ref, parts, *scratch = refs[2 * n_terms :]
    _, rows, cols = parts.shape
    f32 = jnp.float32

    def prepare(b, c):
        for first in range(0, n_dp // 4, 4):
            blocks = [number(first + i, b, c) for i in range(4)]

            def step(j, _):
                at = pl.ds(pl.multiple_of(j * 256, 256), 256)
                total = jnp.zeros((4 * rows, 256), f32)
                for left, right in zip(lefts, rights):
                    stacked = jnp.concatenate([left[k] for k in blocks], axis=0)
                    total += jnp.dot(stacked, right[:, at], preferred_element_type=f32)
                for i, k in enumerate(blocks):
                    parts[k, :, at] = total[i * rows : (i + 1) * rows].astype(parts.dtype)
                return 0

            lax.fori_loop(0, cols // 256, step, 0)

    def produce(block, terms, dst):
        if terms is None:
            return
        tile = row_tiles(rows)

        def step(i, _):
            at = pl.ds(pl.multiple_of(i * tile, tile), tile)
            total = parts[block, at, :].astype(f32)
            for term in terms:
                total += term[at, :].astype(f32)
            dst[at, :] = total.astype(dst.dtype)
            return 0

        lax.fori_loop(0, rows // tile, step, 0)

    scatter_steps(
        n_dp, place_of(), prepare, produce, lambda block: parts.at[block], out_ref, *scratch
    )


def product_kernel(n_dp, left_a, right_a, left_b, right_b, extra, out_ref, core_out, *scratch):
    cols_a, cols_b = right_a.shape[1], right_b.shape[1]

    def produce(block, terms, dst):
        def part(left, right, first, wide):
            def step(i, _):
                inner = pl.ds(pl.multiple_of(i * wide, wide), wide)
                outer = pl.ds(pl.multiple_of(first + i * wide, 128), wide)
                total = jnp.dot(
                    left[block], right[:, inner], preferred_element_type=jnp.float32
                )
                for term in terms or []:
                    total += term[:, outer].astype(jnp.float32)
                dst[:, outer] = total.astype(dst.dtype)
                return 0

            lax.fori_loop(0, right.shape[1] // wide, step, 0)

        part(left_a, right_a, 0, 256)
        part(left_b, right_b, cols_a, 256)
        last = pl.ds(cols_a + cols_b, extra.shape[2])
        total = extra[block].astype(jnp.float32)
        for term in terms or []:
            total += term[:, last].astype(jnp.float32)
        dst[:, last] = total.astype(dst.dtype)

    scatter_steps(
        n_dp,
        place_of(),
        lambda b, c: None,
        produce,
        lambda block: core_out.at[block // 2],
        out_ref,
        *scratch,
    )


def scatter_scratch(n_dp, rows, cols, dtype):
    line = n_dp // 4
    return (
        [pltpu.VMEM((n_dp // 2, rows, cols), dtype)]
        + [pltpu.VMEM((line, rows, cols), dtype)] * 4
        + [pltpu.SemaphoreType.DMA((n_dp // 2,))] * 2
        + [pltpu.SemaphoreType.DMA((line,))] * 6
    )


def scattered_products(left_a, right_a, left_b, right_b, extra, collective_id):
    n_dp, rows, _ = left_a.shape
    cols = right_a.shape[1] + right_b.shape[1] + extra.shape[2]
    return pl.pallas_call(
        functools.partial(product_kernel, n_dp),
        out_shape=jax.ShapeDtypeStruct((rows, cols), jnp.float32),
        in_specs=[pl.BlockSpec(memory_space=pltpu.VMEM)] * 5,
        out_specs=pl.BlockSpec(memory_space=pltpu.VMEM),
        scratch_shapes=[pltpu.VMEM((n_dp // 2, rows, cols), jnp.bfloat16)]
        + scatter_scratch(n_dp, rows, cols, jnp.bfloat16),
        compiler_params=pltpu.CompilerParams(
            collective_id=collective_id, has_side_effects=True
        ),
        cost_estimate=pl.CostEstimate(
            flops=0, bytes_accessed=200_000_000, transcendentals=0
        ),
    )(left_a, right_a, left_b, right_b, extra)


def scattered_dots(lefts, rights, collective_id):
    n_dp, rows, _ = lefts[0].shape
    cols = rights[0].shape[1]
    held = n_dp * (1 + 1 / 2 + 1) * rows * cols * 2
    pieces = 1
    while held > pieces * 36 * 2**20 or cols % (256 * pieces):
        pieces += 1
    width = cols // pieces
    return jnp.concatenate(
        [
            scattered_piece(
                lefts, [r[:, i * width : (i + 1) * width] for r in rights], collective_id
            )
            for i in range(pieces)
        ],
        axis=1,
    )


def scattered_piece(lefts, rights, collective_id):
    n_dp, rows, _ = lefts[0].shape
    cols = rights[0].shape[1]
    return pl.pallas_call(
        functools.partial(dots_kernel, n_dp, len(lefts)),
        out_shape=jax.ShapeDtypeStruct((rows, cols), jnp.float32),
        in_specs=[pl.BlockSpec(memory_space=pltpu.VMEM)] * (2 * len(lefts)),
        out_specs=pl.BlockSpec(memory_space=pltpu.VMEM),
        scratch_shapes=[pltpu.VMEM((n_dp, rows, cols), jnp.bfloat16)]
        + scatter_scratch(n_dp, rows, cols, jnp.bfloat16),
        compiler_params=pltpu.CompilerParams(
            collective_id=collective_id, has_side_effects=True
        ),
        cost_estimate=pl.CostEstimate(
            flops=0, bytes_accessed=150_000_000, transcendentals=0
        ),
    )(*lefts, *rights)


def row_major(x):
    return with_layout_constraint(x, Layout(major_to_minor=(0, 1)))


def mine_and_other(halves, seq_index):
    first = seq_index == 0
    return (
        jnp.where(first, halves[0], halves[1]),
        jnp.where(first, halves[1], halves[0]),
    )


def in_order(own, other, seq_index):
    first = seq_index == 0
    return jnp.where(first, own, other), jnp.where(first, other, own)


def column_halves(weight):
    q_cols, k_cols = HEADS * HEAD_DIM, KV_HEADS * HEAD_DIM
    starts = (0, q_cols, q_cols + k_cols, q_cols + 2 * k_cols)
    sizes = (q_cols // 2, k_cols // 2, k_cols // 2, q_cols // 2)
    return [
        jnp.concatenate(
            [weight[:, s + h * n : s + (h + 1) * n] for s, n in zip(starts, sizes)], axis=1
        )
        for h in range(2)
    ]


def layer(tokens, doc_lengths, attn_weight, ffn_weight, gains, out_grad):
    tok_rows = tokens.shape[0]
    n_dp = lax.axis_size("dp")
    heads, kv_heads = HEADS // 2, KV_HEADS // 2
    q_cols = heads * HEAD_DIM
    k_cols = kv_heads * HEAD_DIM
    proj_cols = q_cols + 2 * k_cols
    half_cols = proj_cols + q_cols
    group_size = HEADS // KV_HEADS
    query_scale = HEAD_DIM ** (-0.5)
    bf16 = jnp.bfloat16
    seq_index = lax.axis_index("seq")
    weight_rows = attn_weight.shape[0]

    run = jnp.arange(tok_rows, dtype=jnp.int32)
    places = jnp.concatenate([seq_index * tok_rows + run, (1 - seq_index) * tok_rows + run])
    docs, pos = doc_layout(doc_lengths[0], places)
    allowed = key_mask(places, docs, places, docs)

    gain_cols = jnp.pad(gains, ((0, 0), (0, 124)))
    my_cols, other_cols = mine_and_other(column_halves(attn_weight), seq_index)
    my_cols = jnp.concatenate([my_cols, gain_cols], axis=1)
    other_cols = jnp.concatenate([other_cols, gain_cols], axis=1)
    partner_cols = swapped(other_cols)
    other_tokens = swapped(tokens)
    ffn_own, partner_cols = lax.optimization_barrier((ffn_weight, partner_cols))
    ffn_other = swapped(ffn_own)
    block = jnp.concatenate(in_order(my_cols, partner_cols, seq_index), axis=0)
    attn_full = gathered(block, n_dp, 0).reshape(-1, half_cols + 128)
    gain_vals = attn_full[:, half_cols : half_cols + 4].astype(jnp.float32).T
    attn_weights = attn_full[:, :proj_cols]
    out_weights = attn_full[:, proj_cols:half_cols]

    pack_tokens = jnp.concatenate([tokens, other_tokens]).astype(jnp.float32)
    tokens_f = tokens.astype(jnp.float32)
    attn_in = rms_norm(pack_tokens, gain_vals[0]).astype(bf16)
    projected = jnp.dot(attn_in, attn_weights, preferred_element_type=jnp.float32)
    pack = 2 * tok_rows
    queries = (
        rotate(projected[:, :q_cols].reshape(pack, heads, HEAD_DIM), pos) * query_scale
    ).astype(bf16)
    queries = queries.reshape(pack, kv_heads, group_size, HEAD_DIM)
    keys = rotate(
        projected[:, q_cols : q_cols + k_cols].reshape(pack, kv_heads, HEAD_DIM), pos
    ).astype(bf16)
    values = projected[:, q_cols + k_cols :].reshape(pack, kv_heads, HEAD_DIM).astype(bf16)
    scores, capped = attn_scores(queries, keys, allowed)
    row_max = jnp.max(capped, axis=-1, keepdims=True)
    exp_terms = jnp.exp(capped - row_max)
    row_total = jnp.sum(exp_terms, axis=-1, keepdims=True)
    log_total = row_max + jnp.log(row_total)
    attn_probs = (exp_terms / row_total).astype(bf16)
    mixed_heads = jnp.einsum(
        "kgqp,pkd->qkgd", attn_probs, values, preferred_element_type=jnp.float32
    )
    mixed_heads = mixed_heads.reshape(pack, q_cols).astype(bf16)
    attn_part_out = contract_cols(mixed_heads, out_weights)
    attn_part_other = swapped(attn_part_out[tok_rows:].astype(bf16))
    attn_out = attn_part_out[:tok_rows] + attn_part_other.astype(jnp.float32)
    middle = tokens_f + rms_norm(attn_out, gain_vals[1])
    ffn_input = rms_norm(middle, gain_vals[2]).astype(bf16)

    gate_weights, up_weights, down_weights = [
        jnp.concatenate([ffn_own[:, k * D : (k + 1) * D], ffn_other[:, k * D : (k + 1) * D]])
        for k in range(3)
    ]
    unit_count = gate_weights.shape[0]
    ffn_all = gathered(ffn_input, n_dp, 1).reshape(-1, D)
    gate = contract_cols(ffn_all, gate_weights)
    up = contract_cols(ffn_all, up_weights)
    hidden = row_major(gated_gelu(gate, up).astype(bf16))
    ffn_out = scattered_dots([hidden.reshape(n_dp, tok_rows, -1)], [down_weights], 2)
    out_gain = gain_vals[3]
    block_out = (middle + rms_norm(ffn_out, out_gain)).astype(bf16)
    cotangent = out_grad.astype(jnp.float32)
    d_ffn_f, d_gain_out = norm_back(ffn_out, out_gain, cotangent)
    d_ffn_all = gathered(d_ffn_f.astype(bf16), n_dp, 1).reshape(-1, D)
    d_hidden = contract_cols(d_ffn_all, down_weights)
    d_gate, d_up = jax.vjp(gated_gelu, gate, up)[1](d_hidden)
    d_gate, d_up = row_major(d_gate.astype(bf16)), row_major(d_up.astype(bf16))
    d_ffn_input = scattered_dots(
        [d_gate.reshape(n_dp, tok_rows, -1), d_up.reshape(n_dp, tok_rows, -1)],
        [gate_weights, up_weights],
        4,
    )

    own_units = unit_count // 2
    weight_sum = [
        contract_rows(d_gate, ffn_all),
        contract_rows(d_up, ffn_all),
        contract_rows(hidden, d_ffn_all),
    ]
    sent = jnp.concatenate([w[own_units:].astype(bf16) for w in weight_sum], axis=1)
    kept = jnp.concatenate([w[:own_units] for w in weight_sum], axis=1)
    grad_other = swapped(sent)
    ffn_weight_grad = kept + grad_other.astype(jnp.float32)

    d_middle_add, d_gain_ffn = norm_back(middle, gain_vals[2], d_ffn_input)
    d_middle = cotangent + d_middle_add
    d_attn_f, d_gain_post = norm_back(attn_out, gain_vals[1], d_middle)
    d_attn_own = d_attn_f.astype(bf16)
    d_attn_other = swapped(d_attn_own)
    d_attn = jnp.concatenate([d_attn_own, d_attn_other])
    d_mixed = jnp.dot(d_attn, out_weights, preferred_element_type=jnp.float32).astype(bf16)
    d_mixed = d_mixed.reshape(pack, kv_heads, group_size, HEAD_DIM)
    attn_p = jnp.exp(capped - log_total)
    d_probs = jnp.einsum("qkgd,pkd->kgqp", d_mixed, values, preferred_element_type=jnp.float32)
    d_values = jnp.einsum(
        "kgqp,qkgd->pkd", attn_probs, d_mixed, preferred_element_type=jnp.float32
    )
    d_capped = attn_p * (d_probs - jnp.sum(attn_p * d_probs, axis=-1, keepdims=True))
    tanh_part = jnp.tanh(scores / soft_cap)
    d_scores = (d_capped * (1.0 - tanh_part * tanh_part)).astype(bf16)
    d_queries = jnp.einsum("kgqp,pkd->qkgd", d_scores, keys, preferred_element_type=jnp.float32)
    d_keys = jnp.einsum("kgqp,qkgd->pkd", d_scores, queries, preferred_element_type=jnp.float32)
    d_query_raw = rotate(d_queries.reshape(pack, heads, HEAD_DIM) * query_scale, -pos)
    d_key_raw = rotate(d_keys, -pos)
    d_projected = jnp.concatenate(
        [
            d_query_raw.reshape(pack, q_cols),
            d_key_raw.reshape(pack, k_cols),
            d_values.reshape(pack, k_cols),
        ],
        axis=1,
    ).astype(bf16)
    d_attn_in_part = contract_cols(d_projected, attn_weights)
    d_attn_in_other = swapped(d_attn_in_part[tok_rows:].astype(bf16))
    d_attn_in = d_attn_in_part[:tok_rows] + d_attn_in_other.astype(jnp.float32)
    normed = pack_tokens * lax.rsqrt(
        jnp.mean(pack_tokens * pack_tokens, axis=-1, keepdims=True) + eps_norm
    )
    d_gain_in = jnp.sum(d_attn_in_part * normed, axis=0)

    gain_part = jnp.stack([d_gain_in, d_gain_post, d_gain_ffn, d_gain_out], axis=1)
    block_rows = (n_dp, 2 * weight_rows)
    attn_sum = scattered_products(
        attn_in.T.reshape(*block_rows, pack),
        d_projected,
        d_attn.T.reshape(*block_rows, pack),
        mixed_heads,
        jnp.pad(gain_part.astype(bf16), ((0, 0), (0, 124))).reshape(*block_rows, 128),
        3,
    )
    d_tokens_add = norm_back(tokens_f, gain_vals[0], d_attn_in)[0]
    tokens_grad = d_middle + d_tokens_add
    mine, others = mine_and_other(
        (attn_sum[:weight_rows], attn_sum[weight_rows:]), seq_index
    )
    partner = swapped(others.astype(bf16)).astype(jnp.float32)
    gains_grad = mine[:, half_cols : half_cols + 4] + partner[:, half_cols : half_cols + 4]
    first, second = in_order(mine, partner, seq_index)
    cuts = ((0, q_cols), (q_cols, q_cols + k_cols), (q_cols + k_cols, proj_cols),
            (proj_cols, half_cols))
    attn_weight_grad = jnp.concatenate(
        [half[:, lo:hi] for lo, hi in cuts for half in (first, second)], axis=1
    )
    return (block_out, tokens_grad, attn_weight_grad, ffn_weight_grad, gains_grad)


def solution(mesh):
    return jax.shard_map(
        layer,
        mesh=mesh,
        in_specs=(
            P(("dp", "seq"), None),
            P("dp", None),
            P(("dp", "seq"), None),
            P(("dp", "seq"), None),
            P(("dp", "seq"), None),
            P(("dp", "seq"), None),
        ),
        out_specs=(
            P(("dp", "seq"), None),
            P(("dp", "seq"), None),
            P(("dp", "seq"), None),
            P(("dp", "seq"), None),
            P(("dp", "seq"), None),
        ),
        check_vma=False,
    )
```

```python
import functools
import math

import jax
import jax.numpy as jnp
from jax import lax
from jax.experimental.layout import Layout, with_layout_constraint
from jax.experimental import pallas as pl
from jax.experimental.pallas import tpu as pltpu
from jax.sharding import PartitionSpec as P

D = 2304
HEADS = 8
KV_HEADS = 4
HEAD_DIM = 256
WINDOW = 128


soft_cap = 50.0
eps_norm = 1e-06
rope_base = 10000.0
gelu_coef = math.sqrt(2.0 / math.pi)


MESH = pl.DeviceIdType.MESH


def gelu_tanh(value):
    return 0.5 * value * (1.0 + jnp.tanh(gelu_coef * (value + 0.044715 * value * value * value)))


def gated_gelu(gate_pre, up_pre):
    return gelu_tanh(gate_pre) * up_pre


def rms_norm(value, gain_vec):
    return value * lax.rsqrt(jnp.mean(value * value, axis=-1, keepdims=True) + eps_norm) * gain_vec


def norm_back(value, gain_vec, incoming):
    return jax.vjp(rms_norm, value, gain_vec)[1](incoming)


def doc_layout(lengths, places):
    doc_ends = jnp.cumsum(lengths, dtype=jnp.int32)
    starts = doc_ends - lengths
    doc_ids = jnp.sum(
        (places[:, None] >= doc_ends[None, :]).astype(jnp.int32), axis=1, dtype=jnp.int32
    )
    onehot = doc_ids[:, None] == jnp.arange(lengths.shape[0], dtype=jnp.int32)[None, :]
    doc_first = jnp.sum(jnp.where(onehot, starts[None, :], 0), axis=1, dtype=jnp.int32)
    return (doc_ids, places - doc_first)


def rotate(value, doc_pos):
    half_dim = value.shape[-1] // 2
    frequency = rope_base ** (-2.0 * jnp.arange(half_dim, dtype=jnp.float32) / value.shape[-1])
    angles = doc_pos.astype(jnp.float32)[:, None] * frequency[None, :]
    cosine = jnp.cos(angles)[:, None, :]
    sine_part = jnp.sin(angles)[:, None, :]
    first_half = value[..., :half_dim]
    second_half = value[..., half_dim:]
    return jnp.concatenate(
        [
            first_half * cosine - second_half * sine_part,
            second_half * cosine + first_half * sine_part,
        ],
        axis=-1,
    )


def contract_rows(left_side, right_side):
    return lax.dot_general(
        left_side, right_side, (((0,), (0,)), ((), ())), preferred_element_type=jnp.float32
    )


def contract_cols(left_side, right_side):
    return lax.dot_general(
        left_side, right_side, (((1,), (1,)), ((), ())), preferred_element_type=jnp.float32
    )


def key_mask(query_places, query_docs, key_places, key_docs):
    return (
        (key_places[None, :] >= 0)
        & (query_docs[:, None] == key_docs[None, :])
        & (key_places[None, :] <= query_places[:, None])
        & (query_places[:, None] - key_places[None, :] < WINDOW)
    )


def attn_scores(queries, all_keys, allowed):
    scores = jnp.einsum("qkgd,pkd->kgqp", queries, all_keys, preferred_element_type=jnp.float32)
    capped = jnp.where(allowed[None, None], soft_cap * jnp.tanh(scores / soft_cap), -1e30)
    return (scores, capped)


def swapped(x):
    return lax.ppermute(x, "seq", [(0, 1), (1, 0)])


def place_of():
    dp = lax.axis_index("dp")
    seq = lax.axis_index("seq")
    a, b, c = dp // 4, lax.rem(dp // 2, 2), lax.rem(dp, 2)
    return a, b, c, seq


def number(a, b, c):
    return (a * 2 + b) * 2 + c


def enter(line, a, b, c, seq):
    barrier = pltpu.get_barrier_semaphore()

    def tell(a2, b2, c2):
        pl.semaphore_signal(
            barrier, inc=1, device_id=(number(a2, b2, c2), seq), device_id_type=MESH
        )

    tell(a, b, 1 - c)
    tell(a, 1 - b, c)

    @pl.when(a > 0)
    def _():
        tell(a - 1, b, c)

    @pl.when(a < line - 1)
    def _():
        tell(a + 1, b, c)

    peers = 2 + jnp.minimum(a, 1) + jnp.minimum(line - 1 - a, 1)
    pl.semaphore_wait(barrier, peers)


def split_at(cols):
    return cols // 768 * 128


def gather_kernel(n_dp, x_ref, out_ref, own_sem, send_sem, recv_sem):
    line = n_dp // 4
    a, b, c, seq = place_of()
    me, pair = number(a, b, c), number(a, 1 - b, c)
    cols = x_ref.shape[1]
    late = split_at(cols)
    spans = (pl.ds(late, cols - late), pl.ds(0, late))
    own = pltpu.make_async_copy(x_ref, out_ref.at[me], own_sem)
    own.start()
    enter(line, a, b, c, seq)

    def copy(way, block, piece, own=False):
        a2 = a + (1 if way == 0 else -1 if way == 1 else 0)
        b2 = 1 - b if way == 2 else b
        c2 = 1 - c if way == 3 else c
        there = out_ref.at[block, :, spans[piece]]
        return pltpu.make_async_remote_copy(
            src_ref=x_ref.at[:, spans[piece]] if own else there,
            dst_ref=there,
            send_sem=send_sem.at[way, block, piece],
            recv_sem=recv_sem.at[block, piece],
            device_id=(number(a2, b2, c2), seq),
            device_id_type=MESH,
        )

    up, down, across, over = range(4)
    has_up, has_down = a < line - 1, a > 0

    def start(way, block, piece, own=False):
        if way in (up, down):

            @pl.when(has_up if way == up else has_down)
            def _():
                copy(way, block, piece, own).start()

        else:
            copy(way, block, piece, own).start()

    def pass_on(block, piece, ways):
        copy(over, block, piece).wait_recv()
        for way in ways:
            start(way, block, piece)

    for way, piece in ((up, 0), (down, 0), (across, 1), (across, 0), (over, 0), (over, 1)):
        start(way, me, piece, own=True)

    def each_at(k, act):
        for sign, way in ((-1, up), (1, down)) if k else ((1, over),):

            @pl.when((a + sign * k >= 0) & (a + sign * k < line))
            def _(sign=sign, way=way):
                act(a + sign * k, way)

    pass_on(pair, 1, (over,))

    def after(k):
        for way, last in ((up, a == k), (down, line - 1 - a == k)):

            @pl.when(last)
            def _(way=way):
                start(way, me, 1, own=True)
                start(way, pair, 1)

    def from_pair(k):
        each_at(k, lambda i, way: pass_on(number(i, 1 - b, c), 0, (over,)))

    after(0)
    for k in range(1, line):
        each_at(k, lambda i, way: pass_on(number(i, b, c), 0, (way, across, over)))
        after(k)
    half = line // 2
    for k in range(half):
        from_pair(k)
    for k in range(1, line):
        for b2 in (b, 1 - b):
            each_at(k, lambda i, way, b2=b2: pass_on(number(i, b2, c), 1, (way, over)))
    for k in range(half, line):
        from_pair(k)

    for other in range(n_dp // 2):
        for piece in range(2):
            copy(over, other * 2 + 1 - c, piece).wait_recv()

    own.wait()
    copy(across, me, 1).wait_send()
    for i in range(line):
        near, far = number(i, b, c), number(i, 1 - b, c)
        copy(across, near, 0).wait_send()
        for block, piece in ((near, 0), (near, 1), (far, 0), (far, 1)):
            copy(over, block, piece).wait_send()
        for block, piece in ((near, 0), (near, 1), (far, 1)):

            @pl.when(has_up & (i <= a))
            def _(block=block, piece=piece):
                copy(up, block, piece).wait_send()

            @pl.when(has_down & (i >= a))
            def _(block=block, piece=piece):
                copy(down, block, piece).wait_send()


def gathered(x, n_dp, collective_id):
    return pl.pallas_call(
        functools.partial(gather_kernel, n_dp),
        out_shape=jax.ShapeDtypeStruct((n_dp, *x.shape), x.dtype),
        in_specs=[pl.BlockSpec(memory_space=pltpu.VMEM)],
        out_specs=pl.BlockSpec(memory_space=pl.ANY),
        scratch_shapes=[
            pltpu.SemaphoreType.DMA,
            pltpu.SemaphoreType.DMA((4, n_dp, 2)),
            pltpu.SemaphoreType.DMA((n_dp, 2)),
        ],
        compiler_params=pltpu.CompilerParams(
            collective_id=collective_id, has_side_effects=True
        ),
        cost_estimate=pl.CostEstimate(
            flops=0, bytes_accessed=150_000_000, transcendentals=0
        ),
    )(x)


def scatter_steps(n_dp, place, prepare, produce, core_source, out_ref, from_core, from_pair, up_buf,
                  down_buf, pair_out, core_send, core_recv, pair_send, pair_recv, up_send,
                  up_recv, down_send, down_recv):
    line = n_dp // 4
    a, b, c, seq = place
    enter(line, a, b, c, seq)

    def core_copy(block):
        half = block // 2
        return pltpu.make_async_remote_copy(
            src_ref=core_source(block),
            dst_ref=from_core.at[half],
            send_sem=core_send.at[half],
            recv_sem=core_recv.at[half],
            device_id=(number(a, b, 1 - c), seq),
            device_id_type=MESH,
        )

    def pair_copy(to):
        return pltpu.make_async_remote_copy(
            src_ref=pair_out.at[to],
            dst_ref=from_pair.at[to],
            send_sem=pair_send.at[to],
            recv_sem=pair_recv.at[to],
            device_id=(number(a, 1 - b, c), seq),
            device_id_type=MESH,
        )

    def up_copy(to):
        return pltpu.make_async_remote_copy(
            src_ref=up_buf.at[to],
            dst_ref=up_buf.at[to],
            send_sem=up_send.at[to],
            recv_sem=up_recv.at[to],
            device_id=(number(a + 1, b, c), seq),
            device_id_type=MESH,
        )

    def down_copy(to):
        return pltpu.make_async_remote_copy(
            src_ref=down_buf.at[to],
            dst_ref=down_buf.at[to],
            send_sem=down_send.at[to],
            recv_sem=down_recv.at[to],
            device_id=(number(a - 1, b, c), seq),
            device_id_type=MESH,
        )

    def each_target(act):
        for k in range(line - 1, 0, -1):

            @pl.when(a + k < line)
            def _(k=k):
                act(a + k, 1)

            @pl.when(a - k >= 0)
            def _(k=k):
                act(a - k, -1)

        act(a, 0)

    def send_core(block):
        produce(block, None, core_source(block))
        core_copy(block).start()

    prepare(1 - b, 1 - c)
    each_target(lambda to, way: send_core(number(to, 1 - b, 1 - c)))
    prepare(1 - b, c)

    def send_pair(to, way):
        block = number(to, 1 - b, c)
        core_copy(block).wait_recv()
        produce(block, [from_core.at[block // 2]], pair_out.at[to])
        pair_copy(to).start()

    each_target(send_pair)
    prepare(b, 1 - c)
    each_target(lambda to, way: send_core(number(to, b, 1 - c)))
    prepare(b, c)

    def line_sum(to, more, dst):
        block = number(to, b, c)
        produce(block, [from_core.at[block // 2], from_pair.at[to], *more], dst)

    def send_line(to, way):
        core_copy(number(to, b, c)).wait_recv()
        pair_copy(to).wait_recv()
        if way:
            buf, copy = (up_buf, up_copy) if way == 1 else (down_buf, down_copy)
            at_end = (a == 0) if way == 1 else (a == line - 1)

            @pl.when(at_end)
            def _():
                line_sum(to, [], buf.at[to])

            @pl.when(jnp.logical_not(at_end))
            def _():
                copy(to).wait_recv()
                line_sum(to, [buf.at[to]], buf.at[to])

            copy(to).start()
        else:
            line_sum(to, [], out_ref)
            for copy, buf, there in (
                (up_copy, up_buf, a > 0),
                (down_copy, down_buf, a < line - 1),
            ):

                @pl.when(there)
                def _(copy=copy, buf=buf):
                    copy(to).wait_recv()
                    add_rows(out_ref, buf.at[to])

    each_target(send_line)

    for i in range(n_dp // 2):
        core_copy(i * 2 + 1 - c).wait_send()
    for i in range(line):
        pair_copy(i).wait_send()

        @pl.when(i > a)
        def _(i=i):
            up_copy(i).wait_send()

        @pl.when(i < a)
        def _(i=i):
            down_copy(i).wait_send()


def row_tiles(rows):
    return 16 if rows % 16 == 0 else rows


def add_rows(out_ref, term):
    tile = row_tiles(out_ref.shape[0])

    def step(i, _):
        at = pl.ds(pl.multiple_of(i * tile, tile), tile)
        out_ref[at, :] += term[at, :].astype(jnp.float32)
        return 0

    lax.fori_loop(0, out_ref.shape[0] // tile, step, 0)


def dots_kernel(n_dp, n_terms, *refs):
    lefts, rights = refs[:n_terms], refs[n_terms : 2 * n_terms]
    out_ref, parts, *scratch = refs[2 * n_terms :]
    _, rows, cols = parts.shape
    f32 = jnp.float32

    def prepare(b, c):
        for first in range(0, n_dp // 4, 4):
            blocks = [number(first + i, b, c) for i in range(4)]

            def step(j, _):
                at = pl.ds(pl.multiple_of(j * 256, 256), 256)
                total = jnp.zeros((4 * rows, 256), f32)
                for left, right in zip(lefts, rights):
                    stacked = jnp.concatenate([left[k] for k in blocks], axis=0)
                    total += jnp.dot(stacked, right[:, at], preferred_element_type=f32)
                for i, k in enumerate(blocks):
                    parts[k, :, at] = total[i * rows : (i + 1) * rows].astype(parts.dtype)
                return 0

            lax.fori_loop(0, cols // 256, step, 0)

    def produce(block, terms, dst):
        if terms is None:
            return
        tile = row_tiles(rows)

        def step(i, _):
            at = pl.ds(pl.multiple_of(i * tile, tile), tile)
            total = parts[block, at, :].astype(f32)
            for term in terms:
                total += term[at, :].astype(f32)
            dst[at, :] = total.astype(dst.dtype)
            return 0

        lax.fori_loop(0, rows // tile, step, 0)

    scatter_steps(
        n_dp, place_of(), prepare, produce, lambda block: parts.at[block], out_ref, *scratch
    )


def product_kernel(n_dp, left_a, right_a, left_b, right_b, extra, out_ref, core_out, *scratch):
    cols_a, cols_b = right_a.shape[1], right_b.shape[1]

    def produce(block, terms, dst):
        def part(left, right, first, wide):
            def step(i, _):
                inner = pl.ds(pl.multiple_of(i * wide, wide), wide)
                outer = pl.ds(pl.multiple_of(first + i * wide, 128), wide)
                total = jnp.dot(
                    left[block], right[:, inner], preferred_element_type=jnp.float32
                )
                for term in terms or []:
                    total += term[:, outer].astype(jnp.float32)
                dst[:, outer] = total.astype(dst.dtype)
                return 0

            lax.fori_loop(0, right.shape[1] // wide, step, 0)

        part(left_a, right_a, 0, 256)
        part(left_b, right_b, cols_a, 256)
        last = pl.ds(cols_a + cols_b, extra.shape[2])
        total = extra[block].astype(jnp.float32)
        for term in terms or []:
            total += term[:, last].astype(jnp.float32)
        dst[:, last] = total.astype(dst.dtype)

    scatter_steps(
        n_dp,
        place_of(),
        lambda b, c: None,
        produce,
        lambda block: core_out.at[block // 2],
        out_ref,
        *scratch,
    )


def scatter_scratch(n_dp, rows, cols, dtype):
    line = n_dp // 4
    return (
        [pltpu.VMEM((n_dp // 2, rows, cols), dtype)]
        + [pltpu.VMEM((line, rows, cols), dtype)] * 4
        + [pltpu.SemaphoreType.DMA((n_dp // 2,))] * 2
        + [pltpu.SemaphoreType.DMA((line,))] * 6
    )


def scattered_products(left_a, right_a, left_b, right_b, extra, collective_id):
    n_dp, rows, _ = left_a.shape
    cols = right_a.shape[1] + right_b.shape[1] + extra.shape[2]
    return pl.pallas_call(
        functools.partial(product_kernel, n_dp),
        out_shape=jax.ShapeDtypeStruct((rows, cols), jnp.float32),
        in_specs=[pl.BlockSpec(memory_space=pltpu.VMEM)] * 5,
        out_specs=pl.BlockSpec(memory_space=pltpu.VMEM),
        scratch_shapes=[pltpu.VMEM((n_dp // 2, rows, cols), jnp.bfloat16)]
        + scatter_scratch(n_dp, rows, cols, jnp.bfloat16),
        compiler_params=pltpu.CompilerParams(
            collective_id=collective_id, has_side_effects=True
        ),
        cost_estimate=pl.CostEstimate(
            flops=0, bytes_accessed=200_000_000, transcendentals=0
        ),
    )(left_a, right_a, left_b, right_b, extra)


def scattered_dots(lefts, rights, collective_id):
    n_dp, rows, _ = lefts[0].shape
    cols = rights[0].shape[1]
    held = n_dp * (1 + 1 / 2 + 1) * rows * cols * 2
    pieces = 1
    while held > pieces * 36 * 2**20 or cols % (256 * pieces):
        pieces += 1
    width = cols // pieces
    return jnp.concatenate(
        [
            scattered_piece(
                lefts, [r[:, i * width : (i + 1) * width] for r in rights], collective_id
            )
            for i in range(pieces)
        ],
        axis=1,
    )


def scattered_piece(lefts, rights, collective_id):
    n_dp, rows, _ = lefts[0].shape
    cols = rights[0].shape[1]
    return pl.pallas_call(
        functools.partial(dots_kernel, n_dp, len(lefts)),
        out_shape=jax.ShapeDtypeStruct((rows, cols), jnp.float32),
        in_specs=[pl.BlockSpec(memory_space=pltpu.VMEM)] * (2 * len(lefts)),
        out_specs=pl.BlockSpec(memory_space=pltpu.VMEM),
        scratch_shapes=[pltpu.VMEM((n_dp, rows, cols), jnp.bfloat16)]
        + scatter_scratch(n_dp, rows, cols, jnp.bfloat16),
        compiler_params=pltpu.CompilerParams(
            collective_id=collective_id, has_side_effects=True
        ),
        cost_estimate=pl.CostEstimate(
            flops=0, bytes_accessed=150_000_000, transcendentals=0
        ),
    )(*lefts, *rights)


def row_major(x):
    return with_layout_constraint(x, Layout(major_to_minor=(0, 1)))


def mine_and_other(halves, seq_index):
    first = seq_index == 0
    return (
        jnp.where(first, halves[0], halves[1]),
        jnp.where(first, halves[1], halves[0]),
    )


def in_order(own, other, seq_index):
    first = seq_index == 0
    return jnp.where(first, own, other), jnp.where(first, other, own)


def column_halves(weight):
    q_cols, k_cols = HEADS * HEAD_DIM, KV_HEADS * HEAD_DIM
    starts = (0, q_cols, q_cols + k_cols, q_cols + 2 * k_cols)
    sizes = (q_cols // 2, k_cols // 2, k_cols // 2, q_cols // 2)
    return [
        jnp.concatenate(
            [weight[:, s + h * n : s + (h + 1) * n] for s, n in zip(starts, sizes)], axis=1
        )
        for h in range(2)
    ]


def layer(tokens, doc_lengths, attn_weight, ffn_weight, gains, out_grad):
    tok_rows = tokens.shape[0]
    n_dp = lax.axis_size("dp")
    heads, kv_heads = HEADS // 2, KV_HEADS // 2
    q_cols = heads * HEAD_DIM
    k_cols = kv_heads * HEAD_DIM
    proj_cols = q_cols + 2 * k_cols
    half_cols = proj_cols + q_cols
    group_size = HEADS // KV_HEADS
    query_scale = HEAD_DIM ** (-0.5)
    bf16 = jnp.bfloat16
    seq_index = lax.axis_index("seq")
    weight_rows = attn_weight.shape[0]

    run = jnp.arange(tok_rows, dtype=jnp.int32)
    places = jnp.concatenate([seq_index * tok_rows + run, (1 - seq_index) * tok_rows + run])
    docs, pos = doc_layout(doc_lengths[0], places)
    allowed = key_mask(places, docs, places, docs)

    gain_cols = jnp.pad(gains, ((0, 0), (0, 124)))
    my_cols, other_cols = mine_and_other(column_halves(attn_weight), seq_index)
    my_cols = jnp.concatenate([my_cols, gain_cols], axis=1)
    other_cols = jnp.concatenate([other_cols, gain_cols], axis=1)
    partner_cols = swapped(other_cols)
    other_tokens = swapped(tokens)
    ffn_own, partner_cols = lax.optimization_barrier((ffn_weight, partner_cols))
    ffn_other = swapped(ffn_own)
    block = jnp.concatenate(in_order(my_cols, partner_cols, seq_index), axis=0)
    attn_full = gathered(block, n_dp, 0).reshape(-1, half_cols + 128)
    gain_vals = attn_full[:, half_cols : half_cols + 4].astype(jnp.float32).T
    attn_weights = attn_full[:, :proj_cols]
    out_weights = attn_full[:, proj_cols:half_cols]

    pack_tokens = jnp.concatenate([tokens, other_tokens]).astype(jnp.float32)
    tokens_f = tokens.astype(jnp.float32)
    attn_in = rms_norm(pack_tokens, gain_vals[0]).astype(bf16)
    block_rows = (n_dp, 2 * weight_rows)
    attn_in_turned = attn_in.T.reshape(*block_rows, 2 * tok_rows)
    projected = jnp.dot(attn_in, attn_weights, preferred_element_type=jnp.float32)
    pack = 2 * tok_rows
    queries = (
        rotate(projected[:, :q_cols].reshape(pack, heads, HEAD_DIM), pos) * query_scale
    ).astype(bf16)
    queries = queries.reshape(pack, kv_heads, group_size, HEAD_DIM)
    keys = rotate(
        projected[:, q_cols : q_cols + k_cols].reshape(pack, kv_heads, HEAD_DIM), pos
    ).astype(bf16)
    values = projected[:, q_cols + k_cols :].reshape(pack, kv_heads, HEAD_DIM).astype(bf16)
    scores, capped = attn_scores(queries, keys, allowed)
    row_max = jnp.max(capped, axis=-1, keepdims=True)
    exp_terms = jnp.exp(capped - row_max)
    row_total = jnp.sum(exp_terms, axis=-1, keepdims=True)
    log_total = row_max + jnp.log(row_total)
    attn_probs = (exp_terms / row_total).astype(bf16)
    mixed_heads = jnp.einsum(
        "kgqp,pkd->qkgd", attn_probs, values, preferred_element_type=jnp.float32
    )
    mixed_heads = mixed_heads.reshape(pack, q_cols).astype(bf16)
    attn_part_out = contract_cols(mixed_heads, out_weights)
    attn_part_other = swapped(attn_part_out[tok_rows:].astype(bf16))
    attn_out = attn_part_out[:tok_rows] + attn_part_other.astype(jnp.float32)
    middle = tokens_f + rms_norm(attn_out, gain_vals[1])
    ffn_input = rms_norm(middle, gain_vals[2]).astype(bf16)

    gate_weights, up_weights, down_weights = [
        jnp.concatenate([ffn_own[:, k * D : (k + 1) * D], ffn_other[:, k * D : (k + 1) * D]])
        for k in range(3)
    ]
    unit_count = gate_weights.shape[0]
    ffn_all = gathered(ffn_input, n_dp, 1).reshape(-1, D)
    gate = contract_cols(ffn_all, gate_weights)
    up = contract_cols(ffn_all, up_weights)
    hidden = row_major(gated_gelu(gate, up).astype(bf16))
    ffn_out = scattered_dots([hidden.reshape(n_dp, tok_rows, -1)], [down_weights], 2)
    out_gain = gain_vals[3]
    block_out = (middle + rms_norm(ffn_out, out_gain)).astype(bf16)
    cotangent = out_grad.astype(jnp.float32)
    d_ffn_f, d_gain_out = norm_back(ffn_out, out_gain, cotangent)
    d_ffn_all = gathered(d_ffn_f.astype(bf16), n_dp, 1).reshape(-1, D)
    d_hidden = contract_cols(d_ffn_all, down_weights)
    d_gate, d_up = jax.vjp(gated_gelu, gate, up)[1](d_hidden)
    d_gate, d_up = row_major(d_gate.astype(bf16)), row_major(d_up.astype(bf16))
    d_ffn_input = scattered_dots(
        [d_gate.reshape(n_dp, tok_rows, -1), d_up.reshape(n_dp, tok_rows, -1)],
        [gate_weights, up_weights],
        4,
    )

    own_units = unit_count // 2
    weight_sum = [
        contract_rows(d_gate, ffn_all),
        contract_rows(d_up, ffn_all),
        contract_rows(hidden, d_ffn_all),
    ]
    sent = jnp.concatenate([w[own_units:].astype(bf16) for w in weight_sum], axis=1)
    kept = jnp.concatenate([w[:own_units] for w in weight_sum], axis=1)
    grad_other = swapped(sent)
    ffn_weight_grad = kept + grad_other.astype(jnp.float32)

    d_middle_add, d_gain_ffn = norm_back(middle, gain_vals[2], d_ffn_input)
    d_middle = cotangent + d_middle_add
    d_attn_f, d_gain_post = norm_back(attn_out, gain_vals[1], d_middle)
    d_attn_own = d_attn_f.astype(bf16)
    d_attn_other = swapped(d_attn_own)
    d_attn = jnp.concatenate([d_attn_own, d_attn_other])
    d_mixed = jnp.dot(d_attn, out_weights, preferred_element_type=jnp.float32).astype(bf16)
    d_mixed = d_mixed.reshape(pack, kv_heads, group_size, HEAD_DIM)
    attn_p = jnp.exp(capped - log_total)
    d_probs = jnp.einsum("qkgd,pkd->kgqp", d_mixed, values, preferred_element_type=jnp.float32)
    d_values = jnp.einsum(
        "kgqp,qkgd->pkd", attn_probs, d_mixed, preferred_element_type=jnp.float32
    )
    d_capped = attn_p * (d_probs - jnp.sum(attn_p * d_probs, axis=-1, keepdims=True))
    tanh_part = jnp.tanh(scores / soft_cap)
    d_scores = (d_capped * (1.0 - tanh_part * tanh_part)).astype(bf16)
    d_queries = jnp.einsum("kgqp,pkd->qkgd", d_scores, keys, preferred_element_type=jnp.float32)
    d_keys = jnp.einsum("kgqp,qkgd->pkd", d_scores, queries, preferred_element_type=jnp.float32)
    d_query_raw = rotate(d_queries.reshape(pack, heads, HEAD_DIM) * query_scale, -pos)
    d_key_raw = rotate(d_keys, -pos)
    d_projected = jnp.concatenate(
        [
            d_query_raw.reshape(pack, q_cols),
            d_key_raw.reshape(pack, k_cols),
            d_values.reshape(pack, k_cols),
        ],
        axis=1,
    ).astype(bf16)
    d_attn_in_part = contract_cols(d_projected, attn_weights)
    d_attn_in_other = swapped(d_attn_in_part[tok_rows:].astype(bf16))
    d_attn_in = d_attn_in_part[:tok_rows] + d_attn_in_other.astype(jnp.float32)
    normed = pack_tokens * lax.rsqrt(
        jnp.mean(pack_tokens * pack_tokens, axis=-1, keepdims=True) + eps_norm
    )
    d_gain_in = jnp.sum(d_attn_in_part * normed, axis=0)

    gain_part = jnp.stack([d_gain_in, d_gain_post, d_gain_ffn, d_gain_out], axis=1)
    attn_sum = scattered_products(
        attn_in_turned,
        d_projected,
        d_attn.T.reshape(*block_rows, pack),
        mixed_heads,
        jnp.pad(gain_part.astype(bf16), ((0, 0), (0, 124))).reshape(*block_rows, 128),
        3,
    )
    d_tokens_add = norm_back(tokens_f, gain_vals[0], d_attn_in)[0]
    tokens_grad = d_middle + d_tokens_add
    mine, others = mine_and_other(
        (attn_sum[:weight_rows], attn_sum[weight_rows:]), seq_index
    )
    partner = swapped(others.astype(bf16))
    partner = partner.astype(jnp.float32)
    gains_grad = mine[:, half_cols : half_cols + 4] + partner[:, half_cols : half_cols + 4]
    first, second = in_order(mine, partner, seq_index)
    cuts = ((0, q_cols), (q_cols, q_cols + k_cols), (q_cols + k_cols, proj_cols),
            (proj_cols, half_cols))
    attn_weight_grad = jnp.concatenate(
        [half[:, lo:hi] for lo, hi in cuts for half in (first, second)], axis=1
    )
    return (block_out, tokens_grad, attn_weight_grad, ffn_weight_grad, gains_grad)


def solution(mesh):
    return jax.shard_map(
        layer,
        mesh=mesh,
        in_specs=(
            P(("dp", "seq"), None),
            P("dp", None),
            P(("dp", "seq"), None),
            P(("dp", "seq"), None),
            P(("dp", "seq"), None),
            P(("dp", "seq"), None),
        ),
        out_specs=(
            P(("dp", "seq"), None),
            P(("dp", "seq"), None),
            P(("dp", "seq"), None),
            P(("dp", "seq"), None),
            P(("dp", "seq"), None),
        ),
        check_vma=False,
    )
```
